32 devices in a mesh: gx: 4 (over z), gy: 8 (over y, x, core).
Axes of the slice: x: 2, y: 2, z: 4, core: 2. Of those that a mesh axis runs over, the one named last changes fastest.
Arguments:
- tokens: bfloat16 [33856, 768], P(('gx', 'gy')), may hold values from -6 to 6
- lengths: int32 [64], P(('gx', 'gy')), may hold values from 40 to 529, as said below
- key_mask: int32 [64, 529], P(('gx', 'gy')), may hold values 0 or 1
- ln1_gain: bfloat16 [768], P(('gx', 'gy')), may hold values from 0.5 to 1.5
- ln1_bias: bfloat16 [768], P(('gx', 'gy')), may hold values from -1.1953125 to 1.1953125
- q_weight: bfloat16 [768, 768], P(('gx', 'gy')), may hold values from -0.21875 to 0.21875
- q_bias: bfloat16 [768], P(('gx', 'gy')), may hold values from -1.1953125 to 1.1953125
- k_weight: bfloat16 [768, 768], P(('gx', 'gy')), may hold values from -0.21875 to 0.21875
- v_weight: bfloat16 [768, 768], P(('gx', 'gy')), may hold values from -0.21875 to 0.21875
- v_bias: bfloat16 [768], P(('gx', 'gy')), may hold values from -1.1953125 to 1.1953125
- o_weight: bfloat16 [768, 768], P(('gx', 'gy')), may hold values from -3.5 to 3.5
- o_bias: bfloat16 [768], P(('gx', 'gy')), may hold values from -1.1953125 to 1.1953125
- ln2_gain: bfloat16 [768], P(('gx', 'gy')), may hold values from 0.5 to 1.5
- ln2_bias: bfloat16 [768], P(('gx', 'gy')), may hold values from -1.1953125 to 1.1953125
- up_weight: bfloat16 [768, 3072], P(('gx', 'gy')), may hold values from -0.21875 to 0.21875
- up_bias: bfloat16 [3072], P(('gx', 'gy')), may hold values from -1.1953125 to 1.1953125
- down_weight: bfloat16 [3072, 768], P(('gx', 'gy')), may hold values from -0.21875 to 0.21875
- down_bias: bfloat16 [768], P(('gx', 'gy')), may hold values from -1.1953125 to 1.1953125
- out_grad: bfloat16 [33856, 768], P(('gx', 'gy')), may hold values from -6 to 6
Outputs:
- block_out: bfloat16 [33856, 768], P(('gx', 'gy'))
- grad_tokens: float32 [33856, 768], P(('gx', 'gy'))
- grad_ln1_gain: float32 [768], P(('gx', 'gy'))
- grad_ln1_bias: float32 [768], P(('gx', 'gy'))
- grad_q_weight: float32 [768, 768], P(('gx', 'gy'))
- grad_q_bias: float32 [768], P(('gx', 'gy'))
- grad_k_weight: float32 [768, 768], P(('gx', 'gy'))
- grad_v_weight: float32 [768, 768], P(('gx', 'gy'))
- grad_v_bias: float32 [768], P(('gx', 'gy'))
- grad_o_weight: float32 [768, 768], P(('gx', 'gy'))
- grad_o_bias: float32 [768], P(('gx', 'gy'))
- grad_ln2_gain: float32 [768], P(('gx', 'gy'))
- grad_ln2_bias: float32 [768], P(('gx', 'gy'))
- grad_up_weight: float32 [768, 3072], P(('gx', 'gy'))
- grad_up_bias: float32 [3072], P(('gx', 'gy'))
- grad_down_weight: float32 [3072, 768], P(('gx', 'gy'))
- grad_down_bias: float32 [768], P(('gx', 'gy'))
The draws below stay inside these ranges and needn't reach their ends.
Inputs may be any that keep to these rules, and one draw needn't show every extreme that they name: `lengths`: most strips are nearly full, and strip 0 holds 529 filled slots.
All inputs are finite; a program needn't handle non-finite values. No bound on the sum of `key_mask` on one device may be relied on, other than what follows from the above.
Results may differ from the reference program's by a relative error of at most 0.012.
Values may be sent and summed in bfloat16 or wider, within the bound.
A program may use at most 192 MiB of HBM per device.

```python
import math
import jax
import jax.numpy as jnp
from jax import lax

D = 768
FF = 3072
HEAD_DIM = 64
SLOTS = 529
STRIPS = 64


def draw_lengths(key, part):
    first, second, third = jax.random.split(key, 3)
    lowest = min(40, SLOTS // 2)
    near_low = max(SLOTS - SLOTS // 10, lowest)
    choose = jax.random.randint(first, (STRIPS,), 0, 4)
    nearly = jax.random.randint(second, (STRIPS,), near_low, SLOTS + 1)
    spread = jax.random.randint(third, (STRIPS,), lowest, SLOTS + 1)
    drawn = jnp.where(choose > 0, nearly, spread)
    return drawn.at[0].set(SLOTS).astype(jnp.int32)


def plant(result, stream_key, smallest, high):
    extent = result.shape
    spot = [jax.random.randint(jax.random.fold_in(stream_key, axis), (), 0, extent[axis]) for axis in range(len(extent))]
    result = result.at[tuple(spot)].set(smallest)
    longest = extent.index(max(extent))
    spot[longest] = (spot[longest] + 1) % extent[longest]
    return result.at[tuple(spot)].set(high)


def with_spikes(array, own_key, source, target, shards_of, factor):
    owner, partner = [(jnp.arange(array.shape[axis_at]) // (array.shape[axis_at] // shards_of)).reshape([-1 if axis == axis_at else 1 for axis in range(array.ndim)]) for axis_at in (source, target)]
    chosen = jax.random.permutation(own_key, shards_of)[partner]
    strong = (owner == chosen) | (owner == (partner + shards_of // 2) % shards_of)
    return jnp.where(strong, factor * array, array)


def block_levels(stream_key, extent, cuts, smallest, top_value):
    def one(position, shards_of):
        heights = jax.random.uniform(jax.random.fold_in(jax.random.fold_in(stream_key, 6), position), (shards_of,), jnp.float32, smallest / len(cuts), top_value / len(cuts))
        return jnp.repeat(jnp.exp(heights), extent[position] // shards_of).reshape((-1,) + (1,) * (len(extent) - position - 1))

    gain = one(*cuts[0])
    for cut in cuts[1:]:
        gain = gain * one(*cut)
    return gain


def gaussian(stream_key, shape, scale, limit, cuts=(), kind=jnp.bfloat16):
    values = scale * jax.random.normal(stream_key, shape, jnp.float32)
    if cuts:
        values = values * block_levels(stream_key, shape, cuts, -0.22, 0.18)
    return jnp.clip(values, -limit, limit).astype(kind)


def noise_with(rng, shape, scale, most, shards, heavy, kind=jnp.bfloat16):
    entries = scale * jax.random.normal(rng, shape, jnp.float32)
    if shards:
        entries = entries * block_levels(rng, shape, shards, -0.22, 0.18)
    return jnp.clip(with_spikes(entries, jax.random.fold_in(rng, 3), *heavy), -most, most).astype(kind)


def setup_inputs(seed: int = 0) -> dict:
    keys = jax.random.split(jax.random.key(seed), 20)
    return {
        "tokens": noise_with(keys[0], (STRIPS * SLOTS, D), 1.0, 6.0, ((0, 32),), (0, 1, 32, 2.75)),
        "lengths": draw_lengths(jax.random.fold_in(keys[19], 71), 0),
        "key_mask": plant((jax.random.randint(keys[2], (STRIPS, SLOTS), 0, 8) < 7).astype(jnp.int32), jax.random.fold_in(keys[2], 1), 0, 1),
        "ln1_gain": jnp.clip(1.0 + 0.1 * jax.random.normal(keys[3], (D,), jnp.float32), 0.5, 1.5).astype(jnp.bfloat16),
        "ln1_bias": gaussian(keys[4], (D,), 0.2, 1.1953125, ((0, 32),)),
        "q_weight": gaussian(keys[5], (D, D), D ** -0.5, 0.21875, ((0, 32),)),
        "q_bias": gaussian(keys[6], (D,), 0.2, 1.1953125, ((0, 32),)),
        "k_weight": gaussian(keys[7], (D, D), D ** -0.5, 0.21875, ((0, 32),)),
        "v_weight": gaussian(keys[8], (D, D), D ** -0.5, 0.21875, ((0, 32),)),
        "v_bias": gaussian(keys[9], (D,), 0.2, 1.1953125, ((0, 32),)),
        "o_weight": gaussian(keys[10], (D, D), (D // 256) ** -0.5, 3.5, ((0, 32),)),
        "o_bias": gaussian(keys[11], (D,), 0.2, 1.1953125, ((0, 32),)),
        "ln2_gain": jnp.clip(1.0 + 0.1 * jax.random.normal(keys[12], (D,), jnp.float32), 0.5, 1.5).astype(jnp.bfloat16),
        "ln2_bias": gaussian(keys[13], (D,), 0.2, 1.1953125, ((0, 32),)),
        "up_weight": gaussian(keys[14], (D, FF), D ** -0.5, 0.21875, ((0, 32),)),
        "up_bias": gaussian(keys[15], (FF,), 0.2, 1.1953125, ((0, 32),)),
        "down_weight": gaussian(keys[16], (FF, D), (FF // 4) ** -0.5, 0.21875, ((0, 32),)),
        "down_bias": gaussian(keys[17], (D,), 0.2, 1.1953125, ((0, 32),)),
        "out_grad": gaussian(keys[18], (STRIPS * SLOTS, D), 1.0, 6.0, ((0, 32),)),
    }


@jax.custom_vjp
def low(v):
    return lax.optimization_barrier(v.astype(jnp.bfloat16)).astype(jnp.float32)

@jax.custom_vjp
def low_back(v):
    return v

def low_keep(v):
    return (low(v), None)

def low_pass(kept, grad):
    return (grad,)

def back_keep(v):
    return (v, None)

def back_low(kept, grad):
    return (low(grad),)
low.defvjp(low_keep, low_pass)
low_back.defvjp(back_keep, back_low)
EPSILON = 1e-06
NEG_FILL = -1e+30
PRECISE = lax.Precision.HIGHEST

def layer_norm(values, gain_vec, bias_vec):
    center = values - lax.optimization_barrier(jnp.mean(values, axis=-1, keepdims=True))
    spread = lax.optimization_barrier(jnp.mean(center * center, axis=-1, keepdims=True))
    return center * lax.rsqrt(spread + EPSILON) * gain_vec + bias_vec

def product(left_arg, right_arg):
    return jnp.dot(left_arg, right_arg, precision=PRECISE, preferred_element_type=jnp.float32)

def strip_forward(inputs, visible, params):
    ln1_gain, ln1_bias, q_weight, q_bias, k_weight, v_weight, v_bias, o_weight, o_bias, ln2_gain, ln2_bias, up_weight, up_bias, down_weight, down_bias = params
    head_count = D // HEAD_DIM
    score_scale = 1.0 / math.sqrt(HEAD_DIM)
    normed = low(layer_norm(inputs, ln1_gain, ln1_bias))
    queries = low(low_back(product(normed, q_weight) + q_bias)).reshape(SLOTS, head_count, HEAD_DIM)
    key_rows = low(low_back(product(normed, k_weight))).reshape(SLOTS, head_count, HEAD_DIM)
    value_rows = low(low_back(product(normed, v_weight) + v_bias)).reshape(SLOTS, head_count, HEAD_DIM)
    scores = low_back(jnp.einsum('qhd,khd->hqk', queries, key_rows, precision=PRECISE) * score_scale)
    scores = jnp.where(visible[None, None, :], scores, NEG_FILL)
    attn_probs = low(jax.nn.softmax(scores, axis=-1))
    context = jnp.einsum('hqk,khd->qhd', attn_probs, value_rows, precision=PRECISE).reshape(SLOTS, D)
    context = low(low_back(context))
    attended = low_back(product(context, o_weight) + o_bias)
    residual = inputs + attended
    normed2 = low(layer_norm(residual, ln2_gain, ln2_bias))
    hidden = low_back(product(normed2, up_weight) + up_bias)
    active = low(jax.nn.gelu(hidden, approximate=False))
    mlp_out = low_back(product(active, down_weight) + down_bias)
    return residual + mlp_out

def reference(tokens, lengths, key_mask, ln1_gain, ln1_bias, q_weight, q_bias, k_weight, v_weight, v_bias, o_weight, o_bias, ln2_gain, ln2_bias, up_weight, up_bias, down_weight, down_bias, out_grad):
    params = (ln1_gain.astype(jnp.float32), ln1_bias.astype(jnp.float32), q_weight.astype(jnp.float32), q_bias.astype(jnp.float32), k_weight.astype(jnp.float32), v_weight.astype(jnp.float32), v_bias.astype(jnp.float32), o_weight.astype(jnp.float32), o_bias.astype(jnp.float32), ln2_gain.astype(jnp.float32), ln2_bias.astype(jnp.float32), up_weight.astype(jnp.float32), up_bias.astype(jnp.float32), down_weight.astype(jnp.float32), down_bias.astype(jnp.float32))
    slot_ids = jnp.arange(SLOTS, dtype=jnp.int32)
    strips_in = tokens.astype(jnp.float32).reshape(STRIPS, SLOTS, D)
    grads_in = out_grad.astype(jnp.float32).reshape(STRIPS, SLOTS, D)

    def one_strip(totals, member):
        inputs, cotangent, length, mask_row = member
        visible = (slot_ids == 0) | (slot_ids < length) & (mask_row == 1)
        outputs, pull = jax.vjp(lambda values, weights: strip_forward(values, visible, weights), inputs, params)
        input_grad, weight_grads = pull(cotangent)
        totals = jax.tree.map(lambda running, added: running + added, totals, weight_grads)
        return (totals, (outputs.astype(jnp.bfloat16), input_grad))
    initial = tuple((jnp.zeros_like(weight_arg) for weight_arg in params))
    totals, (block_rows, grad_rows) = lax.scan(one_strip, initial, (strips_in, grads_in, lengths, key_mask))
    return (block_rows.reshape(STRIPS * SLOTS, D), grad_rows.reshape(STRIPS * SLOTS, D), totals[0], totals[1], totals[2], totals[3], totals[4], totals[5], totals[6], totals[7], totals[8], totals[9], totals[10], totals[11], totals[12], totals[13], totals[14])
```

```python
import functools
import math

import jax
import jax.numpy as jnp
from jax import lax
from jax.experimental import pallas as pl
from jax.experimental.pallas import tpu as pltpu
from jax.sharding import PartitionSpec as P

HEAD_DIM = 64


EPSILON = 1e-06
NEG_FILL = -1e30


def layer_norm(values, gain_vec, bias_vec):
    center = values - jnp.mean(values, axis=-1, keepdims=True)
    spread = jnp.mean(center * center, axis=-1, keepdims=True)
    return center * lax.rsqrt(spread + EPSILON) * gain_vec + bias_vec


def gelu_exact(values):
    return jax.nn.gelu(values, approximate=False)


def right_mul(left_arg, right_arg):
    return jnp.dot(left_arg, right_arg, preferred_element_type=jnp.float32)


def left_mul(left_arg, right_arg):
    return lax.dot_general(
        left_arg, right_arg, (((0,), (0,)), ((), ())), preferred_element_type=jnp.float32
    )


def back_mul(left_arg, right_arg):
    return lax.dot_general(
        left_arg, right_arg, (((1,), (1,)), ((), ())), preferred_element_type=jnp.float32
    )


MESH = pl.DeviceIdType.MESH


def grid_of(mesh):
    z_size, plane = mesh.shape["gx"], mesh.shape["gy"] // 2
    x_size = max(n for n in range(1, plane + 1) if plane % n == 0 and n * n <= plane)
    return z_size, plane // x_size, x_size


class Place:
    def __init__(self, dims):
        self.dims = dims
        g = lax.axis_index("gy")
        self.z = lax.axis_index("gx")
        self.c = lax.rem(g, 2)
        self.x = lax.rem(lax.div(g, 2), dims[2])
        self.y = lax.div(g, 2 * dims[2])

    def at(self, axis, step):
        here = (self.z, self.y, self.x)[axis]
        return lax.rem(here + step, self.dims[axis])

    def device(self, axis, step):
        where = [self.z, self.y, self.x, self.c]
        if axis == 3:
            where[3] = 1 - self.c
        else:
            where[axis] = self.at(axis, step)
        return (where[0], (where[1] * self.dims[2] + where[2]) * 2 + where[3])

    def peers(self):
        for axis in range(3):
            for step in range(1, self.dims[axis]):
                yield axis, step
        yield 3, 1

    def barrier(self):
        sem = pltpu.get_barrier_semaphore()
        count = 0
        for axis, step in self.peers():
            pl.semaphore_signal(sem, inc=1, device_id=self.device(axis, step), device_id_type=MESH)
            count += 1
        pl.semaphore_wait(sem, count)


class Lanes:
    def __init__(self, place, send, recv):
        self.place, self.send, self.recv, self.used = place, send, recv, 0
        self.all = []

    def remote(self, src, dst, axis, step):
        n = self.used
        self.used += 1
        copy = pltpu.make_async_remote_copy(
            src_ref=src, dst_ref=dst, send_sem=self.send.at[n], recv_sem=self.recv.at[n],
            device_id=self.place.device(axis, step), device_id_type=MESH,
        )
        self.all.append(copy)
        return copy


def gather_copies(dims):
    z, y, x = dims
    return (z - 1) + 3 * (max(x, y) - 1) + 3 * (max(x, y) - 1) + 1


class Gather:
    def __init__(self, lanes, shard, buf, first, local_sem):
        p, dims = lanes.place, lanes.place.dims
        second = 3 - first
        own = buf.at[p.z, p.y, p.x, p.c]
        self.local = pltpu.make_async_copy(shard, own, local_sem)
        self.along_z = [lanes.remote(shard, own, 0, s) for s in range(1, dims[0])]

        def column(step):
            where = [p.y, p.x]
            where[first - 1] = p.at(first, step)
            return buf.at[:, where[0], where[1], p.c]

        def sheet(step):
            if second == 1:
                return buf.at[:, p.at(1, step), :, p.c]
            return buf.at[:, :, p.at(2, step), p.c]

        self.along_first = [lanes.remote(column(0), column(0), first, s) for s in range(1, dims[first])]
        self.core_one = [lanes.remote(column(0), column(0), 3, 1)]
        self.along_second = [lanes.remote(sheet(0), sheet(0), second, s) for s in range(1, dims[second])]
        self.core_two = [lanes.remote(column(s), column(s), 3, 1) for s in range(1, dims[first])]
        self.core_three = [lanes.remote(sheet(s), sheet(s), 3, 1) for s in range(1, dims[second])]

    def start(self):
        for copy in self.along_z:
            copy.start()
        self.local.start()

    def plane_first(self):
        self.local.wait()
        for copy in self.along_z:
            copy.wait_recv()
        for copy in self.along_first + self.core_one:
            copy.start()

    def plane_second(self):
        for copy in self.along_first:
            copy.wait_recv()
        for copy in self.along_second + self.core_two:
            copy.start()

    def other_core(self):
        for copy in self.along_second:
            copy.wait_recv()
        for copy in self.core_three:
            copy.start()

    def arrived(self):
        for copy in self.core_one + self.core_two + self.core_three:
            copy.wait_recv()

    def drain(self):
        for copy in self.along_z + self.along_first + self.core_one + self.along_second + self.core_two + self.core_three:
            copy.wait_send()


def scatter_copies(dims):
    z, y, x = dims
    return 1 + (z - 1) + (y - 1) + (x - 1)


def scatter_scratch(dims, shape, dtype, first):
    z, y, x = dims
    n_first, n_second = (y, x) if first == 1 else (x, y)
    return [
        pltpu.VMEM((z, y, x) + shape, dtype),
        pltpu.VMEM((z, y, x) + shape, dtype),
        pltpu.VMEM((max(n_first - 1, 1), z, n_second) + shape, dtype),
        pltpu.VMEM((max(n_second - 1, 1), z) + shape, dtype),
        pltpu.VMEM((max(z - 1, 1),) + shape, dtype),
    ]


class Scatter:
    def __init__(self, lanes, grads, out, bufs, first, local_sem):
        p, dims = lanes.place, lanes.place.dims
        self.p, self.dims, self.first, self.second = p, dims, first, 3 - first
        self.out = out
        self.mine, self.from_core, self.from_first, self.from_second, self.from_z = bufs
        mine = self.mine
        self.local = pltpu.make_async_copy(grads.at[:, :, :, p.c], mine, local_sem)
        self.over_core = lanes.remote(grads.at[:, :, :, 1 - p.c], self.from_core, 3, 1)

        def sheet(step):
            if first == 1:
                return mine.at[:, p.at(1, step)]
            return mine.at[:, :, p.at(2, step)]

        def column(step):
            where = [p.y, p.x]
            where[self.second - 1] = p.at(self.second, step)
            return mine.at[:, where[0], where[1]]

        self.over_first = [lanes.remote(sheet(s), self.from_first.at[s - 1], first, s) for s in range(1, dims[first])]
        self.over_second = [
            lanes.remote(column(s), self.from_second.at[s - 1], self.second, s) for s in range(1, dims[self.second])
        ]
        self.over_z = [
            lanes.remote(mine.at[p.at(0, s), p.y, p.x], self.from_z.at[s - 1], 0, s) for s in range(1, dims[0])
        ]

    def start(self):
        self.over_core.start()
        self.local.start()

    def add_core(self):
        self.local.wait()
        self.over_core.wait_recv()
        z, y, x = self.dims

        def body(n, carry):
            at = (lax.div(n, y * x), lax.rem(lax.div(n, x), y), lax.rem(n, x))
            both = self.mine[at].astype(jnp.float32) + self.from_core[at].astype(jnp.float32)
            self.mine[at] = both.astype(self.mine.dtype)
            return carry

        lax.fori_loop(0, z * y * x, body, 0)

    def send_first(self):
        for copy in self.over_first:
            copy.start()

    def add_first(self):
        for copy in self.over_first:
            copy.wait_recv()
        z, wide = self.dims[0], self.dims[self.second]

        def body(n, carry):
            row, other = lax.div(n, wide), lax.rem(n, wide)
            at = (row, self.p.y, other) if self.first == 1 else (row, other, self.p.x)
            total = self.mine[at].astype(jnp.float32)
            for s in range(len(self.over_first)):
                total = total + self.from_first[s, row, other].astype(jnp.float32)
            self.mine[at] = total.astype(self.mine.dtype)
            return carry

        lax.fori_loop(0, z * wide, body, 0)

    def send_second(self):
        for copy in self.over_second:
            copy.start()

    def add_second(self):
        for copy in self.over_second:
            copy.wait_recv()

        def body(row, carry):
            at = (row, self.p.y, self.p.x)
            total = self.mine[at].astype(jnp.float32)
            for s in range(len(self.over_second)):
                total = total + self.from_second[s, row].astype(jnp.float32)
            self.mine[at] = total.astype(self.mine.dtype)
            return carry

        lax.fori_loop(0, self.dims[0], body, 0)

    def send_z(self):
        for copy in self.over_z:
            copy.start()

    def finish(self):
        for copy in self.over_z:
            copy.wait_recv()
        total = self.mine[self.p.z, self.p.y, self.p.x].astype(jnp.float32)
        for s in range(len(self.over_z)):
            total = total + self.from_z[s].astype(jnp.float32)
        self.out[...] = total
        for copy in [self.over_core] + self.over_first + self.over_second + self.over_z:
            copy.wait_send()

VMEM_LIMIT = 60 * 1024 * 1024


def gather_kernel(dims, count, *refs):
    shards, bufs, (local, send, recv) = refs[:count], refs[count : 2 * count], refs[2 * count :]
    place = Place(dims)
    place.barrier()
    lanes = Lanes(place, send, recv)
    jobs = [Gather(lanes, shards[n], bufs[n], 2 - n % 2, local.at[n]) for n in range(count)]
    for stage in ("start", "plane_first", "plane_second", "other_core", "arrived", "drain"):
        for job in jobs:
            getattr(job, stage)()


def gather_all(dims, arrays):
    count = len(arrays)
    copies = gather_copies(dims) * count
    return pl.pallas_call(
        functools.partial(gather_kernel, dims, count),
        out_shape=[jax.ShapeDtypeStruct(dims + (2,) + a.shape, a.dtype) for a in arrays],
        in_specs=[pl.BlockSpec(memory_space=pltpu.VMEM)] * count,
        out_specs=[pl.BlockSpec(memory_space=pl.ANY)] * count,
        scratch_shapes=[
            pltpu.SemaphoreType.DMA((count,)),
            pltpu.SemaphoreType.DMA((copies,)),
            pltpu.SemaphoreType.DMA((copies,)),
        ],
        compiler_params=pltpu.CompilerParams(collective_id=0, has_side_effects=True, vmem_limit_bytes=VMEM_LIMIT),
        name="gather",
    )(*arrays)


def scatter_kernel(dims, count, *refs):
    grads, outs, scratch = refs[:count], refs[count : 2 * count], refs[2 * count :]
    local, send, recv = scratch[-3:]
    place = Place(dims)
    place.barrier()
    lanes = Lanes(place, send, recv)
    jobs = [
        Scatter(lanes, grads[n], outs[n], scratch[5 * n : 5 * n + 5], 1 + n % 2, local.at[n]) for n in range(count)
    ]
    for job in jobs:
        job.start()
    for add, ship in (("add_core", "send_first"), ("add_first", "send_second"), ("add_second", "send_z")):
        for n, job in enumerate(jobs):
            getattr(job, add)()
            if n:
                getattr(jobs[n - 1], ship)()
        getattr(jobs[-1], ship)()
    for job in jobs:
        job.finish()


def scatter_all(dims, arrays):
    count = len(arrays)
    copies = scatter_copies(dims) * count
    scratch = []
    for n, a in enumerate(arrays):
        scratch += scatter_scratch(dims, a.shape[4:], a.dtype, 1 + n % 2)
    return pl.pallas_call(
        functools.partial(scatter_kernel, dims, count),
        out_shape=[jax.ShapeDtypeStruct(a.shape[4:], jnp.float32) for a in arrays],
        in_specs=[pl.BlockSpec(memory_space=pl.ANY)] * count,
        out_specs=[pl.BlockSpec(memory_space=pltpu.VMEM)] * count,
        scratch_shapes=scratch
        + [
            pltpu.SemaphoreType.DMA((count,)),
            pltpu.SemaphoreType.DMA((copies,)),
            pltpu.SemaphoreType.DMA((copies,)),
        ],
        compiler_params=pltpu.CompilerParams(collective_id=1, has_side_effects=True, vmem_limit_bytes=VMEM_LIMIT),
        name="scatter",
    )(*arrays)


def lane_pad(rows, width):
    return jnp.pad(rows, ((0, 0), (0, width - rows.shape[1])))


def pack_vectors(vectors, wide):
    width = 128 * -(-wide.shape[0] // 128)
    rows = lane_pad(jnp.stack(vectors).astype(jnp.float32), width)
    last = lane_pad(wide[None].astype(jnp.float32), width)
    return jnp.pad(jnp.concatenate([rows, last]), ((0, 15 - len(vectors)), (0, 0)))


def unpack_vectors(block, part, wide_part):
    flat = block.reshape((-1,) + block.shape[-2:])
    rows = flat[:, :8, :part].transpose(1, 0, 2).reshape(8, -1)
    return rows, flat[:, 8, :wide_part].reshape(-1)


def pack_vector_grads(dims, vectors, wide):
    n = 2 * dims[0] * dims[1] * dims[2]
    part, wide_part = vectors[0].shape[0] // n, wide.shape[0] // n
    width = 128 * -(-wide_part // 128)
    rows = jnp.stack(vectors).reshape(8, n, part).transpose(1, 0, 2)
    rows = jnp.pad(rows, ((0, 0), (0, 0), (0, width - part)))
    last = jnp.pad(wide.reshape(n, 1, wide_part), ((0, 0), (0, 0), (0, width - wide_part)))
    block = jnp.pad(jnp.concatenate([rows, last], axis=1), ((0, 0), (0, 7), (0, 0)))
    return block.reshape(dims + (2,) + block.shape[1:])


def shards(
    dims,
    tokens,
    lengths,
    key_mask,
    ln1_gain,
    ln1_bias,
    q_weight,
    q_bias,
    k_weight,
    v_weight,
    v_bias,
    o_weight,
    o_bias,
    ln2_gain,
    ln2_bias,
    up_weight,
    up_bias,
    down_weight,
    down_bias,
    out_grad,
):
    weights = (q_weight, k_weight, v_weight, o_weight, up_weight, down_weight)
    vectors = (ln1_gain, ln1_bias, q_bias, v_bias, o_bias, ln2_gain, ln2_bias, down_bias)
    *wide, packed = gather_all(dims, list(weights) + [pack_vectors(vectors, up_bias)])
    q_full, k_full, v_full, o_full, up_full, down_full = [w.reshape((-1,) + w.shape[-1:]) for w in wide]
    rows, up_bias_full = unpack_vectors(packed, ln1_gain.shape[0], up_bias.shape[0])
    gathered = (
        rows[0], rows[1], q_full, rows[2], k_full, v_full, rows[3], o_full, rows[4], rows[5], rows[6],
        up_full, up_bias_full, down_full, rows[7],
    )
    regathered = gathered
    row_count = tokens.shape[0]
    feature_count = tokens.shape[1]
    strip_count = lengths.shape[0]
    slot_count = row_count // strip_count
    head_count = feature_count // HEAD_DIM
    score_scale = 1.0 / math.sqrt(HEAD_DIM)
    slot_ids = lax.iota(jnp.int32, slot_count)
    visible = (slot_ids[None, :] == 0) | (slot_ids[None, :] < lengths[:, None]) & (key_mask == 1)

    def split_heads(values):
        return values.reshape(strip_count, slot_count, head_count, HEAD_DIM)

    gain_one = gathered[0].astype(jnp.float32)
    bias_one = gathered[1].astype(jnp.float32)
    gain_two = gathered[9].astype(jnp.float32)
    bias_two = gathered[10].astype(jnp.float32)
    inputs = tokens.astype(jnp.float32)
    normed = layer_norm(inputs, gain_one, bias_one).astype(jnp.bfloat16)
    queries = (right_mul(normed, gathered[2]) + gathered[3].astype(jnp.float32)).astype(
        jnp.bfloat16
    )
    key_rows = right_mul(normed, gathered[4]).astype(jnp.bfloat16)
    value_rows = (right_mul(normed, gathered[5]) + gathered[6].astype(jnp.float32)).astype(
        jnp.bfloat16
    )

    def attend(pieces):
        queries_in, keys_in, values_in, visible_in = pieces
        scores = (
            jnp.einsum("qhd,khd->hqk", queries_in, keys_in, preferred_element_type=jnp.float32)
            * score_scale
        )
        scores = jnp.where(visible_in[None, None, :], scores, NEG_FILL)
        row_max = jnp.max(scores, axis=-1, keepdims=True)
        powers = jnp.exp(scores - row_max)
        row_sum = jnp.sum(powers, axis=-1, keepdims=True)
        attn_low = (powers / row_sum).astype(jnp.bfloat16)
        context = jnp.einsum(
            "hqk,khd->qhd", attn_low, values_in, preferred_element_type=jnp.float32
        )
        return (context, row_max + jnp.log(row_sum))

    context, log_sums = lax.map(
        attend, (split_heads(queries), split_heads(key_rows), split_heads(value_rows), visible)
    )
    context = context.reshape(row_count, feature_count).astype(jnp.bfloat16)
    residual = inputs + right_mul(context, gathered[7]) + gathered[8].astype(jnp.float32)
    normed2 = layer_norm(residual, gain_two, bias_two).astype(jnp.bfloat16)
    hidden = right_mul(normed2, gathered[11]) + gathered[12].astype(jnp.float32)
    active = gelu_exact(hidden).astype(jnp.bfloat16)
    mlp_out = right_mul(active, gathered[13]) + gathered[14].astype(jnp.float32)
    block_out = (residual + mlp_out).astype(jnp.bfloat16)
    cotangent = out_grad.astype(jnp.float32)
    grad_wdown = left_mul(active, out_grad)
    grad_bdown = jnp.sum(cotangent, axis=0)
    grad_active = back_mul(out_grad, regathered[13])
    _, gelu_pull = jax.vjp(gelu_exact, hidden)
    grad_hidden = gelu_pull(grad_active)[0].astype(jnp.bfloat16)
    grad_wup = left_mul(normed2, grad_hidden)
    grad_bup = jnp.sum(grad_hidden.astype(jnp.float32), axis=0)
    grad_normed2 = back_mul(grad_hidden, regathered[11])
    _, second_pull = jax.vjp(layer_norm, residual, gain_two, bias_two)
    grad_res, grad_g2, grad_b2 = second_pull(grad_normed2)
    grad_res = cotangent + grad_res
    grad_att = grad_res.astype(jnp.bfloat16)
    grad_wo = left_mul(context, grad_att)
    grad_bo = jnp.sum(grad_att.astype(jnp.float32), axis=0)
    grad_context = back_mul(grad_att, regathered[7]).astype(jnp.bfloat16)

    def attend_back(pieces):
        queries_in, keys_in, values_in, visible_in, lse_in, grad_in = pieces
        scores = (
            jnp.einsum("qhd,khd->hqk", queries_in, keys_in, preferred_element_type=jnp.float32)
            * score_scale
        )
        scores = jnp.where(visible_in[None, None, :], scores, NEG_FILL)
        attn_probs = jnp.exp(scores - lse_in)
        attn_low = attn_probs.astype(jnp.bfloat16)
        grad_values = jnp.einsum(
            "hqk,qhd->khd", attn_low, grad_in, preferred_element_type=jnp.float32
        )
        grad_probs = jnp.einsum(
            "qhd,khd->hqk", grad_in, values_in, preferred_element_type=jnp.float32
        )
        row_inner = jnp.sum(attn_probs * grad_probs, axis=-1, keepdims=True)
        grad_scores = (attn_probs * (grad_probs - row_inner)).astype(jnp.bfloat16)
        grad_queries = (
            jnp.einsum("hqk,khd->qhd", grad_scores, keys_in, preferred_element_type=jnp.float32)
            * score_scale
        )
        grad_keys = (
            jnp.einsum("hqk,qhd->khd", grad_scores, queries_in, preferred_element_type=jnp.float32)
            * score_scale
        )
        return (
            grad_queries.astype(jnp.bfloat16),
            grad_keys.astype(jnp.bfloat16),
            grad_values.astype(jnp.bfloat16),
        )

    grad_queries, grad_keys, grad_values = lax.map(
        attend_back,
        (
            split_heads(queries),
            split_heads(key_rows),
            split_heads(value_rows),
            visible,
            log_sums,
            split_heads(grad_context),
        ),
    )
    grad_queries = grad_queries.reshape(row_count, feature_count)
    grad_keys = grad_keys.reshape(row_count, feature_count)
    grad_values = grad_values.reshape(row_count, feature_count)
    grad_wq = left_mul(normed, grad_queries)
    grad_wk = left_mul(normed, grad_keys)
    grad_wv = left_mul(normed, grad_values)
    grad_bq = jnp.sum(grad_queries.astype(jnp.float32), axis=0)
    grad_bv = jnp.sum(grad_values.astype(jnp.float32), axis=0)
    grad_normed = (
        back_mul(grad_queries, regathered[2])
        + back_mul(grad_keys, regathered[4])
        + back_mul(grad_values, regathered[5])
    )
    _, first_pull = jax.vjp(layer_norm, inputs, gain_one, bias_one)
    grad_inputs, grad_g1, grad_b1 = first_pull(grad_normed)
    grad_tokens = grad_res + grad_inputs

    def blocks(grad, like):
        return grad.astype(jnp.bfloat16).reshape(dims + (2,) + like.shape)

    vector_grads = pack_vector_grads(
        dims, (grad_g1, grad_b1, grad_bq, grad_bv, grad_bo, grad_g2, grad_b2, grad_bdown), grad_bup
    )
    full = (grad_wq, grad_wk, grad_wv, grad_wo, grad_wup, grad_wdown)
    *sums, small = scatter_all(dims, [blocks(g, w) for g, w in zip(full, weights)] + [vector_grads])
    sum_wq, sum_wk, sum_wv, sum_wo, sum_wup, sum_wdown = sums
    vec = [small[n, : ln1_gain.shape[0]] for n in range(8)]
    return (
        block_out, grad_tokens, vec[0], vec[1], sum_wq, vec[2], sum_wk, sum_wv, vec[3], sum_wo, vec[4], vec[5], vec[6],
        sum_wup, small[8, : up_bias.shape[0]], sum_wdown, vec[7],
    )


def solution(mesh):
    dims = grid_of(mesh)
    return jax.shard_map(
        functools.partial(shards, dims),
        mesh=mesh,
        in_specs=(
            P(("gx", "gy"), None),
            P(("gx", "gy")),
            P(("gx", "gy"), None),
            P(("gx", "gy")),
            P(("gx", "gy")),
            P(("gx", "gy"), None),
            P(("gx", "gy")),
            P(("gx", "gy"), None),
            P(("gx", "gy"), None),
            P(("gx", "gy")),
            P(("gx", "gy"), None),
            P(("gx", "gy")),
            P(("gx", "gy")),
            P(("gx", "gy")),
            P(("gx", "gy"), None),
            P(("gx", "gy")),
            P(("gx", "gy"), None),
            P(("gx", "gy")),
            P(("gx", "gy"), None),
        ),
        out_specs=(
            P(("gx", "gy"), None),
            P(("gx", "gy"), None),
            P(("gx", "gy")),
            P(("gx", "gy")),
            P(("gx", "gy"), None),
            P(("gx", "gy")),
            P(("gx", "gy"), None),
            P(("gx", "gy"), None),
            P(("gx", "gy")),
            P(("gx", "gy"), None),
            P(("gx", "gy")),
            P(("gx", "gy")),
            P(("gx", "gy")),
            P(("gx", "gy"), None),
            P(("gx", "gy")),
            P(("gx", "gy"), None),
            P(("gx", "gy")),
        ),
        check_vma=False,
    )
```

```python
import functools
import math

import jax
import jax.numpy as jnp
from jax import lax
from jax.experimental import pallas as pl
from jax.experimental.pallas import tpu as pltpu
from jax.sharding import PartitionSpec as P

HEAD_DIM = 64
EPSILON = 1e-06
NEG_FILL = -1e30
VMEM_LIMIT = 63 * 1024 * 1024


def right_mul(left_arg, right_arg):
    return jnp.dot(left_arg, right_arg, preferred_element_type=jnp.float32)


def left_mul(left_arg, right_arg):
    return lax.dot_general(
        left_arg, right_arg, (((0,), (0,)), ((), ())), preferred_element_type=jnp.float32
    )


def back_mul(left_arg, right_arg):
    return lax.dot_general(
        left_arg, right_arg, (((1,), (1,)), ((), ())), preferred_element_type=jnp.float32
    )


MESH = pl.DeviceIdType.MESH


def grid_of(mesh):
    z_size, plane = mesh.shape["gx"], mesh.shape["gy"] // 2
    x_size = max(n for n in range(1, plane + 1) if plane % n == 0 and n * n <= plane)
    return z_size, plane // x_size, x_size


class Place:
    def __init__(self, dims):
        self.dims = dims
        g = lax.axis_index("gy")
        self.z = lax.axis_index("gx")
        self.c = lax.rem(g, 2)
        self.x = lax.rem(lax.div(g, 2), dims[2])
        self.y = lax.div(g, 2 * dims[2])

    def at(self, axis, step):
        here = (self.z, self.y, self.x)[axis]
        return lax.rem(here + step, self.dims[axis])

    def device(self, axis, step):
        where = [self.z, self.y, self.x, self.c]
        if axis == 3:
            where[3] = 1 - self.c
        else:
            where[axis] = self.at(axis, step)
        return (where[0], (where[1] * self.dims[2] + where[2]) * 2 + where[3])

    def peers(self):
        for axis in range(3):
            for step in range(1, self.dims[axis]):
                yield axis, step
        yield 3, 1

    def barrier(self):
        sem = pltpu.get_barrier_semaphore()
        count = 0
        for axis, step in self.peers():
            pl.semaphore_signal(sem, inc=1, device_id=self.device(axis, step), device_id_type=MESH)
            count += 1
        pl.semaphore_wait(sem, count)


class Lanes:
    def __init__(self, place, send, recv):
        self.place, self.send, self.recv, self.used = place, send, recv, 0
        self.all = []

    def remote(self, src, dst, axis, step):
        n = self.used
        self.used += 1
        copy = pltpu.make_async_remote_copy(
            src_ref=src, dst_ref=dst, send_sem=self.send.at[n], recv_sem=self.recv.at[n],
            device_id=self.place.device(axis, step), device_id_type=MESH,
        )
        self.all.append(copy)
        return copy


def gather_copies(dims):
    z, y, x = dims
    return (z - 1) + 3 * (max(x, y) - 1) + 3 * (max(x, y) - 1) + 1


class Gather:
    def __init__(self, lanes, shard, buf, first, local_sem):
        p, dims = lanes.place, lanes.place.dims
        second = 3 - first
        own = buf.at[p.z, p.y, p.x, p.c]
        self.local = pltpu.make_async_copy(shard, own, local_sem)
        self.along_z = [lanes.remote(shard, own, 0, s) for s in range(1, dims[0])]

        def column(step):
            where = [p.y, p.x]
            where[first - 1] = p.at(first, step)
            return buf.at[:, where[0], where[1], p.c]

        def sheet(step):
            if second == 1:
                return buf.at[:, p.at(1, step), :, p.c]
            return buf.at[:, :, p.at(2, step), p.c]

        self.along_first = [lanes.remote(column(0), column(0), first, s) for s in range(1, dims[first])]
        self.core_one = [lanes.remote(column(0), column(0), 3, 1)]
        self.along_second = [lanes.remote(sheet(0), sheet(0), second, s) for s in range(1, dims[second])]
        self.core_two = [lanes.remote(column(s), column(s), 3, 1) for s in range(1, dims[first])]
        self.core_three = [lanes.remote(sheet(s), sheet(s), 3, 1) for s in range(1, dims[second])]

    def start(self):
        for copy in self.along_z:
            copy.start()
        self.local.start()

    def plane_first(self):
        self.local.wait()
        for copy in self.along_z:
            copy.wait_recv()
        for copy in self.along_first + self.core_one:
            copy.start()

    def plane_second(self):
        for copy in self.along_first:
            copy.wait_recv()
        for copy in self.along_second + self.core_two:
            copy.start()

    def other_core(self):
        for copy in self.along_second:
            copy.wait_recv()
        for copy in self.core_three:
            copy.start()

    def arrived(self):
        for copy in self.core_one + self.core_two + self.core_three:
            copy.wait_recv()

    def drain(self):
        for copy in self.along_z + self.along_first + self.core_one + self.along_second + self.core_two + self.core_three:
            copy.wait_send()


def scatter_copies(dims):
    z, y, x = dims
    return 1 + (z - 1) + (y - 1) + (x - 1)


def scatter_scratch(dims, shape, dtype, first):
    z, y, x = dims
    n_first, n_second = (y, x) if first == 1 else (x, y)
    return [
        pltpu.VMEM((z, y, x) + shape, dtype),
        pltpu.VMEM((z, y, x) + shape, dtype),
        pltpu.VMEM((max(n_first - 1, 1), z, n_second) + shape, dtype),
        pltpu.VMEM((max(n_second - 1, 1), z) + shape, dtype),
        pltpu.VMEM((max(z - 1, 1),) + shape, dtype),
    ]


class Scatter:
    def __init__(self, lanes, grads, out, bufs, first, local_sem):
        p, dims = lanes.place, lanes.place.dims
        self.p, self.dims, self.first, self.second = p, dims, first, 3 - first
        self.out = out
        self.mine, self.from_core, self.from_first, self.from_second, self.from_z = bufs
        mine = self.mine
        self.local = pltpu.make_async_copy(grads.at[:, :, :, p.c], mine, local_sem)
        self.over_core = lanes.remote(grads.at[:, :, :, 1 - p.c], self.from_core, 3, 1)

        def sheet(step):
            if first == 1:
                return mine.at[:, p.at(1, step)]
            return mine.at[:, :, p.at(2, step)]

        def column(step):
            where = [p.y, p.x]
            where[self.second - 1] = p.at(self.second, step)
            return mine.at[:, where[0], where[1]]

        self.over_first = [lanes.remote(sheet(s), self.from_first.at[s - 1], first, s) for s in range(1, dims[first])]
        self.over_second = [
            lanes.remote(column(s), self.from_second.at[s - 1], self.second, s) for s in range(1, dims[self.second])
        ]
        self.over_z = [
            lanes.remote(mine.at[p.at(0, s), p.y, p.x], self.from_z.at[s - 1], 0, s) for s in range(1, dims[0])
        ]

    def start(self):
        self.over_core.start()
        self.local.start()

    def add_core(self):
        self.local.wait()
        self.over_core.wait_recv()
        z, y, x = self.dims

        def body(n, carry):
            at = (lax.div(n, y * x), lax.rem(lax.div(n, x), y), lax.rem(n, x))
            both = self.mine[at].astype(jnp.float32) + self.from_core[at].astype(jnp.float32)
            self.mine[at] = both.astype(self.mine.dtype)
            return carry

        lax.fori_loop(0, z * y * x, body, 0)

    def send_first(self):
        for copy in self.over_first:
            copy.start()

    def add_first(self):
        for copy in self.over_first:
            copy.wait_recv()
        z, wide = self.dims[0], self.dims[self.second]

        def body(n, carry):
            row, other = lax.div(n, wide), lax.rem(n, wide)
            at = (row, self.p.y, other) if self.first == 1 else (row, other, self.p.x)
            total = self.mine[at].astype(jnp.float32)
            for s in range(len(self.over_first)):
                total = total + self.from_first[s, row, other].astype(jnp.float32)
            self.mine[at] = total.astype(self.mine.dtype)
            return carry

        lax.fori_loop(0, z * wide, body, 0)

    def send_second(self):
        for copy in self.over_second:
            copy.start()

    def add_second(self):
        for copy in self.over_second:
            copy.wait_recv()

        def body(row, carry):
            at = (row, self.p.y, self.p.x)
            total = self.mine[at].astype(jnp.float32)
            for s in range(len(self.over_second)):
                total = total + self.from_second[s, row].astype(jnp.float32)
            self.mine[at] = total.astype(self.mine.dtype)
            return carry

        lax.fori_loop(0, self.dims[0], body, 0)

    def send_z(self):
        for copy in self.over_z:
            copy.start()

    def finish(self):
        for copy in self.over_z:
            copy.wait_recv()
        total = self.mine[self.p.z, self.p.y, self.p.x].astype(jnp.float32)
        for s in range(len(self.over_z)):
            total = total + self.from_z[s].astype(jnp.float32)
        self.out[...] = total
        for copy in [self.over_core] + self.over_first + self.over_second + self.over_z:
            copy.wait_send()


def layer_norm_parts(values):
    center = values - jnp.mean(values, axis=-1, keepdims=True)
    scale = lax.rsqrt(jnp.mean(center * center, axis=-1, keepdims=True) + EPSILON)
    return center * scale, scale


def layer_norm_back(grad, xhat, scale, gain):
    scaled = grad * gain
    inner = scaled - jnp.mean(scaled, axis=-1, keepdims=True)
    back = scale * (inner - xhat * jnp.mean(scaled * xhat, axis=-1, keepdims=True))
    return back, jnp.sum(grad * xhat, axis=0, keepdims=True), jnp.sum(grad, axis=0, keepdims=True)


def gelu_and_slope(v):
    size = jnp.abs(v)
    t = 1.0 / (1.0 + (0.3275911 * math.sqrt(0.5)) * size)
    bell = jnp.exp(-0.5 * v * v)
    poly = ((((0.5 * 1.061405429) * t - 0.5 * 1.453152027) * t + 0.5 * 1.421413741) * t - 0.5 * 0.284496736) * t
    tail = (poly + 0.5 * 0.254829592) * t * bell
    share = jnp.where(v >= 0, 1.0 - tail, tail)
    return v * share, share + (v * (1.0 / math.sqrt(2.0 * math.pi))) * bell


def ffn_kernel(
    a_rows, b_rows, ff_tile, c_rows, tile,
    tokens, context, out_grad, o_weight, up_weight, down_weight, vectors, up_bias,
    block_out, grad_res, grad_context, grad_wo, grad_wup, grad_wdown, small, grad_bup,
    normed2, active, grad_hidden, grad_att, normed2_t,
):
    rows, width = tokens.shape
    ff = up_weight.shape[1]
    o_bias, gain, bias, down_bias = vectors[4:5, :], vectors[5:6, :], vectors[6:7, :], vectors[7:8, :]
    small[...] = jnp.zeros_like(small)

    def attended(n, carry):
        at = pl.ds(pl.multiple_of(n * a_rows, a_rows), a_rows)
        residual = tokens[at, :].astype(jnp.float32) + right_mul(context[at, :], o_weight[...]) + o_bias
        grad_res[at, :] = residual
        xhat, _ = layer_norm_parts(residual)
        normed2[at, :] = (xhat * gain + bias).astype(jnp.bfloat16)
        return carry

    lax.fori_loop(0, rows // a_rows, attended, 0)

    def hidden_tile(n, carry):
        cols = pl.ds(pl.multiple_of(n * ff_tile, ff_tile), ff_tile)
        sums = jnp.zeros((1, ff_tile), jnp.float32)

        def piece(m, sums):
            at = pl.ds(pl.multiple_of(m * b_rows, b_rows), b_rows)
            hidden = right_mul(normed2[at, :], up_weight[:, cols]) + up_bias[:, cols]
            grad_active = back_mul(out_grad[at, :], down_weight[cols, :])
            value, slope = gelu_and_slope(hidden)
            active[at, cols] = value.astype(jnp.bfloat16)
            back = (slope * grad_active).astype(jnp.bfloat16)
            grad_hidden[at, cols] = back
            return sums + jnp.sum(back.astype(jnp.float32), axis=0, keepdims=True)

        grad_bup[:, cols] = lax.fori_loop(0, rows // b_rows, piece, sums)
        return carry

    lax.fori_loop(0, ff // ff_tile, hidden_tile, 0)

    def finish(n, carry):
        at = pl.ds(pl.multiple_of(n * c_rows, c_rows), c_rows)
        residual = grad_res[at, :]
        cotangent = out_grad[at, :].astype(jnp.float32)
        block_out[at, :] = (residual + right_mul(active[at, :], down_weight[...]) + down_bias).astype(jnp.bfloat16)
        grad = back_mul(grad_hidden[at, :], up_weight[...])
        xhat, scale = layer_norm_parts(residual)
        back, gain_sum, bias_sum = layer_norm_back(grad, xhat, scale, gain)
        total = cotangent + back
        grad_res[at, :] = total
        low = total.astype(jnp.bfloat16)
        grad_att[at, :] = low
        grad_context[at, :] = back_mul(low, o_weight[...]).astype(jnp.bfloat16)
        small[4:5, :] += jnp.sum(low.astype(jnp.float32), axis=0, keepdims=True)
        small[5:6, :] += gain_sum
        small[6:7, :] += bias_sum
        small[7:8, :] += jnp.sum(cotangent, axis=0, keepdims=True)
        return carry

    lax.fori_loop(0, rows // c_rows, finish, 0)

    def o_tile(n, carry):
        cols = pl.ds(pl.multiple_of(n * tile, tile), tile)
        normed2_t[cols, :] = normed2[:, cols].T
        grad_wo[cols, :] = left_mul(context[:, cols], grad_att[...]).astype(jnp.bfloat16)
        return carry

    lax.fori_loop(0, width // tile, o_tile, 0)

    def ff_tile_grads(n, carry):
        cols = pl.ds(pl.multiple_of(n * tile, tile), tile)
        grad_wdown[cols, :] = left_mul(active[:, cols], out_grad[...]).astype(jnp.bfloat16)
        grad_wup[:, cols] = right_mul(normed2_t[...], grad_hidden[:, cols]).astype(jnp.bfloat16)
        return carry

    lax.fori_loop(0, ff // tile, ff_tile_grads, 0)


def ffn(tokens, context, out_grad, o_weight, up_weight, down_weight, vectors, up_bias):
    rows, width = tokens.shape
    ff = up_weight.shape[1]
    low = functools.partial(jax.ShapeDtypeStruct, dtype=jnp.bfloat16)
    full = functools.partial(jax.ShapeDtypeStruct, dtype=jnp.float32)
    vmem = pl.BlockSpec(memory_space=pltpu.VMEM)
    return pl.pallas_call(
        functools.partial(ffn_kernel, rows, rows, 1024, rows // 2, width),
        out_shape=[
            low((rows, width)), full((rows, width)), low((rows, width)),
            low((width, width)), low((width, ff)), low((ff, width)), full((8, width)), full((1, ff)),
        ],
        in_specs=[vmem] * 8,
        out_specs=[vmem] * 8,
        scratch_shapes=[
            pltpu.VMEM((rows, width), jnp.bfloat16),
            pltpu.VMEM((rows, ff), jnp.bfloat16),
            pltpu.VMEM((rows, ff), jnp.bfloat16),
            pltpu.VMEM((rows, width), jnp.bfloat16),
            pltpu.VMEM((width, rows), jnp.bfloat16),
        ],
        compiler_params=pltpu.CompilerParams(vmem_limit_bytes=VMEM_LIMIT),
        name="ffn",
    )(tokens, context, out_grad, o_weight, up_weight, down_weight, vectors, up_bias)


def head_lanes(pair, head):
    lane = lax.broadcasted_iota(jnp.int32, pair.shape, 1)
    return jnp.where(lax.div(lane, HEAD_DIM) == head, pair, jnp.zeros_like(pair))


def attend_kernel(strips, tokens, q_weight, k_weight, v_weight, vectors, mask, normed, queries, keys, values, probs, context):
    rows, width = tokens.shape
    slots, pairs = rows // strips, width // 128
    step = pl.program_id(0)

    @pl.when(step == 0)
    def _():
        xhat, _ = layer_norm_parts(tokens[...].astype(jnp.float32))
        normed[...] = (xhat * vectors[0:1, :] + vectors[1:2, :]).astype(jnp.bfloat16)
        scale = 1.0 / math.sqrt(HEAD_DIM)
        low = (right_mul(normed[...], q_weight[...]) + vectors[2:3, :]).astype(jnp.bfloat16)
        queries[...] = low * jnp.bfloat16(scale)
        keys[...] = right_mul(normed[...], k_weight[...]).astype(jnp.bfloat16)
        values[...] = (right_mul(normed[...], v_weight[...]) + vectors[3:4, :]).astype(jnp.bfloat16)

    at = pl.ds(pl.multiple_of(lax.div(step, pairs) * slots, slots), slots)
    cols = pl.ds(pl.multiple_of(lax.rem(step, pairs) * 128, 128), 128)
    query, key, value = queries[at, cols], keys[at, cols], values[at, cols]
    hidden = mask[at, 0:1]
    total = jnp.zeros((slots, 128), jnp.float32)
    for head in range(2):
        scores = back_mul(key, head_lanes(query, head)) + hidden
        powers = jnp.exp(scores - jnp.max(scores, axis=0, keepdims=True))
        low = (powers * (1.0 / jnp.sum(powers, axis=0, keepdims=True))).astype(jnp.bfloat16)
        probs[0, head] = low
        total = total + left_mul(low, head_lanes(value, head))
    context[at, cols] = total.astype(jnp.bfloat16)


def attend(strips, tokens, q_weight, k_weight, v_weight, vectors, mask):
    rows, width = tokens.shape
    slots, pairs = rows // strips, width // 128
    low = functools.partial(jax.ShapeDtypeStruct, dtype=jnp.bfloat16)
    whole = pl.BlockSpec((rows, width), lambda n: (0, 0))
    return pl.pallas_call(
        functools.partial(attend_kernel, strips),
        grid=(strips * pairs,),
        out_shape=[low((rows, width))] * 4 + [low((strips * pairs, 2, slots, slots)), low((rows, width))],
        in_specs=[pl.BlockSpec(memory_space=pltpu.VMEM)] * 6,
        out_specs=[whole] * 4 + [pl.BlockSpec((1, 2, slots, slots), lambda n: (n, 0, 0, 0)), whole],
        compiler_params=pltpu.CompilerParams(vmem_limit_bytes=VMEM_LIMIT),
        name="attend",
    )(tokens, q_weight, k_weight, v_weight, vectors, mask)


def attend_back_kernel(
    strips, tokens, normed, queries, keys, values, probs, grad_context, grad_res, q_weight, k_weight, v_weight, vectors,
    grad_tokens, grad_wq, grad_wk, grad_wv, small,
    grad_q, grad_k, grad_v,
):
    rows, width = tokens.shape
    slots, pairs = rows // strips, width // 128
    step = pl.program_id(0)
    at = pl.ds(pl.multiple_of(lax.div(step, pairs) * slots, slots), slots)
    cols = pl.ds(pl.multiple_of(lax.rem(step, pairs) * 128, 128), 128)
    query, key, value, grad = queries[at, cols], keys[at, cols], values[at, cols], grad_context[at, cols]
    back_q = back_k = back_v = jnp.zeros((slots, 128), jnp.float32)
    for head in range(2):
        low = probs[0, head]
        own = head_lanes(grad, head)
        back_v = back_v + right_mul(low, own)
        wide = low.astype(jnp.float32)
        slope = back_mul(value, own)
        inner = jnp.sum(wide * slope, axis=0, keepdims=True)
        pull = (wide * (slope - inner)).astype(jnp.bfloat16)
        back_q = back_q + left_mul(pull, head_lanes(key, head))
        back_k = back_k + right_mul(pull, head_lanes(query, head))
    grad_q[at, cols] = (back_q * (1.0 / math.sqrt(HEAD_DIM))).astype(jnp.bfloat16)
    grad_k[at, cols] = back_k.astype(jnp.bfloat16)
    grad_v[at, cols] = back_v.astype(jnp.bfloat16)

    @pl.when(step == strips * pairs - 1)
    def _():
        turned = normed[...].T
        grad_wq[...] = right_mul(turned, grad_q[...]).astype(jnp.bfloat16)
        grad_wk[...] = right_mul(turned, grad_k[...]).astype(jnp.bfloat16)
        grad_wv[...] = right_mul(turned, grad_v[...]).astype(jnp.bfloat16)
        small[...] = jnp.zeros_like(small)
        small[2:3, :] = jnp.sum(grad_q[...].astype(jnp.float32), axis=0, keepdims=True)
        small[3:4, :] = jnp.sum(grad_v[...].astype(jnp.float32), axis=0, keepdims=True)

        def finish(n, carry):
            at = pl.ds(pl.multiple_of(n * slots, slots), slots)
            grad = back_mul(grad_q[at, :], q_weight[...]) + back_mul(grad_k[at, :], k_weight[...])
            grad = grad + back_mul(grad_v[at, :], v_weight[...])
            xhat, scale = layer_norm_parts(tokens[at, :].astype(jnp.float32))
            back, gain_sum, bias_sum = layer_norm_back(grad, xhat, scale, vectors[0:1, :])
            grad_tokens[at, :] = grad_res[at, :] + back
            small[0:1, :] += gain_sum
            small[1:2, :] += bias_sum
            return carry

        lax.fori_loop(0, strips, finish, 0)


def attend_back(strips, tokens, normed, queries, keys, values, probs, grad_context, grad_res, q_weight, k_weight, v_weight, vectors):
    rows, width = tokens.shape
    slots, pairs = rows // strips, width // 128
    low = functools.partial(jax.ShapeDtypeStruct, dtype=jnp.bfloat16)
    full = functools.partial(jax.ShapeDtypeStruct, dtype=jnp.float32)
    vmem = pl.BlockSpec(memory_space=pltpu.VMEM)
    block = pl.BlockSpec((1, 2, slots, slots), lambda n: (n, 0, 0, 0))
    return pl.pallas_call(
        functools.partial(attend_back_kernel, strips),
        grid=(strips * pairs,),
        out_shape=[full((rows, width)), low((width, width)), low((width, width)), low((width, width)), full((8, width))],
        in_specs=[vmem] * 5 + [block] + [vmem] * 6,
        out_specs=[vmem] * 5,
        scratch_shapes=[pltpu.VMEM((rows, width), jnp.bfloat16)] * 3,
        compiler_params=pltpu.CompilerParams(vmem_limit_bytes=VMEM_LIMIT),
        name="attend_back",
    )(tokens, normed, queries, keys, values, probs, grad_context, grad_res, q_weight, k_weight, v_weight, vectors)


def pieces_of(shapes):
    pieces = []
    for n, shape in enumerate(shapes):
        parts = max(1, shape[-1] // 768)
        if parts == 1 and shape[-2] > shapes[0][-2] and shape[-1] == 768:
            parts = 3
        for k in range(parts):
            size = shape[-1] // parts
            pieces.append((n, k * size, size, 1 + len(pieces) % 2))
    return pieces


def staggered(count, stages):
    return [(step - s, s) for step in range(count + stages - 1) for s in range(stages) if 0 <= step - s < count]


def gather_kernel(dims, pieces, count, *refs):
    shards, bufs, (local, send, recv) = refs[:count], refs[count : 2 * count], refs[2 * count :]
    place = Place(dims)
    place.barrier()
    lanes = Lanes(place, send, recv)
    jobs = [
        Gather(lanes, shards[n].at[:, pl.ds(at, size)], bufs[n].at[:, :, :, :, :, pl.ds(at, size)], first, local.at[k])
        for k, (n, at, size, first) in enumerate(pieces)
    ]
    for job in jobs:
        job.start()
    for n, stage in staggered(len(jobs), 3):
        getattr(jobs[n], ("plane_first", "plane_second", "other_core")[stage])()
    for job in jobs:
        job.arrived()
        job.drain()


def gather_all(dims, arrays):
    count = len(arrays)
    pieces = pieces_of([a.shape for a in arrays])
    copies = gather_copies(dims) * len(pieces)
    return pl.pallas_call(
        functools.partial(gather_kernel, dims, pieces, count),
        out_shape=[jax.ShapeDtypeStruct(dims + (2,) + a.shape, a.dtype) for a in arrays],
        in_specs=[pl.BlockSpec(memory_space=pltpu.VMEM)] * count,
        out_specs=[pl.BlockSpec(memory_space=pl.ANY)] * count,
        scratch_shapes=[
            pltpu.SemaphoreType.DMA((len(pieces),)),
            pltpu.SemaphoreType.DMA((copies,)),
            pltpu.SemaphoreType.DMA((copies,)),
        ],
        compiler_params=pltpu.CompilerParams(collective_id=0, has_side_effects=True, vmem_limit_bytes=VMEM_LIMIT),
        name="gather",
    )(*arrays)


def scatter_kernel(dims, pieces, count, *refs):
    grads, outs, scratch = refs[:count], refs[count : 2 * count], refs[2 * count :]
    local, send, recv = scratch[-3:]
    place = Place(dims)
    place.barrier()
    lanes = Lanes(place, send, recv)
    jobs = [
        Scatter(
            lanes, grads[n].at[:, :, :, :, :, pl.ds(at, size)], outs[n].at[:, pl.ds(at, size)],
            scratch[5 * k : 5 * k + 5], first, local.at[k],
        )
        for k, (n, at, size, first) in enumerate(pieces)
    ]
    for job in jobs:
        job.start()
    ship = ("send_first", "send_second", "send_z")
    waiting = None
    for n, stage in staggered(len(jobs), 3):
        getattr(jobs[n], ("add_core", "add_first", "add_second")[stage])()
        if waiting is not None:
            waiting()
        waiting = getattr(jobs[n], ship[stage])
    waiting()
    for job in jobs:
        job.finish()


def scatter_all(dims, arrays):
    count = len(arrays)
    pieces = pieces_of([a.shape[4:] for a in arrays])
    copies = scatter_copies(dims) * len(pieces)
    scratch = []
    for n, at, size, first in pieces:
        scratch += scatter_scratch(dims, (arrays[n].shape[4], size), arrays[n].dtype, first)
    return pl.pallas_call(
        functools.partial(scatter_kernel, dims, pieces, count),
        out_shape=[jax.ShapeDtypeStruct(a.shape[4:], jnp.float32) for a in arrays],
        in_specs=[pl.BlockSpec(memory_space=pl.ANY)] * count,
        out_specs=[pl.BlockSpec(memory_space=pltpu.VMEM)] * count,
        scratch_shapes=scratch
        + [
            pltpu.SemaphoreType.DMA((len(pieces),)),
            pltpu.SemaphoreType.DMA((copies,)),
            pltpu.SemaphoreType.DMA((copies,)),
        ],
        compiler_params=pltpu.CompilerParams(collective_id=1, has_side_effects=True, vmem_limit_bytes=VMEM_LIMIT),
        name="scatter",
    )(*arrays)


def lane_pad(rows, width):
    return jnp.pad(rows, ((0, 0), (0, width - rows.shape[1])))


def pack_vectors(vectors, wide):
    width = 128 * -(-wide.shape[0] // 128)
    rows = lane_pad(jnp.stack(vectors).astype(jnp.float32), width)
    last = lane_pad(wide[None].astype(jnp.float32), width)
    return jnp.pad(jnp.concatenate([rows, last]), ((0, 15 - len(vectors)), (0, 0)))


def unpack_vectors(block, part, wide_part):
    flat = block.reshape((-1,) + block.shape[-2:])
    rows = flat[:, :8, :part].transpose(1, 0, 2).reshape(8, -1)
    return rows, flat[:, 8, :wide_part].reshape(1, -1)


def pack_vector_grads(dims, vectors, wide):
    n = 2 * dims[0] * dims[1] * dims[2]
    part, wide_part = vectors.shape[1] // n, wide.shape[1] // n
    width = 128 * -(-wide_part // 128)
    rows = vectors.reshape(8, n, part).transpose(1, 0, 2)
    rows = jnp.pad(rows, ((0, 0), (0, 0), (0, width - part)))
    last = jnp.pad(wide.reshape(n, 1, wide_part), ((0, 0), (0, 0), (0, width - wide_part)))
    block = jnp.pad(jnp.concatenate([rows, last], axis=1), ((0, 0), (0, 7), (0, 0)))
    return block.reshape(dims + (2,) + block.shape[1:])


def shards(
    dims,
    tokens,
    lengths,
    key_mask,
    ln1_gain,
    ln1_bias,
    q_weight,
    q_bias,
    k_weight,
    v_weight,
    v_bias,
    o_weight,
    o_bias,
    ln2_gain,
    ln2_bias,
    up_weight,
    up_bias,
    down_weight,
    down_bias,
    out_grad,
):
    weights = (q_weight, k_weight, v_weight, o_weight, up_weight, down_weight)
    vectors = (ln1_gain, ln1_bias, q_bias, v_bias, o_bias, ln2_gain, ln2_bias, down_bias)
    *wide, packed = gather_all(dims, list(weights) + [pack_vectors(vectors, up_bias)])
    q_full, k_full, v_full, o_full, up_full, down_full = [w.reshape((-1,) + w.shape[-1:]) for w in wide]
    rows, up_bias_full = unpack_vectors(packed, ln1_gain.shape[0], up_bias.shape[0])

    row_count, width = tokens.shape
    strips = lengths.shape[0]
    slots = row_count // strips
    extra = -slots % 16

    def padded(values):
        return jnp.pad(values.reshape(strips, slots, width), ((0, 0), (0, extra), (0, 0))).reshape(-1, width)

    def cropped(values):
        return values.reshape(strips, slots + extra, width)[:, :slots].reshape(row_count, width)

    slot_ids = lax.iota(jnp.int32, slots)
    visible = (slot_ids[None, :] == 0) | (slot_ids[None, :] < lengths[:, None]) & (key_mask == 1)
    mask = jnp.where(jnp.pad(visible, ((0, 0), (0, extra))), 0.0, NEG_FILL).reshape(-1, 1)
    tokens_in, grads_in = padded(tokens), padded(out_grad)

    normed, queries, keys, values, probs, context = attend(strips, tokens_in, q_full, k_full, v_full, rows, mask)
    block_out, grad_res, grad_context, grad_wo, grad_wup, grad_wdown, small, grad_bup = ffn(
        tokens_in, context, grads_in, o_full, up_full, down_full, rows, up_bias_full
    )
    grad_tokens, grad_wq, grad_wk, grad_wv, small_two = attend_back(
        strips, tokens_in, normed, queries, keys, values, probs, grad_context, grad_res, q_full, k_full, v_full, rows
    )

    def blocks(grad, like):
        return grad.reshape(dims + (2,) + like.shape)

    vector_grads = pack_vector_grads(dims, small + small_two, grad_bup)
    full = (grad_wq, grad_wk, grad_wv, grad_wo, grad_wup, grad_wdown)
    *sums, least = scatter_all(dims, [blocks(g, w) for g, w in zip(full, weights)] + [vector_grads])
    sum_wq, sum_wk, sum_wv, sum_wo, sum_wup, sum_wdown = sums
    vec = [least[n, : ln1_gain.shape[0]] for n in range(8)]
    return (
        cropped(block_out), cropped(grad_tokens), vec[0], vec[1], sum_wq, vec[2], sum_wk, sum_wv, vec[3], sum_wo, vec[4],
        vec[5], vec[6], sum_wup, least[8, : up_bias.shape[0]], sum_wdown, vec[7],
    )


def solution(mesh):
    rows, flat = P(("gx", "gy"), None), P(("gx", "gy"))
    return jax.shard_map(
        functools.partial(shards, grid_of(mesh)),
        mesh=mesh,
        in_specs=(
            rows, flat, rows, flat, flat, rows, flat, rows, rows, flat, rows, flat, flat, flat, rows, flat, rows, flat, rows,
        ),
        out_specs=(
            rows, rows, flat, flat, rows, flat, rows, rows, flat, rows, flat, flat, flat, rows, flat, rows, flat,
        ),
        check_vma=False,
    )
```

```python
import functools
import math

import jax
import jax.numpy as jnp
from jax import lax
from jax.experimental import pallas as pl
from jax.experimental.pallas import tpu as pltpu
from jax.sharding import PartitionSpec as P

HEAD_DIM = 64
EPSILON = 1e-06
NEG_FILL = -1e30
VMEM_LIMIT = 63 * 1024 * 1024
GATHER_PACE = 2.0
SCATTER_LAG = 12.0
SCATTER_GAP = 6.0


def right_mul(left_arg, right_arg):
    return jnp.dot(left_arg, right_arg, preferred_element_type=jnp.float32)


def left_mul(left_arg, right_arg):
    return lax.dot_general(
        left_arg, right_arg, (((0,), (0,)), ((), ())), preferred_element_type=jnp.float32
    )


def back_mul(left_arg, right_arg):
    return lax.dot_general(
        left_arg, right_arg, (((1,), (1,)), ((), ())), preferred_element_type=jnp.float32
    )


MESH = pl.DeviceIdType.MESH


def grid_of(mesh):
    z_size, plane = mesh.shape["gx"], mesh.shape["gy"] // 2
    x_size = max(n for n in range(1, plane + 1) if plane % n == 0 and n * n <= plane)
    return z_size, plane // x_size, x_size


class Place:
    def __init__(self, dims):
        self.dims = dims
        g = lax.axis_index("gy")
        self.z = lax.axis_index("gx")
        self.c = lax.rem(g, 2)
        self.x = lax.rem(lax.div(g, 2), dims[2])
        self.y = lax.div(g, 2 * dims[2])

    def at(self, axis, step):
        here = (self.z, self.y, self.x)[axis]
        return lax.rem(here + step, self.dims[axis])

    def plane(self, first, step, other_step):
        a, b = self.at(first, step), self.at(3 - first, other_step)
        return (a, b) if first == 1 else (b, a)

    def device(self, axis, step):
        where = [self.z, self.y, self.x, self.c]
        if axis == 3:
            where[3] = 1 - self.c
        else:
            where[axis] = self.at(axis, step)
        return (where[0], (where[1] * self.dims[2] + where[2]) * 2 + where[3])

    def barrier(self):
        sem = pltpu.get_barrier_semaphore()
        peers = [(axis, step) for axis in range(3) for step in range(1, self.dims[axis])] + [(3, 1)]
        for axis, step in peers:
            pl.semaphore_signal(sem, inc=1, device_id=self.device(axis, step), device_id_type=MESH)
        pl.semaphore_wait(sem, len(peers))


class Lanes:
    def __init__(self, place, local, send, recv):
        self.place, self.local_sem, self.send, self.recv = place, local, send, recv
        self.used = self.local_used = 0

    def remote(self, src, dst, axis, step):
        n = self.used
        self.used += 1
        return pltpu.make_async_remote_copy(
            src_ref=src, dst_ref=dst, send_sem=self.send.at[n], recv_sem=self.recv.at[n],
            device_id=self.place.device(axis, step), device_id_type=MESH,
        )

    def local(self, src, dst):
        n = self.local_used
        self.local_used += 1
        return pltpu.make_async_copy(src, dst, self.local_sem.at[n])


def gather_copies(dims, z_last):
    z, y, x = dims
    if z_last:
        return (x * y - 1) + (z - 1) + z
    return (z - 1) + (x * y - 1) + x * y


class Gather:
    def __init__(self, lanes, shard, buf, first, z_last):
        p, dims = lanes.place, lanes.place.dims
        firsts, seconds = range(1, dims[first]), range(1, dims[3 - first])
        own = buf.at[p.z, p.y, p.x, p.c]
        local = lanes.local(shard, own)
        remote = lanes.remote

        def cell(step, other):
            y, x = p.plane(first, step, other)
            return buf.at[p.z, y, x, p.c] if z_last else buf.at[:, y, x, p.c]

        def layer(step):
            return buf.at[p.at(0, step), :, :, p.c]

        mine = shard if z_last else cell(0, 0)
        to_first = [remote(mine, cell(0, 0), first, s) for s in firsts]
        to_second = [remote(mine, cell(0, 0), 3 - first, t) for t in seconds]
        onward = [remote(cell(s, 0), cell(s, 0), 3 - first, t) for s in firsts for t in seconds]
        if z_last:
            along_z = [remote(layer(0), layer(0), 0, s) for s in range(1, dims[0])]
            cores = [remote(layer(s), layer(s), 3, 1) for s in range(dims[0])]
            self.stages = [
                ([], [], to_first + to_second + [local]),
                ([], to_first, onward),
                ([local], to_second + onward, along_z + cores[:1]),
                ([], along_z, cores[1:]),
            ]
        else:
            along_z = [remote(shard, own, 0, s) for s in range(1, dims[0])]
            core = {(s, t): remote(cell(s, t), cell(s, t), 3, 1) for s in range(dims[first]) for t in range(dims[3 - first])}
            cores = list(core.values())
            self.stages = [
                ([], [], along_z + [local]),
                ([local], along_z, to_first + to_second + [core[0, 0]]),
                ([], to_first, onward + [core[s, 0] for s in firsts]),
                ([], to_second + onward, [core[s, t] for s in range(dims[first]) for t in seconds]),
            ]
        self.handed = cores
        self.remotes = to_first + to_second + onward + along_z + cores

    def run(self, stage):
        done, arrived, starts = self.stages[stage]
        for copy in done:
            copy.wait()
        for copy in arrived:
            copy.wait_recv()
        for copy in starts:
            copy.start()

    def finish(self):
        for copy in self.handed:
            copy.wait_recv()
        for copy in self.remotes:
            copy.wait_send()


def scatter_copies(dims):
    z, y, x = dims
    return 1 + (z - 1) + (x * y - 1)


def scatter_copies(dims):
    z, y, x = dims
    return 1 + (z - 1) + (x * y - 1)


def pieces_of(shapes, narrow):
    pieces = []
    for n, shape in enumerate(shapes):
        parts = max(1, shape[-1] // 768)
        if parts == 1 and shape[-2] > narrow and shape[-1] == 768:
            parts = 3
        for k in range(parts):
            size = shape[-1] // parts
            pieces.append((n, k * size, size, 1 + len(pieces) % 2))
    return pieces


def waves(count, stages):
    return [[(b + 1 - s, s) for s in range(1, stages) if 0 <= b + 1 - s < count] for b in range(count + stages - 2)]


def gather_jobs(lanes, pieces, shards, bufs):
    return [
        Gather(lanes, shards[n].at[:, pl.ds(at, size)], bufs[n].at[:, :, :, :, :, pl.ds(at, size)], first, False)
        for n, at, size, first in pieces
    ]


def comm_semaphores(pieces, copies):
    return [
        pltpu.SemaphoreType.DMA((len(pieces),)),
        pltpu.SemaphoreType.DMA((copies * len(pieces),)),
        pltpu.SemaphoreType.DMA((copies * len(pieces),)),
    ]


def run_wave(jobs, wave):
    for n, stage in wave:
        jobs[n].run(stage)


def gather_kernel(dims, pieces, count, *refs):
    shards, bufs, sems = refs[:count], refs[count : 2 * count], refs[2 * count :]
    place = Place(dims)
    jobs = gather_jobs(Lanes(place, *sems), pieces, shards, bufs)
    place.barrier()
    for job in jobs:
        job.run(0)
    for wave in waves(len(jobs), 4):
        run_wave(jobs, wave)
    for job in jobs:
        job.finish()


def gather_all(dims, arrays):
    count = len(arrays)
    pieces = pieces_of([a.shape for a in arrays], arrays[0].shape[0])
    return pl.pallas_call(
        functools.partial(gather_kernel, dims, pieces, count),
        out_shape=[jax.ShapeDtypeStruct(dims + (2,) + a.shape, a.dtype) for a in arrays],
        in_specs=[pl.BlockSpec(memory_space=pltpu.VMEM)] * count,
        out_specs=[pl.BlockSpec(memory_space=pl.ANY)] * count,
        scratch_shapes=comm_semaphores(pieces, gather_copies(dims, False)),
        compiler_params=pltpu.CompilerParams(collective_id=0, has_side_effects=True, vmem_limit_bytes=VMEM_LIMIT),
        name="gather",
    )(*arrays)


def layer_norm_parts(values):
    center = values - jnp.mean(values, axis=-1, keepdims=True)
    scale = lax.rsqrt(jnp.mean(center * center, axis=-1, keepdims=True) + EPSILON)
    return center * scale, scale


def layer_norm_back(grad, xhat, scale, gain):
    scaled = grad * gain
    inner = scaled - jnp.mean(scaled, axis=-1, keepdims=True)
    back = scale * (inner - xhat * jnp.mean(scaled * xhat, axis=-1, keepdims=True))
    return back, jnp.sum(grad * xhat, axis=0, keepdims=True), jnp.sum(grad, axis=0, keepdims=True)


def gelu_and_slope(v):
    size = jnp.abs(v)
    t = 1.0 / (1.0 + (0.3275911 * math.sqrt(0.5)) * size)
    bell = jnp.exp(-0.5 * v * v)
    poly = ((((0.5 * 1.061405429) * t - 0.5 * 1.453152027) * t + 0.5 * 1.421413741) * t - 0.5 * 0.284496736) * t
    tail = (poly + 0.5 * 0.254829592) * t * bell
    share = jnp.where(v >= 0, 1.0 - tail, tail)
    return v * share, share + (v * (1.0 / math.sqrt(2.0 * math.pi))) * bell


def ffn_kernel(
    a_rows, b_rows, ff_tile, c_rows,
    tokens, context, out_grad, o_weight, up_weight, down_weight, vectors, up_bias,
    block_out, grad_res, grad_context, grad_wo, active, grad_hidden, normed2_t, small, grad_bup,
    normed2, grad_att,
):
    rows, width = tokens.shape
    ff = up_weight.shape[1]
    o_bias, gain, bias, down_bias = vectors[4:5, :], vectors[5:6, :], vectors[6:7, :], vectors[7:8, :]
    small[...] = jnp.zeros_like(small)

    def attended(n, carry):
        at = pl.ds(pl.multiple_of(n * a_rows, a_rows), a_rows)
        residual = tokens[at, :].astype(jnp.float32) + right_mul(context[at, :], o_weight[...]) + o_bias
        grad_res[at, :] = residual
        xhat, _ = layer_norm_parts(residual)
        normed2[at, :] = (xhat * gain + bias).astype(jnp.bfloat16)
        return carry

    lax.fori_loop(0, rows // a_rows, attended, 0)

    def hidden_tile(n, carry):
        cols = pl.ds(pl.multiple_of(n * ff_tile, ff_tile), ff_tile)
        sums = jnp.zeros((1, ff_tile), jnp.float32)

        def piece(m, sums):
            at = pl.ds(pl.multiple_of(m * b_rows, b_rows), b_rows)
            hidden = right_mul(normed2[at, :], up_weight[:, cols]) + up_bias[:, cols]
            grad_active = back_mul(out_grad[at, :], down_weight[cols, :])
            value, slope = gelu_and_slope(hidden)
            active[at, cols] = value.astype(jnp.bfloat16)
            back = (slope * grad_active).astype(jnp.bfloat16)
            grad_hidden[at, cols] = back
            return sums + jnp.sum(back.astype(jnp.float32), axis=0, keepdims=True)

        grad_bup[:, cols] = lax.fori_loop(0, rows // b_rows, piece, sums)
        return carry

    lax.fori_loop(0, ff // ff_tile, hidden_tile, 0)

    def finish(n, carry):
        at = pl.ds(pl.multiple_of(n * c_rows, c_rows), c_rows)
        residual = grad_res[at, :]
        cotangent = out_grad[at, :].astype(jnp.float32)
        block_out[at, :] = (residual + right_mul(active[at, :], down_weight[...]) + down_bias).astype(jnp.bfloat16)
        grad = back_mul(grad_hidden[at, :], up_weight[...])
        xhat, scale = layer_norm_parts(residual)
        back, gain_sum, bias_sum = layer_norm_back(grad, xhat, scale, gain)
        total = cotangent + back
        grad_res[at, :] = total
        low = total.astype(jnp.bfloat16)
        grad_att[at, :] = low
        grad_context[at, :] = back_mul(low, o_weight[...]).astype(jnp.bfloat16)
        small[4:5, :] += jnp.sum(low.astype(jnp.float32), axis=0, keepdims=True)
        small[5:6, :] += gain_sum
        small[6:7, :] += bias_sum
        small[7:8, :] += jnp.sum(cotangent, axis=0, keepdims=True)
        return carry

    lax.fori_loop(0, rows // c_rows, finish, 0)

    normed2_t[...] = normed2[...].T
    grad_wo[...] = left_mul(context[...], grad_att[...]).astype(jnp.bfloat16)


def ffn(tokens, context, out_grad, o_weight, up_weight, down_weight, vectors, up_bias):
    rows, width = tokens.shape
    ff = up_weight.shape[1]
    low = functools.partial(jax.ShapeDtypeStruct, dtype=jnp.bfloat16)
    full = functools.partial(jax.ShapeDtypeStruct, dtype=jnp.float32)
    vmem = pl.BlockSpec(memory_space=pltpu.VMEM)
    return pl.pallas_call(
        functools.partial(ffn_kernel, rows, rows, 1024, rows // 2),
        out_shape=[
            low((rows, width)), full((rows, width)), low((rows, width)),
            low((width, width)), low((rows, ff)), low((rows, ff)), low((width, rows)), full((8, width)), full((1, ff)),
        ],
        in_specs=[vmem] * 8,
        out_specs=[vmem] * 9,
        scratch_shapes=[pltpu.VMEM((rows, width), jnp.bfloat16)] * 2,
        compiler_params=pltpu.CompilerParams(vmem_limit_bytes=VMEM_LIMIT),
        name="ffn",
    )(tokens, context, out_grad, o_weight, up_weight, down_weight, vectors, up_bias)


def head_lanes(pair, head):
    lane = lax.broadcasted_iota(jnp.int32, pair.shape, 1)
    return jnp.where(lax.div(lane, HEAD_DIM) == head, pair, jnp.zeros_like(pair))


def attend_kernel(dims, pieces, count, pace, strips, tokens, q_weight, k_weight, v_weight, vectors, mask, *refs):
    shards, refs = refs[:count], refs[count:]
    (turned, queries, keys, values, probs, context), bufs, scratch = refs[:6], refs[6 : 6 + count], refs[6 + count :]
    normed, *sems = scratch
    rows, width = tokens.shape
    slots, pairs = rows // strips, width // 128
    step = pl.program_id(0)
    due, late, jobs = {}, [], []
    if count:
        place = Place(dims)
        jobs = gather_jobs(Lanes(place, *sems), pieces, shards, bufs)
        late = waves(len(jobs), 4)
        for k, wave in enumerate(list(late)):
            when = 1 + int(pace * k)
            if when < strips * pairs:
                due[when] = wave
                late = late[1:]

    @pl.when(step == 0)
    def _():
        if count:
            place.barrier()
        for job in jobs:
            job.run(0)
        xhat, _ = layer_norm_parts(tokens[...].astype(jnp.float32))
        normed[...] = (xhat * vectors[0:1, :] + vectors[1:2, :]).astype(jnp.bfloat16)
        turned[...] = normed[...].T
        scale = 1.0 / math.sqrt(HEAD_DIM)
        low = (right_mul(normed[...], q_weight[...]) + vectors[2:3, :]).astype(jnp.bfloat16)
        queries[...] = low * jnp.bfloat16(scale)
        keys[...] = right_mul(normed[...], k_weight[...]).astype(jnp.bfloat16)
        values[...] = (right_mul(normed[...], v_weight[...]) + vectors[3:4, :]).astype(jnp.bfloat16)

    for when, wave in due.items():
        pl.when(step == when)(functools.partial(run_wave, jobs, wave))

    at = pl.ds(pl.multiple_of(lax.div(step, pairs) * slots, slots), slots)
    cols = pl.ds(pl.multiple_of(lax.rem(step, pairs) * 128, 128), 128)
    query, key, value = queries[at, cols], keys[at, cols], values[at, cols]
    hidden = mask[at, 0:1]
    total = jnp.zeros((slots, 128), jnp.float32)
    for head in range(2):
        scores = back_mul(key, head_lanes(query, head)) + hidden
        powers = jnp.exp(scores - jnp.max(scores, axis=0, keepdims=True))
        low = (powers * (1.0 / jnp.sum(powers, axis=0, keepdims=True))).astype(jnp.bfloat16)
        probs[0, head] = low
        total = total + left_mul(low, head_lanes(value, head))
    context[at, cols] = total.astype(jnp.bfloat16)

    @pl.when(step == strips * pairs - 1)
    def _():
        for wave in late:
            run_wave(jobs, wave)
        for job in jobs:
            job.finish()


def attend(dims, shards, strips, tokens, q_weight, k_weight, v_weight, vectors, mask):
    rows, width = tokens.shape
    slots, pairs = rows // strips, width // 128
    low = functools.partial(jax.ShapeDtypeStruct, dtype=jnp.bfloat16)
    vmem = pl.BlockSpec(memory_space=pltpu.VMEM)
    pieces = pieces_of([s.shape for s in shards], shards[0].shape[0]) if shards else []
    exchange = dict(collective_id=2, has_side_effects=True) if shards else {}
    return pl.pallas_call(
        functools.partial(attend_kernel, dims, pieces, len(shards), GATHER_PACE, strips),
        grid=(strips * pairs,),
        out_shape=[low((width, rows))]
        + [low((rows, width))] * 3
        + [low((strips * pairs, 2, slots, slots)), low((rows, width))]
        + [low(dims + (2,) + s.shape) for s in shards],
        in_specs=[vmem] * (6 + len(shards)),
        out_specs=[vmem] * 4
        + [pl.BlockSpec((1, 2, slots, slots), lambda n: (n, 0, 0, 0)), vmem]
        + [pl.BlockSpec(memory_space=pl.ANY)] * len(shards),
        scratch_shapes=[pltpu.VMEM((rows, width), jnp.bfloat16)]
        + (comm_semaphores(pieces, gather_copies(dims, False)) if shards else []),
        compiler_params=pltpu.CompilerParams(vmem_limit_bytes=VMEM_LIMIT, **exchange),
        name="attend",
    )(tokens, q_weight, k_weight, v_weight, vectors, mask, *shards)


def attend_back_kernel(
    strips, tokens, turned, queries, keys, values, probs, grad_context, grad_res, q_weight, k_weight, v_weight, vectors,
    grad_tokens, grad_wq, grad_wk, grad_wv, small,
    grad_q, grad_k, grad_v,
):
    rows, width = tokens.shape
    slots, pairs = rows // strips, width // 128
    step = pl.program_id(0)
    at = pl.ds(pl.multiple_of(lax.div(step, pairs) * slots, slots), slots)
    cols = pl.ds(pl.multiple_of(lax.rem(step, pairs) * 128, 128), 128)
    query, key, value, grad = queries[at, cols], keys[at, cols], values[at, cols], grad_context[at, cols]
    back_q = back_k = back_v = jnp.zeros((slots, 128), jnp.float32)
    for head in range(2):
        low = probs[0, head]
        own = head_lanes(grad, head)
        back_v = back_v + right_mul(low, own)
        wide = low.astype(jnp.float32)
        slope = back_mul(value, own)
        inner = jnp.sum(wide * slope, axis=0, keepdims=True)
        pull = (wide * (slope - inner)).astype(jnp.bfloat16)
        back_q = back_q + left_mul(pull, head_lanes(key, head))
        back_k = back_k + right_mul(pull, head_lanes(query, head))
    grad_q[at, cols] = (back_q * (1.0 / math.sqrt(HEAD_DIM))).astype(jnp.bfloat16)
    grad_k[at, cols] = back_k.astype(jnp.bfloat16)
    grad_v[at, cols] = back_v.astype(jnp.bfloat16)

    @pl.when(step == strips * pairs - 1)
    def _():
        grad_wq[...] = right_mul(turned[...], grad_q[...]).astype(jnp.bfloat16)
        grad_wk[...] = right_mul(turned[...], grad_k[...]).astype(jnp.bfloat16)
        grad_wv[...] = right_mul(turned[...], grad_v[...]).astype(jnp.bfloat16)
        small[...] = jnp.zeros_like(small)
        small[2:3, :] = jnp.sum(grad_q[...].astype(jnp.float32), axis=0, keepdims=True)
        small[3:4, :] = jnp.sum(grad_v[...].astype(jnp.float32), axis=0, keepdims=True)

        def finish(n, carry):
            at = pl.ds(pl.multiple_of(n * slots, slots), slots)
            grad = back_mul(grad_q[at, :], q_weight[...]) + back_mul(grad_k[at, :], k_weight[...])
            grad = grad + back_mul(grad_v[at, :], v_weight[...])
            xhat, scale = layer_norm_parts(tokens[at, :].astype(jnp.float32))
            back, gain_sum, bias_sum = layer_norm_back(grad, xhat, scale, vectors[0:1, :])
            grad_tokens[at, :] = grad_res[at, :] + back
            small[0:1, :] += gain_sum
            small[1:2, :] += bias_sum
            return carry

        lax.fori_loop(0, strips, finish, 0)


def attend_back(strips, tokens, turned, queries, keys, values, probs, grad_context, grad_res, q_weight, k_weight, v_weight, vectors):
    rows, width = tokens.shape
    slots, pairs = rows // strips, width // 128
    low = functools.partial(jax.ShapeDtypeStruct, dtype=jnp.bfloat16)
    full = functools.partial(jax.ShapeDtypeStruct, dtype=jnp.float32)
    vmem = pl.BlockSpec(memory_space=pltpu.VMEM)
    block = pl.BlockSpec((1, 2, slots, slots), lambda n: (n, 0, 0, 0))
    return pl.pallas_call(
        functools.partial(attend_back_kernel, strips),
        grid=(strips * pairs,),
        out_shape=[full((rows, width)), low((width, width)), low((width, width)), low((width, width)), full((8, width))],
        in_specs=[vmem] * 5 + [block] + [vmem] * 6,
        out_specs=[vmem] * 5,
        scratch_shapes=[pltpu.VMEM((rows, width), jnp.bfloat16)] * 3,
        compiler_params=pltpu.CompilerParams(vmem_limit_bytes=VMEM_LIMIT),
        name="attend_back",
    )(tokens, turned, queries, keys, values, probs, grad_context, grad_res, q_weight, k_weight, v_weight, vectors)


class Reduce:
    def __init__(self, lanes, whole, bufs, first, write):
        p, dims = lanes.place, lanes.place.dims
        self.p, self.dims, self.first, self.write = p, dims, first, write
        self.firsts, self.seconds = range(1, dims[first]), range(1, dims[3 - first])
        self.from_core, self.from_far, self.from_first, self.from_second, self.from_z = bufs
        self.mine, remote = whole.at[:, :, :, p.c], lanes.remote

        def cell(step, other):
            y, x = p.plane(first, step, other)
            return whole.at[:, y, x, p.c]

        core = [remote(whole.at[:, :, :, 1 - p.c], self.from_core, 3, 1)]
        self.far = [remote(cell(s, t), self.from_far.at[s - 1, t - 1], first, s) for s in self.firsts for t in self.seconds]
        self.to_first = [remote(cell(s, 0), self.from_first.at[s - 1], first, s) for s in self.firsts]
        self.to_second = [remote(cell(0, t), self.from_second.at[t - 1], 3 - first, t) for t in self.seconds]
        along_z = [
            remote(whole.at[p.at(0, s), p.y, p.x, p.c], self.from_z.at[s - 1], 0, s) for s in range(1, dims[0])
        ]
        self.ships = [core, self.far + self.to_first, self.to_second, along_z]

    def total(self, at, terms):
        total = self.mine[at].astype(jnp.float32)
        for ref, index in terms:
            total = total + ref[index].astype(jnp.float32)
        return total

    def add(self, at, terms):
        self.mine[at] = self.total(at, terms).astype(self.mine.dtype)

    def run(self, stage):
        p, (z_size, y_size, x_size) = self.p, self.dims
        arrivals = (self.ships[0], self.far, self.to_first + self.to_second, self.ships[3])[stage - 1]
        for copy in arrivals:
            copy.wait_recv()
        if stage == 1:
            def body(n, carry):
                at = (lax.div(n, y_size * x_size), lax.rem(lax.div(n, x_size), y_size), lax.rem(n, x_size))
                self.add(at, [(self.from_core, at)])
                return carry

            lax.fori_loop(0, z_size * y_size * x_size, body, 0)
        elif stage == 2:
            for z in range(z_size):
                for t in self.seconds:
                    self.add((z,) + p.plane(self.first, 0, t), [(self.from_far, (s - 1, t - 1, z)) for s in self.firsts])
        elif stage == 3:
            for z in range(z_size):
                terms = [(self.from_first, (s - 1, z)) for s in self.firsts]
                self.add((z, p.y, p.x), terms + [(self.from_second, (t - 1, z)) for t in self.seconds])
        else:
            self.write(self.total((p.z, p.y, p.x), [(self.from_z, (s,)) for s in range(z_size - 1)]))

    def ship(self, stage):
        if stage < 4:
            for copy in self.ships[stage]:
                copy.start()

    def finish(self):
        for copies in self.ships:
            for copy in copies:
                copy.wait_send()


def reduce_scratch(dims, shape, dtype, first):
    z, y, x = dims
    f, s = max(dims[first] - 1, 1), max(dims[3 - first] - 1, 1)
    leads = [(z, y, x), (f, s, z), (f, z), (s, z), (max(z - 1, 1),)]
    return [pltpu.VMEM(lead + shape, dtype) for lead in leads]


def add_wave(jobs, wave):
    left = None
    for n, stage in wave:
        if stage:
            jobs[n].run(stage)
        if left:
            jobs[left[0]].ship(left[1])
        left = (n, stage)
    return left


FF_TILE = 384
FINISH = 4
PAIRS_PER_PIECE = 2


class Plan:
    def __init__(self, dims, strips, rows, width, ff, lag, gap):
        self.tiles, self.pairs = ff // FF_TILE, width // 128
        self.down = self.tiles
        self.attention = 2 * self.tiles
        self.finish = self.attention + strips * self.pairs
        self.steps = self.finish + FINISH
        n = 2 * dims[0] * dims[1] * dims[2]
        model, wide = width // n, ff // n
        per_up = width // FF_TILE
        lasts = [0] + [per_up * (k + 1) for k in range(ff // width)] + [self.attention] * 3
        groups = self.pairs // PAIRS_PER_PIECE
        lasts += [self.attention + strips * PAIRS_PER_PIECE * (g + 1) for g in range(groups)]
        self.wholes = [(model, width)] * (1 + ff // width) + [(wide, width)]
        self.wholes += [(3 * model, width // groups)] * groups
        self.shapes = [(model, width)] * (1 + ff // width) + [(wide, width // 3)] * 3 + [(3 * model, width // groups)] * groups
        ends = [1.4] * self.attention + [3.2] * (strips * self.pairs) + [1.6] * FINISH
        starts = [sum(ends[:k]) for k in range(self.steps)]
        events, free = [], 0.0
        for piece, step in enumerate(lasts):
            begin = max(starts[step], free)
            free = begin + gap
            events += [(starts[step], 0, piece, step)]
            events += [(begin + 2.0 + lag * (k - 1), k, piece, 0) for k in range(1, 5)]
        self.waves, self.late = {}, []
        for when, stage, piece, step in sorted(events):
            fits = [k for k in range(self.steps) if starts[k] >= when and k >= step]
            if fits:
                self.waves.setdefault(fits[0], []).append((piece, stage))
            else:
                self.late.append((piece, stage))


def backward_kernel(dims, plan, strips, *refs):
    (turned, turned_two, out_grad, q_weight, k_weight, v_weight, vectors, small_in, bup_in) = refs[:9]
    (grad_hidden, active, probs, query_b, key_b, value_b, grad_b, tokens, grad_res, wo_hbm) = refs[9:19]
    (grad_tokens, sum_q, sum_k, sum_v, sum_o, sum_up, sum_down, sum_vec) = refs[19:27]
    refs = refs[27:]
    grad_q, grad_k, grad_v, small, vec_whole = refs[:5]
    wholes, refs = refs[5 : 5 + len(plan.wholes)], refs[5 + len(plan.wholes) :]
    local, send, recv = refs[-3:]
    width, rows = turned.shape
    slots, ff_pieces, groups = rows // strips, sum_up.shape[1] // width, len(plan.wholes) - 2 - sum_up.shape[1] // width
    step = pl.program_id(0)
    place = Place(dims)
    lanes = Lanes(place, local, send, recv)
    o_copy = lanes.local(wo_hbm, wholes[0])

    model = sum_q.shape[0]
    columns = width // groups

    def write_to(ref, at, size):
        def write(total):
            ref[:, pl.ds(at, size)] = total
        return write

    def write_group(g):
        def write(total):
            for n, ref in enumerate((sum_q, sum_k, sum_v)):
                ref[:, pl.ds(g * columns, columns)] = total[n * model : (n + 1) * model]
        return write

    third = width // 3
    down_whole = wholes[1 + ff_pieces]
    views = [(wholes[0], write_to(sum_o, 0, width))]
    views += [(wholes[1 + k], write_to(sum_up, k * width, width)) for k in range(ff_pieces)]
    views += [
        (down_whole.at[:, :, :, :, :, pl.ds(k * third, third)], write_to(sum_down, k * third, third)) for k in range(3)
    ]
    views += [(wholes[2 + ff_pieces + g], write_group(g)) for g in range(groups)]
    views += [(vec_whole, write_to(sum_vec, 0, sum_vec.shape[1]))]
    jobs = [Reduce(lanes, whole, refs[5 * n : 5 * n + 5], 1 + n % 2, write) for n, (whole, write) in enumerate(views)]
    last = len(jobs) - 1

    @pl.when(step == 0)
    def _():
        place.barrier()
        o_copy.start()
        small[...] = small_in[...]
        o_copy.wait()

    for when, wave in plan.waves.items():
        pl.when(step == when)(lambda wave=wave: add_wave(jobs, wave) and None)

    def rows_to_blocks(product):
        n = 2 * dims[0] * dims[1] * dims[2]
        return product.reshape(dims + (2, product.shape[0] // n, product.shape[1])).astype(jnp.bfloat16)

    for k in range(plan.tiles):
        @pl.when(step == k)
        def _():
            piece, part = divmod(k * FF_TILE, width)
            wholes[1 + piece][:, :, :, :, :, pl.ds(part, FF_TILE)] = rows_to_blocks(right_mul(turned_two[...], grad_hidden[...]))

        @pl.when(step == plan.down + k)
        def _():
            product = left_mul(active[...], out_grad[...])
            wide = down_whole.shape[4]
            for b in range(FF_TILE // wide):
                d = k * (FF_TILE // wide) + b
                at = (d // (2 * dims[1] * dims[2]), d // (2 * dims[2]) % dims[1], d // 2 % dims[2], d % 2)
                down_whole[at] = product[b * wide : (b + 1) * wide].astype(jnp.bfloat16)

    pair, strip = lax.div(step - plan.attention, strips), lax.rem(step - plan.attention, strips)
    in_attention = (step >= plan.attention) & (step < plan.finish)

    @pl.when(in_attention)
    def _():
        at = pl.ds(pl.multiple_of(strip * slots, slots), slots)
        cols = pl.ds(pl.multiple_of(pair * 128, 128), 128)
        query, key, value, grad = query_b[...], key_b[...], value_b[...], grad_b[...]
        back_q = back_k = back_v = jnp.zeros((slots, 128), jnp.float32)
        for head in range(2):
            low = probs[0, head]
            own = head_lanes(grad, head)
            back_v = back_v + right_mul(low, own)
            wide = low.astype(jnp.float32)
            slope = back_mul(value, own)
            inner = jnp.sum(wide * slope, axis=0, keepdims=True)
            pull = (wide * (slope - inner)).astype(jnp.bfloat16)
            back_q = back_q + left_mul(pull, head_lanes(key, head))
            back_k = back_k + right_mul(pull, head_lanes(query, head))
        grad_q[at, cols] = (back_q * (1.0 / math.sqrt(HEAD_DIM))).astype(jnp.bfloat16)
        grad_k[at, cols] = back_k.astype(jnp.bfloat16)
        grad_v[at, cols] = back_v.astype(jnp.bfloat16)

    for g in range(groups):
        @pl.when(step == plan.attention + strips * PAIRS_PER_PIECE * (g + 1) - 1)
        def _():
            whole = wholes[2 + ff_pieces + g]
            for n, grad in enumerate((grad_q, grad_k, grad_v)):
                part = grad[:, pl.ds(g * columns, columns)]
                whole[:, :, :, :, pl.ds(n * model, model), :] = rows_to_blocks(right_mul(turned[...], part))
                if n != 1:
                    small[2 + n // 2 : 3 + n // 2, pl.ds(g * columns, columns)] = jnp.sum(
                        part.astype(jnp.float32), axis=0, keepdims=True
                    )

    @pl.when(step >= plan.finish)
    def _():
        size = rows // FINISH
        at = pl.ds(pl.multiple_of((step - plan.finish) * size, size), size)
        grad = back_mul(grad_q[at, :], q_weight[...]) + back_mul(grad_k[at, :], k_weight[...])
        grad = grad + back_mul(grad_v[at, :], v_weight[...])
        xhat, scale = layer_norm_parts(tokens[...].astype(jnp.float32))
        back, gain_sum, bias_sum = layer_norm_back(grad, xhat, scale, vectors[0:1, :])
        grad_tokens[...] = grad_res[...] + back
        small[0:1, :] += gain_sum
        small[1:2, :] += bias_sum

    for when, wave in plan.waves.items():
        n, stage = wave[-1]
        pl.when(step == when)(functools.partial(jobs[n].ship, stage))

    @pl.when(step == plan.steps - 1)
    def _():
        vec_whole[...] = jnp.zeros_like(vec_whole)
        wide = bup_in.shape[1] // (width // model)
        for d in range(width // model):
            at = (d // (2 * dims[1] * dims[2]), d // (2 * dims[2]) % dims[1], d // 2 % dims[2], d % 2)
            vec_whole[at + (pl.ds(0, 8), pl.ds(0, model))] = small[:, d * model : (d + 1) * model]
            vec_whole[at + (pl.ds(8, 1), pl.ds(0, wide))] = bup_in[:, d * wide : (d + 1) * wide]
        late = list(plan.late)
        spread = max(1, len(late) // 5)
        left = None
        for k in range(5):
            take = late[k * spread : (k + 1) * spread] if k < 4 else late[4 * spread :]
            left = add_wave(jobs, take + [(last, k)]) if k < 4 else add_wave(jobs, take[:-1] + [(last, k)] + take[-1:])
            jobs[left[0]].ship(left[1])
        for job in jobs:
            job.finish()


def backward(dims, strips, turned, turned_two, out_grad, q_weight, k_weight, v_weight, vectors, small, grad_bup,
             grad_hidden, active, probs, queries, keys, values, grad_context, tokens, grad_res, grad_wo):
    width, rows = turned.shape
    ff = grad_hidden.shape[1]
    slots = rows // strips
    plan = Plan(dims, strips, rows, width, ff, SCATTER_LAG, SCATTER_GAP)
    n = 2 * dims[0] * dims[1] * dims[2]
    model, wide = width // n, ff // n
    lanes_wide = 128 * -(-wide // 128)
    full = functools.partial(jax.ShapeDtypeStruct, dtype=jnp.float32)
    vmem = pl.BlockSpec(memory_space=pltpu.VMEM)

    def part(step, first, count):
        return jnp.clip(step - first, 0, count - 1)

    def strip_pair(step):
        k = part(step, plan.attention, strips * plan.pairs)
        return lax.rem(k, strips), lax.div(k, strips)

    def probs_at(step):
        strip, pair = strip_pair(step)
        return (strip * plan.pairs + pair, 0, 0, 0)

    qkv = pl.BlockSpec((slots, 128), strip_pair)
    ending = pl.BlockSpec((rows // FINISH, width), lambda step: (part(step, plan.finish, FINISH), 0))
    shapes = plan.shapes
    bufs = []
    for k, shape in enumerate(shapes):
        bufs += reduce_scratch(dims, shape, jnp.bfloat16, 1 + k % 2)
    bufs += reduce_scratch(dims, (16, lanes_wide), jnp.float32, 1 + len(shapes) % 2)
    copies = scatter_copies(dims) * (len(shapes) + 1)
    return pl.pallas_call(
        functools.partial(backward_kernel, dims, plan, strips),
        grid=(plan.steps,),
        out_shape=[full((rows, width))] + [full((model, width))] * 4 + [full((model, ff)), full((wide, width)), full((16, lanes_wide))],
        in_specs=[vmem] * 9
        + [
            pl.BlockSpec((rows, FF_TILE), lambda step: (0, part(step, 0, plan.tiles))),
            pl.BlockSpec((rows, FF_TILE), lambda step: (0, part(step, plan.down, plan.tiles))),
            pl.BlockSpec((1, 2, slots, slots), probs_at),
            qkv, qkv, qkv, qkv, ending, ending,
            pl.BlockSpec(memory_space=pl.ANY),
        ],
        out_specs=[ending] + [vmem] * 7,
        scratch_shapes=[pltpu.VMEM((rows, width), jnp.bfloat16)] * 3
        + [pltpu.VMEM((8, width), jnp.float32), pltpu.VMEM(dims + (2, 16, lanes_wide), jnp.float32)]
        + [pltpu.VMEM(dims + (2,) + shape, jnp.bfloat16) for shape in plan.wholes]
        + bufs
        + [pltpu.SemaphoreType.DMA((1,)), pltpu.SemaphoreType.DMA((copies,)), pltpu.SemaphoreType.DMA((copies,))],
        compiler_params=pltpu.CompilerParams(collective_id=3, has_side_effects=True, vmem_limit_bytes=VMEM_LIMIT),
        name="backward",
    )(turned, turned_two, out_grad, q_weight, k_weight, v_weight, vectors, small, grad_bup,
      grad_hidden, active, probs, queries, keys, values, grad_context, tokens, grad_res, grad_wo)


def lane_pad(rows, width):
    return jnp.pad(rows, ((0, 0), (0, width - rows.shape[1])))


def pack_vectors(vectors, wide):
    width = 128 * -(-wide.shape[0] // 128)
    rows = lane_pad(jnp.stack(vectors).astype(jnp.float32), width)
    last = lane_pad(wide[None].astype(jnp.float32), width)
    return jnp.pad(jnp.concatenate([rows, last]), ((0, 15 - len(vectors)), (0, 0)))


def unpack_vectors(block, part, wide_part):
    flat = block.reshape((-1,) + block.shape[-2:])
    rows = flat[:, :8, :part].transpose(1, 0, 2).reshape(8, -1)
    return rows, flat[:, 8, :wide_part].reshape(1, -1)


def shards(
    dims,
    tokens,
    lengths,
    key_mask,
    ln1_gain,
    ln1_bias,
    q_weight,
    q_bias,
    k_weight,
    v_weight,
    v_bias,
    o_weight,
    o_bias,
    ln2_gain,
    ln2_bias,
    up_weight,
    up_bias,
    down_weight,
    down_bias,
    out_grad,
):
    early_weights, late_weights = (q_weight, k_weight, v_weight), (o_weight, up_weight, down_weight)
    vectors = (ln1_gain, ln1_bias, q_bias, v_bias, o_bias, ln2_gain, ln2_bias, down_bias)
    fused = q_weight.shape[0] % 8 == 0
    axes = ("gx", "gy")

    def whole(shard):
        return lax.all_gather(shard, axes, axis=0, tiled=True)

    if fused:
        *wide, packed = gather_all(dims, list(early_weights) + [pack_vectors(vectors, up_bias)])
        q_full, k_full, v_full = [w.reshape((-1,) + w.shape[-1:]) for w in wide]
        rows, up_bias_full = unpack_vectors(packed, ln1_gain.shape[0], up_bias.shape[0])
    else:
        q_full, k_full, v_full = [whole(w) for w in early_weights]
        rows = jnp.stack([whole(v) for v in vectors]).astype(jnp.float32)
        up_bias_full = whole(up_bias).astype(jnp.float32)[None]

    row_count, width = tokens.shape
    strips = lengths.shape[0]
    slots = row_count // strips
    extra = -slots % 16

    def padded(values):
        return jnp.pad(values.reshape(strips, slots, width), ((0, 0), (0, extra), (0, 0))).reshape(-1, width)

    def cropped(values):
        return values.reshape(strips, slots + extra, width)[:, :slots].reshape(row_count, width)

    slot_ids = lax.iota(jnp.int32, slots)
    visible = (slot_ids[None, :] == 0) | (slot_ids[None, :] < lengths[:, None]) & (key_mask == 1)
    mask = jnp.where(jnp.pad(visible, ((0, 0), (0, extra))), 0.0, NEG_FILL).reshape(-1, 1)
    tokens_in, grads_in = padded(tokens), padded(out_grad)

    turned, queries, keys, values, probs, context, *late = attend(
        dims, late_weights if fused else (), strips, tokens_in, q_full, k_full, v_full, rows, mask
    )
    if fused:
        o_full, up_full, down_full = [w.reshape((-1,) + w.shape[-1:]) for w in late]
    else:
        o_full, up_full, down_full = [whole(w) for w in late_weights]
    block_out, grad_res, grad_context, grad_wo, active, grad_hidden, turned_two, small, grad_bup = ffn(
        tokens_in, context, grads_in, o_full, up_full, down_full, rows, up_bias_full
    )
    if fused:
        grad_tokens, sum_wq, sum_wk, sum_wv, sum_wo, sum_wup, sum_wdown, least = backward(
            dims, strips, turned, turned_two, grads_in, q_full, k_full, v_full, rows, small, grad_bup,
            grad_hidden, active, probs, queries, keys, values, grad_context, tokens_in, grad_res,
            grad_wo.reshape(dims + (2,) + o_weight.shape),
        )
        vec = [least[n, : ln1_gain.shape[0]] for n in range(8)]
        sum_bup = least[8, : up_bias.shape[0]]
    else:
        grad_tokens, grad_wq, grad_wk, grad_wv, small_two = attend_back(
            strips, tokens_in, turned, queries, keys, values, probs, grad_context, grad_res, q_full, k_full, v_full, rows
        )
        small = small + small_two
        full = [grad_wq, grad_wk, grad_wv, grad_wo, right_mul(turned_two, grad_hidden), left_mul(active, grads_in), grad_bup[0]]
        full = [g.astype(jnp.float32) for g in full] + [small[n] for n in range(8)]
        sum_wq, sum_wk, sum_wv, sum_wo, sum_wup, sum_wdown, sum_bup, *vec = [
            lax.psum_scatter(g, axes, scatter_dimension=0, tiled=True) for g in full
        ]
    return (
        cropped(block_out), cropped(grad_tokens), vec[0], vec[1], sum_wq, vec[2], sum_wk, sum_wv, vec[3], sum_wo, vec[4],
        vec[5], vec[6], sum_wup, sum_bup, sum_wdown, vec[7],
    )


def solution(mesh):
    rows, flat = P(("gx", "gy"), None), P(("gx", "gy"))
    return jax.shard_map(
        functools.partial(shards, grid_of(mesh)),
        mesh=mesh,
        in_specs=(
            rows, flat, rows, flat, flat, rows, flat, rows, rows, flat, rows, flat, flat, flat, rows, flat, rows, flat, rows,
        ),
        out_specs=(
            rows, rows, flat, flat, rows, flat, rows, rows, flat, rows, flat, flat, flat, rows, flat, rows, flat,
        ),
        check_vma=False,
    )
```

```python
import functools
import math

import jax
import jax.numpy as jnp
from jax import lax
from jax.experimental import pallas as pl
from jax.experimental.pallas import tpu as pltpu
from jax.sharding import PartitionSpec as P

HEAD_DIM = 64
EPSILON = 1e-06
NEG_FILL = -1e30
VMEM_LIMIT = 63 * 1024 * 1024
GATHER_LAG = 12.0
GATHER_GAP = 5.0
SCATTER_LAG = 12.0
SCATTER_GAP = 6.0


def right_mul(left_arg, right_arg):
    return jnp.dot(left_arg, right_arg, preferred_element_type=jnp.float32)


def left_mul(left_arg, right_arg):
    return lax.dot_general(
        left_arg, right_arg, (((0,), (0,)), ((), ())), preferred_element_type=jnp.float32
    )


def back_mul(left_arg, right_arg):
    return lax.dot_general(
        left_arg, right_arg, (((1,), (1,)), ((), ())), preferred_element_type=jnp.float32
    )


MESH = pl.DeviceIdType.MESH


def grid_of(mesh):
    z_size, plane = mesh.shape["gx"], mesh.shape["gy"] // 2
    x_size = max(n for n in range(1, plane + 1) if plane % n == 0 and n * n <= plane)
    return z_size, plane // x_size, x_size


class Place:
    def __init__(self, dims):
        self.dims = dims
        g = lax.axis_index("gy")
        self.z = lax.axis_index("gx")
        self.c = lax.rem(g, 2)
        self.x = lax.rem(lax.div(g, 2), dims[2])
        self.y = lax.div(g, 2 * dims[2])

    def at(self, axis, step):
        here = (self.z, self.y, self.x)[axis]
        return lax.rem(here + step, self.dims[axis])

    def plane(self, first, step, other_step):
        a, b = self.at(first, step), self.at(3 - first, other_step)
        return (a, b) if first == 1 else (b, a)

    def device(self, axis, step):
        where = [self.z, self.y, self.x, self.c]
        if axis == 3:
            where[3] = 1 - self.c
        else:
            where[axis] = self.at(axis, step)
        return (where[0], (where[1] * self.dims[2] + where[2]) * 2 + where[3])

    def barrier(self):
        sem = pltpu.get_barrier_semaphore()
        peers = [(axis, step) for axis in range(3) for step in range(1, self.dims[axis])] + [(3, 1)]
        for axis, step in peers:
            pl.semaphore_signal(sem, inc=1, device_id=self.device(axis, step), device_id_type=MESH)
        pl.semaphore_wait(sem, len(peers))


class Lanes:
    def __init__(self, place, local, send, recv):
        self.place, self.local_sem, self.send, self.recv = place, local, send, recv
        self.used = self.local_used = 0

    def remote(self, src, dst, axis, step):
        n = self.used
        self.used += 1
        return pltpu.make_async_remote_copy(
            src_ref=src, dst_ref=dst, send_sem=self.send.at[n], recv_sem=self.recv.at[n],
            device_id=self.place.device(axis, step), device_id_type=MESH,
        )

    def local(self, src, dst):
        n = self.local_used
        self.local_used += 1
        return pltpu.make_async_copy(src, dst, self.local_sem.at[n])


def gather_copies(dims, z_last):
    z, y, x = dims
    if z_last:
        return (x * y - 1) + (z - 1) + z
    return (z - 1) + (x * y - 1) + x * y


class Gather:
    def __init__(self, lanes, shard, buf, first, z_last):
        p, dims = lanes.place, lanes.place.dims
        firsts, seconds = range(1, dims[first]), range(1, dims[3 - first])
        own = buf.at[p.z, p.y, p.x, p.c]
        local = lanes.local(shard, own)
        remote = lanes.remote

        def cell(step, other):
            y, x = p.plane(first, step, other)
            return buf.at[p.z, y, x, p.c] if z_last else buf.at[:, y, x, p.c]

        def layer(step):
            return buf.at[p.at(0, step), :, :, p.c]

        mine = shard if z_last else cell(0, 0)
        to_first = [remote(mine, cell(0, 0), first, s) for s in firsts]
        to_second = [remote(mine, cell(0, 0), 3 - first, t) for t in seconds]
        onward = [remote(cell(s, 0), cell(s, 0), 3 - first, t) for s in firsts for t in seconds]
        if z_last:
            along_z = [remote(layer(0), layer(0), 0, s) for s in range(1, dims[0])]
            cores = [remote(layer(s), layer(s), 3, 1) for s in range(dims[0])]
            self.stages = [
                ([], [], to_first + to_second + [local]),
                ([], to_first, onward),
                ([local], to_second + onward, along_z + cores[:1]),
                ([], along_z, cores[1:]),
            ]
        else:
            along_z = [remote(shard, own, 0, s) for s in range(1, dims[0])]
            core = {(s, t): remote(cell(s, t), cell(s, t), 3, 1) for s in range(dims[first]) for t in range(dims[3 - first])}
            cores = list(core.values())
            self.stages = [
                ([], [], along_z + [local]),
                ([local], along_z, to_first + to_second + [core[0, 0]]),
                ([], to_first, onward + [core[s, 0] for s in firsts]),
                ([], to_second + onward, [core[s, t] for s in range(dims[first]) for t in seconds]),
            ]
        self.handed = cores
        self.remotes = to_first + to_second + onward + along_z + cores

    def run(self, stage):
        done, arrived, starts = self.stages[stage]
        for copy in done:
            copy.wait()
        for copy in arrived:
            copy.wait_recv()
        for copy in starts:
            copy.start()

    def arrive(self):
        for copy in self.handed:
            copy.wait_recv()

    def finish(self):
        for copy in self.remotes:
            copy.wait_send()


def scatter_copies(dims):
    z, y, x = dims
    return 1 + (z - 1) + (x * y - 1)


def pieces_of(shapes, narrow):
    pieces = []
    for n, shape in enumerate(shapes):
        parts = max(1, shape[-1] // 768)
        if parts == 1 and shape[-2] > narrow and shape[-1] == 768:
            parts = 3
        for k in range(parts):
            size = shape[-1] // parts
            pieces.append((n, k * size, size, 1 + len(pieces) % 2))
    return pieces


def waves(count, stages):
    return [[(b + 1 - s, s) for s in range(1, stages) if 0 <= b + 1 - s < count] for b in range(count + stages - 2)]


def gather_jobs(lanes, pieces, shards, bufs):
    return [
        Gather(lanes, shards[n].at[:, pl.ds(at, size)], bufs[n].at[:, :, :, :, :, pl.ds(at, size)], first, False)
        for n, at, size, first in pieces
    ]


def comm_semaphores(pieces, copies):
    return [
        pltpu.SemaphoreType.DMA((len(pieces),)),
        pltpu.SemaphoreType.DMA((copies * len(pieces),)),
        pltpu.SemaphoreType.DMA((copies * len(pieces),)),
    ]


def run_wave(jobs, wave):
    for n, stage in wave:
        jobs[n].run(stage)


def layer_norm_parts(values):
    center = values - jnp.mean(values, axis=-1, keepdims=True)
    scale = lax.rsqrt(jnp.mean(center * center, axis=-1, keepdims=True) + EPSILON)
    return center * scale, scale


def layer_norm_back(grad, xhat, scale, gain):
    scaled = grad * gain
    inner = scaled - jnp.mean(scaled, axis=-1, keepdims=True)
    back = scale * (inner - xhat * jnp.mean(scaled * xhat, axis=-1, keepdims=True))
    return back, jnp.sum(grad * xhat, axis=0, keepdims=True), jnp.sum(grad, axis=0, keepdims=True)


def gelu_and_slope(v):
    size = jnp.abs(v)
    t = 1.0 / (1.0 + (0.3275911 * math.sqrt(0.5)) * size)
    bell = jnp.exp(-0.5 * v * v)
    poly = ((((0.5 * 1.061405429) * t - 0.5 * 1.453152027) * t + 0.5 * 1.421413741) * t - 0.5 * 0.284496736) * t
    tail = (poly + 0.5 * 0.254829592) * t * bell
    share = jnp.where(v >= 0, 1.0 - tail, tail)
    return v * share, share + (v * (1.0 / math.sqrt(2.0 * math.pi))) * bell


def ffn_kernel(
    a_rows, b_rows, ff_tile, c_rows,
    tokens, context, out_grad, o_weight, up_weight, down_weight, vectors, up_bias,
    block_out, grad_res, grad_context, grad_wo, active, grad_hidden, normed2_t, small, grad_bup,
    normed2, grad_att,
):
    rows, width = tokens.shape
    ff = up_weight.shape[1]
    o_bias, gain, bias, down_bias = vectors[4:5, :], vectors[5:6, :], vectors[6:7, :], vectors[7:8, :]
    small[...] = jnp.zeros_like(small)

    def attended(n, carry):
        at = pl.ds(pl.multiple_of(n * a_rows, a_rows), a_rows)
        residual = tokens[at, :].astype(jnp.float32) + right_mul(context[at, :], o_weight[...]) + o_bias
        grad_res[at, :] = residual
        xhat, _ = layer_norm_parts(residual)
        normed2[at, :] = (xhat * gain + bias).astype(jnp.bfloat16)
        return carry

    lax.fori_loop(0, rows // a_rows, attended, 0)

    def hidden_tile(n, carry):
        cols = pl.ds(pl.multiple_of(n * ff_tile, ff_tile), ff_tile)
        sums = jnp.zeros((1, ff_tile), jnp.float32)

        def piece(m, sums):
            at = pl.ds(pl.multiple_of(m * b_rows, b_rows), b_rows)
            hidden = right_mul(normed2[at, :], up_weight[:, cols]) + up_bias[:, cols]
            grad_active = back_mul(out_grad[at, :], down_weight[cols, :])
            value, slope = gelu_and_slope(hidden)
            active[at, cols] = value.astype(jnp.bfloat16)
            back = (slope * grad_active).astype(jnp.bfloat16)
            grad_hidden[at, cols] = back
            return sums + jnp.sum(back.astype(jnp.float32), axis=0, keepdims=True)

        grad_bup[:, cols] = lax.fori_loop(0, rows // b_rows, piece, sums)
        return carry

    lax.fori_loop(0, ff // ff_tile, hidden_tile, 0)

    def finish(n, carry):
        at = pl.ds(pl.multiple_of(n * c_rows, c_rows), c_rows)
        residual = grad_res[at, :]
        cotangent = out_grad[at, :].astype(jnp.float32)
        block_out[at, :] = (residual + right_mul(active[at, :], down_weight[...]) + down_bias).astype(jnp.bfloat16)
        grad = back_mul(grad_hidden[at, :], up_weight[...])
        xhat, scale = layer_norm_parts(residual)
        back, gain_sum, bias_sum = layer_norm_back(grad, xhat, scale, gain)
        total = cotangent + back
        grad_res[at, :] = total
        low = total.astype(jnp.bfloat16)
        grad_att[at, :] = low
        grad_context[at, :] = back_mul(low, o_weight[...]).astype(jnp.bfloat16)
        small[4:5, :] += jnp.sum(low.astype(jnp.float32), axis=0, keepdims=True)
        small[5:6, :] += gain_sum
        small[6:7, :] += bias_sum
        small[7:8, :] += jnp.sum(cotangent, axis=0, keepdims=True)
        return carry

    lax.fori_loop(0, rows // c_rows, finish, 0)

    normed2_t[...] = normed2[...].T
    grad_wo[...] = left_mul(context[...], grad_att[...]).astype(jnp.bfloat16)


def ffn(tokens, context, out_grad, o_weight, up_weight, down_weight, vectors, up_bias):
    rows, width = tokens.shape
    ff = up_weight.shape[1]
    low = functools.partial(jax.ShapeDtypeStruct, dtype=jnp.bfloat16)
    full = functools.partial(jax.ShapeDtypeStruct, dtype=jnp.float32)
    vmem = pl.BlockSpec(memory_space=pltpu.VMEM)
    return pl.pallas_call(
        functools.partial(ffn_kernel, rows, rows, 1024, rows // 2),
        out_shape=[
            low((rows, width)), full((rows, width)), low((rows, width)),
            low((width, width)), low((rows, ff)), low((rows, ff)), low((width, rows)), full((8, width)), full((1, ff)),
        ],
        in_specs=[vmem] * 8,
        out_specs=[vmem] * 9,
        scratch_shapes=[pltpu.VMEM((rows, width), jnp.bfloat16)] * 2,
        compiler_params=pltpu.CompilerParams(vmem_limit_bytes=VMEM_LIMIT),
        name="ffn",
    )(tokens, context, out_grad, o_weight, up_weight, down_weight, vectors, up_bias)


def head_lanes(pair, head):
    lane = lax.broadcasted_iota(jnp.int32, pair.shape, 1)
    return jnp.where(lax.div(lane, HEAD_DIM) == head, pair, jnp.zeros_like(pair))


def attend_pair(strips, step, mask, queries, keys, values, probs, context):
    rows, width = queries.shape
    slots, pairs = rows // strips, width // 128
    at = pl.ds(pl.multiple_of(lax.div(step, pairs) * slots, slots), slots)
    cols = pl.ds(pl.multiple_of(lax.rem(step, pairs) * 128, 128), 128)
    query, key, value = queries[at, cols], keys[at, cols], values[at, cols]
    hidden = mask[at, 0:1]
    total = jnp.zeros((slots, 128), jnp.float32)
    for head in range(2):
        scores = back_mul(key, head_lanes(query, head)) + hidden
        powers = jnp.exp(scores - jnp.max(scores, axis=0, keepdims=True))
        low = (powers * (1.0 / jnp.sum(powers, axis=0, keepdims=True))).astype(jnp.bfloat16)
        probs[0, head] = low
        total = total + left_mul(low, head_lanes(value, head))
    context[at, cols] = total.astype(jnp.bfloat16)


def attend_kernel(strips, tokens, q_weight, k_weight, v_weight, vectors, mask, turned, queries, keys, values, probs, context, normed):
    rows, width = tokens.shape
    slots, pairs = rows // strips, width // 128
    step = pl.program_id(0)

    @pl.when(step == 0)
    def _():
        xhat, _ = layer_norm_parts(tokens[...].astype(jnp.float32))
        normed[...] = (xhat * vectors[0:1, :] + vectors[1:2, :]).astype(jnp.bfloat16)
        turned[...] = normed[...].T
        scale = 1.0 / math.sqrt(HEAD_DIM)
        low = (right_mul(normed[...], q_weight[...]) + vectors[2:3, :]).astype(jnp.bfloat16)
        queries[...] = low * jnp.bfloat16(scale)
        keys[...] = right_mul(normed[...], k_weight[...]).astype(jnp.bfloat16)
        values[...] = (right_mul(normed[...], v_weight[...]) + vectors[3:4, :]).astype(jnp.bfloat16)

    attend_pair(strips, step, mask, queries, keys, values, probs, context)


def attend(strips, tokens, q_weight, k_weight, v_weight, vectors, mask):
    rows, width = tokens.shape
    slots, pairs = rows // strips, width // 128
    low = functools.partial(jax.ShapeDtypeStruct, dtype=jnp.bfloat16)
    return pl.pallas_call(
        functools.partial(attend_kernel, strips),
        grid=(strips * pairs,),
        out_shape=[low((width, rows))] + [low((rows, width))] * 3 + [low((strips * pairs, 2, slots, slots)), low((rows, width))],
        in_specs=[pl.BlockSpec(memory_space=pltpu.VMEM)] * 6,
        out_specs=[pl.BlockSpec(memory_space=pltpu.VMEM)] * 4
        + [pl.BlockSpec((1, 2, slots, slots), lambda n: (n, 0, 0, 0)), pl.BlockSpec(memory_space=pltpu.VMEM)],
        scratch_shapes=[pltpu.VMEM((rows, width), jnp.bfloat16)],
        compiler_params=pltpu.CompilerParams(vmem_limit_bytes=VMEM_LIMIT),
        name="attend",
    )(tokens, q_weight, k_weight, v_weight, vectors, mask)


def attend_back_kernel(
    strips, tokens, turned, queries, keys, values, probs, grad_context, grad_res, q_weight, k_weight, v_weight, vectors,
    grad_tokens, grad_wq, grad_wk, grad_wv, small,
    grad_q, grad_k, grad_v,
):
    rows, width = tokens.shape
    slots, pairs = rows // strips, width // 128
    step = pl.program_id(0)
    at = pl.ds(pl.multiple_of(lax.div(step, pairs) * slots, slots), slots)
    cols = pl.ds(pl.multiple_of(lax.rem(step, pairs) * 128, 128), 128)
    query, key, value, grad = queries[at, cols], keys[at, cols], values[at, cols], grad_context[at, cols]
    back_q = back_k = back_v = jnp.zeros((slots, 128), jnp.float32)
    for head in range(2):
        low = probs[0, head]
        own = head_lanes(grad, head)
        back_v = back_v + right_mul(low, own)
        wide = low.astype(jnp.float32)
        slope = back_mul(value, own)
        inner = jnp.sum(wide * slope, axis=0, keepdims=True)
        pull = (wide * (slope - inner)).astype(jnp.bfloat16)
        back_q = back_q + left_mul(pull, head_lanes(key, head))
        back_k = back_k + right_mul(pull, head_lanes(query, head))
    grad_q[at, cols] = (back_q * (1.0 / math.sqrt(HEAD_DIM))).astype(jnp.bfloat16)
    grad_k[at, cols] = back_k.astype(jnp.bfloat16)
    grad_v[at, cols] = back_v.astype(jnp.bfloat16)

    @pl.when(step == strips * pairs - 1)
    def _():
        grad_wq[...] = right_mul(turned[...], grad_q[...]).astype(jnp.bfloat16)
        grad_wk[...] = right_mul(turned[...], grad_k[...]).astype(jnp.bfloat16)
        grad_wv[...] = right_mul(turned[...], grad_v[...]).astype(jnp.bfloat16)
        small[...] = jnp.zeros_like(small)
        small[2:3, :] = jnp.sum(grad_q[...].astype(jnp.float32), axis=0, keepdims=True)
        small[3:4, :] = jnp.sum(grad_v[...].astype(jnp.float32), axis=0, keepdims=True)

        def finish(n, carry):
            at = pl.ds(pl.multiple_of(n * slots, slots), slots)
            grad = back_mul(grad_q[at, :], q_weight[...]) + back_mul(grad_k[at, :], k_weight[...])
            grad = grad + back_mul(grad_v[at, :], v_weight[...])
            xhat, scale = layer_norm_parts(tokens[at, :].astype(jnp.float32))
            back, gain_sum, bias_sum = layer_norm_back(grad, xhat, scale, vectors[0:1, :])
            grad_tokens[at, :] = grad_res[at, :] + back
            small[0:1, :] += gain_sum
            small[1:2, :] += bias_sum
            return carry

        lax.fori_loop(0, strips, finish, 0)


def attend_back(strips, tokens, turned, queries, keys, values, probs, grad_context, grad_res, q_weight, k_weight, v_weight, vectors):
    rows, width = tokens.shape
    slots, pairs = rows // strips, width // 128
    low = functools.partial(jax.ShapeDtypeStruct, dtype=jnp.bfloat16)
    full = functools.partial(jax.ShapeDtypeStruct, dtype=jnp.float32)
    vmem = pl.BlockSpec(memory_space=pltpu.VMEM)
    block = pl.BlockSpec((1, 2, slots, slots), lambda n: (n, 0, 0, 0))
    return pl.pallas_call(
        functools.partial(attend_back_kernel, strips),
        grid=(strips * pairs,),
        out_shape=[full((rows, width)), low((width, width)), low((width, width)), low((width, width)), full((8, width))],
        in_specs=[vmem] * 5 + [block] + [vmem] * 6,
        out_specs=[vmem] * 5,
        scratch_shapes=[pltpu.VMEM((rows, width), jnp.bfloat16)] * 3,
        compiler_params=pltpu.CompilerParams(vmem_limit_bytes=VMEM_LIMIT),
        name="attend_back",
    )(tokens, turned, queries, keys, values, probs, grad_context, grad_res, q_weight, k_weight, v_weight, vectors)


def forward_plan(sizes, early, steps, lag, gap):
    project, attend = 5.0, 2.3
    events, start = [], 0.0
    for n, size in enumerate(sizes):
        start = start + gap * size
        events += [(start + 2.0 + lag * (k - 1), k, n) for k in range(1, 4)]
    events.sort()
    first = max(k for k, (_, _, n) in enumerate(events) if n < early) + 1
    begin = events[first - 1][0] + project
    plan, late = {0: [(n, k) for _, k, n in events[:first]]}, []
    for when, k, n in events[first:]:
        fits = [s for s in range(1, steps) if begin + attend * (s - 1) >= when]
        plan.setdefault(fits[0], []).append((n, k)) if fits else late.append((n, k))
    return plan, late


def forward_kernel(dims, pieces, early, plan, late, strips, tokens, mask, *refs):
    count = early + 3
    shards, refs = refs[:count], refs[count:]
    (turned, heads, probs, context), refs = refs[:4], refs[4:]
    queries, keys, values = heads.at[0], heads.at[1], heads.at[2]
    weights, (vectors, up_bias), bufs, refs = refs[: early - 1], refs[early - 1 : early + 1], refs[early + 1 : early + 4], refs[early + 4 :]
    near, normed, sems = refs[:early], refs[early], refs[early + 1 :]
    rows, width = tokens.shape
    slots, pairs = rows // strips, width // 128
    step = pl.program_id(0)
    place = Place(dims)
    jobs = gather_jobs(Lanes(place, *sems), pieces, shards, list(near) + list(bufs))

    @pl.when(step == 0)
    def _():
        place.barrier()
        for job in jobs:
            job.run(0)
        xhat, _ = layer_norm_parts(tokens[...].astype(jnp.float32))
        run_wave(jobs, plan[0])
        for job in jobs[:early]:
            job.arrive()
        model, wide = shards[1].shape[0], up_bias.shape[1] // (width // shards[1].shape[0])
        for d in range(width // model):
            at = (d // (2 * dims[1] * dims[2]), d // (2 * dims[2]) % dims[1], d // 2 % dims[2], d % 2)
            vectors[:, d * model : (d + 1) * model] = near[0][at + (pl.ds(0, 8), pl.ds(0, model))]
            up_bias[:, d * wide : (d + 1) * wide] = near[0][at + (pl.ds(8, 1), pl.ds(0, wide))]
        for whole, buf in zip(weights, near[1:]):
            whole[...] = buf[...].astype(jnp.float32).reshape(width, width).astype(jnp.bfloat16)
        q_weight, k_weight, v_weight = weights
        normed[...] = (xhat * vectors[0:1, :] + vectors[1:2, :]).astype(jnp.bfloat16)
        turned[...] = normed[...].T
        scale = 1.0 / math.sqrt(HEAD_DIM)
        low = (right_mul(normed[...], q_weight[...]) + vectors[2:3, :]).astype(jnp.bfloat16)
        queries[...] = low * jnp.bfloat16(scale)
        keys[...] = right_mul(normed[...], k_weight[...]).astype(jnp.bfloat16)
        values[...] = (right_mul(normed[...], v_weight[...]) + vectors[3:4, :]).astype(jnp.bfloat16)

    for when, wave in plan.items():
        if when:
            pl.when(step == when)(functools.partial(run_wave, jobs, wave))

    attend_pair(strips, step, mask, queries, keys, values, probs, context)

    @pl.when(step == strips * pairs - 1)
    def _():
        run_wave(jobs, late)
        for job in jobs[early:]:
            job.arrive()
        for job in jobs:
            job.finish()


def forward(dims, strips, tokens, mask, packed, early_shards, late_shards):
    rows, width = tokens.shape
    slots, pairs = rows // strips, width // 128
    shards = [packed] + list(early_shards) + list(late_shards)
    early = 1 + len(early_shards)
    model = early_shards[0].shape[0]
    ff = late_shards[1].shape[1]
    low = functools.partial(jax.ShapeDtypeStruct, dtype=jnp.bfloat16)
    full = functools.partial(jax.ShapeDtypeStruct, dtype=jnp.float32)
    vmem = pl.BlockSpec(memory_space=pltpu.VMEM)
    pieces = pieces_of([s.shape for s in shards], model)
    sizes = [shards[n].shape[0] * size * shards[n].dtype.itemsize / (model * width * 2) for n, _, size, _ in pieces]
    plan, late = forward_plan(sizes, early, strips * pairs, GATHER_LAG, GATHER_GAP)
    return pl.pallas_call(
        functools.partial(forward_kernel, dims, pieces, early, plan, late, strips),
        grid=(strips * pairs,),
        out_shape=[low((width, rows))]
        + [low((3, rows, width))]
        + [low((strips * pairs, 2, slots, slots)), low((rows, width))]
        + [low((width, width))] * len(early_shards)
        + [full((8, width)), full((1, ff))]
        + [low(dims + (2,) + s.shape) for s in late_shards],
        in_specs=[vmem] * (2 + len(shards)),
        out_specs=[vmem] * 2
        + [pl.BlockSpec((1, 2, slots, slots), lambda n: (n, 0, 0, 0)), vmem]
        + [vmem] * (early + 1)
        + [pl.BlockSpec(memory_space=pl.ANY)] * 3,
        scratch_shapes=[pltpu.VMEM(dims + (2,) + s.shape, s.dtype) for s in shards[:early]]
        + [pltpu.VMEM((rows, width), jnp.bfloat16)]
        + comm_semaphores(pieces, gather_copies(dims, False)),
        compiler_params=pltpu.CompilerParams(vmem_limit_bytes=VMEM_LIMIT, collective_id=2, has_side_effects=True),
        name="forward",
    )(tokens, mask, *shards)


class Reduce:
    def __init__(self, lanes, whole, bufs, first, write):
        p, dims = lanes.place, lanes.place.dims
        self.p, self.dims, self.first, self.write = p, dims, first, write
        self.firsts, self.seconds = range(1, dims[first]), range(1, dims[3 - first])
        self.from_core, self.from_far, self.from_first, self.from_second, self.from_z = bufs
        self.mine, remote = whole.at[:, :, :, p.c], lanes.remote

        def cell(step, other):
            y, x = p.plane(first, step, other)
            return whole.at[:, y, x, p.c]

        core = [remote(whole.at[:, :, :, 1 - p.c], self.from_core, 3, 1)]
        self.far = [remote(cell(s, t), self.from_far.at[s - 1, t - 1], first, s) for s in self.firsts for t in self.seconds]
        self.to_first = [remote(cell(s, 0), self.from_first.at[s - 1], first, s) for s in self.firsts]
        self.to_second = [remote(cell(0, t), self.from_second.at[t - 1], 3 - first, t) for t in self.seconds]
        along_z = [
            remote(whole.at[p.at(0, s), p.y, p.x, p.c], self.from_z.at[s - 1], 0, s) for s in range(1, dims[0])
        ]
        self.ships = [core, self.far + self.to_first, self.to_second, along_z]

    def total(self, at, terms):
        total = self.mine[at].astype(jnp.float32)
        for ref, index in terms:
            total = total + ref[index].astype(jnp.float32)
        return total

    def add(self, at, terms):
        self.mine[at] = self.total(at, terms).astype(self.mine.dtype)

    def run(self, stage):
        p, (z_size, y_size, x_size) = self.p, self.dims
        arrivals = (self.ships[0], self.far, self.to_first + self.to_second, self.ships[3])[stage - 1]
        for copy in arrivals:
            copy.wait_recv()
        if stage == 1:
            def body(n, carry):
                at = (lax.div(n, y_size * x_size), lax.rem(lax.div(n, x_size), y_size), lax.rem(n, x_size))
                self.add(at, [(self.from_core, at)])
                return carry

            lax.fori_loop(0, z_size * y_size * x_size, body, 0)
        elif stage == 2:
            for z in range(z_size):
                for t in self.seconds:
                    self.add((z,) + p.plane(self.first, 0, t), [(self.from_far, (s - 1, t - 1, z)) for s in self.firsts])
        elif stage == 3:
            for z in range(z_size):
                terms = [(self.from_first, (s - 1, z)) for s in self.firsts]
                self.add((z, p.y, p.x), terms + [(self.from_second, (t - 1, z)) for t in self.seconds])
        else:
            self.write(self.total((p.z, p.y, p.x), [(self.from_z, (s,)) for s in range(z_size - 1)]))

    def ship(self, stage):
        if stage < 4:
            for copy in self.ships[stage]:
                copy.start()

    def finish(self):
        for copies in self.ships:
            for copy in copies:
                copy.wait_send()


def reduce_scratch(dims, shape, dtype, first):
    z, y, x = dims
    f, s = max(dims[first] - 1, 1), max(dims[3 - first] - 1, 1)
    leads = [(z, y, x), (f, s, z), (f, z), (s, z), (max(z - 1, 1),)]
    return [pltpu.VMEM(lead + shape, dtype) for lead in leads]


def add_wave(jobs, wave):
    left = None
    for n, stage in wave:
        if stage:
            jobs[n].run(stage)
        if left:
            jobs[left[0]].ship(left[1])
        left = (n, stage)
    return left


FF_TILE = 384
FINISH = 4
PAIRS_PER_PIECE = 2


class Plan:
    def __init__(self, dims, strips, rows, width, ff, lag, gap):
        self.tiles, self.pairs = ff // FF_TILE, width // 128
        self.attention = self.tiles
        self.finish = self.attention + strips * self.pairs
        self.steps = self.finish + FINISH
        n = 2 * dims[0] * dims[1] * dims[2]
        model, wide = width // n, ff // n
        per_up = width // FF_TILE
        lasts = [0] + [per_up * (k + 1) for k in range(ff // width)] + [self.attention] * 3
        groups = self.pairs // PAIRS_PER_PIECE
        lasts += [self.attention + strips * PAIRS_PER_PIECE * (g + 1) for g in range(groups)]
        self.wholes = [((), (model, width)), ((ff // width,), (model, width)), ((), (wide, width))]
        self.wholes += [((groups,), (3 * model, width // groups))]
        self.shapes = [(model, width)] * (1 + ff // width) + [(wide, width // 3)] * 3 + [(3 * model, width // groups)] * groups
        ends = [2.6] * self.attention + [3.2] * (strips * self.pairs) + [1.6] * FINISH
        starts = [sum(ends[:k]) for k in range(self.steps)]
        events, free = [], 0.0
        for piece, step in enumerate(lasts):
            begin = max(starts[step], free)
            free = begin + gap
            events += [(starts[step], 0, piece, step)]
            events += [(begin + 2.0 + lag * (k - 1), k, piece, 0) for k in range(1, 5)]
        self.waves, self.late = {}, []
        for when, stage, piece, step in sorted(events):
            fits = [k for k in range(self.steps) if starts[k] >= when and k >= step]
            if fits:
                self.waves.setdefault(fits[0], []).append((piece, stage))
            else:
                self.late.append((piece, stage))


def by_step(step, table):
    keys = sorted(table)

    def pick(low, high):
        if high - low == 1:
            pl.when(step == keys[low])(table[keys[low]])
            return
        middle = (low + high) // 2
        lax.cond(step < keys[middle], lambda: pick(low, middle), lambda: pick(middle, high))

    pick(0, len(keys))


def backward_kernel(dims, plan, strips, *refs):
    (turned, turned_two, out_grad, q_weight, k_weight, v_weight, vectors, small_in, bup_in) = refs[:9]
    (grad_hidden, active, probs, heads, grad_b, tokens, grad_res, wo_hbm) = refs[9:17]
    (grad_tokens, sum_q, sum_k, sum_v, sum_o, sum_up, sum_down, sum_vec) = refs[17:25]
    refs = refs[25:]
    grad_q, grad_k, grad_v, small, vec_whole, o_whole, up_whole, down_whole, qkv_whole = refs[:9]
    refs = refs[9:]
    local, send, recv = refs[-3:]
    width, rows = turned.shape
    slots, ff_pieces, groups = rows // strips, up_whole.shape[0], qkv_whole.shape[0]
    step = pl.program_id(0)
    place = Place(dims)
    lanes = Lanes(place, local, send, recv)
    o_copy = lanes.local(wo_hbm, o_whole)

    model = sum_q.shape[0]
    columns = width // groups

    def write_to(ref, at, size):
        def write(total):
            ref[:, pl.ds(at, size)] = total
        return write

    def write_group(g):
        def write(total):
            for n, ref in enumerate((sum_q, sum_k, sum_v)):
                ref[:, pl.ds(g * columns, columns)] = total[n * model : (n + 1) * model]
        return write

    third = width // 3
    views = [(o_whole, write_to(sum_o, 0, width))]
    views += [(up_whole.at[k], write_to(sum_up, k * width, width)) for k in range(ff_pieces)]
    views += [
        (down_whole.at[:, :, :, :, :, pl.ds(k * third, third)], write_to(sum_down, k * third, third)) for k in range(3)
    ]
    views += [(qkv_whole.at[g], write_group(g)) for g in range(groups)]
    views += [(vec_whole, write_to(sum_vec, 0, sum_vec.shape[1]))]
    jobs = [Reduce(lanes, whole, refs[5 * n : 5 * n + 5], 1 + n % 2, write) for n, (whole, write) in enumerate(views)]
    last = len(jobs) - 1

    @pl.when(step == 0)
    def _():
        place.barrier()
        o_copy.start()
        small[...] = small_in[...]
        o_copy.wait()

    by_step(step, {when: lambda wave=wave: add_wave(jobs, wave) and None for when, wave in plan.waves.items()})

    def rows_to_blocks(product):
        n = 2 * dims[0] * dims[1] * dims[2]
        return product.reshape(dims + (2, product.shape[0] // n, product.shape[1])).astype(jnp.bfloat16)

    @pl.when(step < plan.attention)
    def _():
        per = width // FF_TILE
        part = pl.ds(pl.multiple_of(lax.rem(step, per) * FF_TILE, FF_TILE), FF_TILE)
        up_whole[lax.div(step, per), :, :, :, :, :, part] = rows_to_blocks(right_mul(turned_two[...], grad_hidden[...]))
        product = left_mul(active[...], out_grad[...])
        wide = down_whole.shape[4]
        for b in range(FF_TILE // wide):
            d = step * (FF_TILE // wide) + b
            y_x = lax.div(d, 2)
            at = (lax.div(y_x, dims[1] * dims[2]), lax.rem(lax.div(y_x, dims[2]), dims[1]), lax.rem(y_x, dims[2]), lax.rem(d, 2))
            down_whole[at] = product[b * wide : (b + 1) * wide].astype(jnp.bfloat16)

    pair, strip = lax.div(step - plan.attention, strips), lax.rem(step - plan.attention, strips)
    in_attention = (step >= plan.attention) & (step < plan.finish)

    @pl.when(in_attention)
    def _():
        at = pl.ds(pl.multiple_of(strip * slots, slots), slots)
        cols = pl.ds(pl.multiple_of(pair * 128, 128), 128)
        query, key, value, grad = heads[0], heads[1], heads[2], grad_b[...]
        back_q = back_k = back_v = jnp.zeros((slots, 128), jnp.float32)
        for head in range(2):
            low = probs[0, head]
            own = head_lanes(grad, head)
            back_v = back_v + right_mul(low, own)
            wide = low.astype(jnp.float32)
            slope = back_mul(value, own)
            inner = jnp.sum(wide * slope, axis=0, keepdims=True)
            pull = (wide * (slope - inner)).astype(jnp.bfloat16)
            back_q = back_q + left_mul(pull, head_lanes(key, head))
            back_k = back_k + right_mul(pull, head_lanes(query, head))
        grad_q[at, cols] = (back_q * (1.0 / math.sqrt(HEAD_DIM))).astype(jnp.bfloat16)
        grad_k[at, cols] = back_k.astype(jnp.bfloat16)
        grad_v[at, cols] = back_v.astype(jnp.bfloat16)

    group_steps = strips * PAIRS_PER_PIECE

    @pl.when(in_attention & (lax.rem(step - plan.attention, group_steps) == group_steps - 1))
    def _():
        g = lax.div(step - plan.attention, group_steps)
        cols = pl.ds(pl.multiple_of(g * columns, columns), columns)
        for n, grad in enumerate((grad_q, grad_k, grad_v)):
            part = grad[:, cols]
            qkv_whole[g, :, :, :, :, pl.ds(n * model, model), :] = rows_to_blocks(right_mul(turned[...], part))
            if n != 1:
                small[2 + n // 2 : 3 + n // 2, cols] = jnp.sum(part.astype(jnp.float32), axis=0, keepdims=True)

    @pl.when(step >= plan.finish)
    def _():
        size = rows // FINISH
        at = pl.ds(pl.multiple_of((step - plan.finish) * size, size), size)
        grad = back_mul(grad_q[at, :], q_weight[...]) + back_mul(grad_k[at, :], k_weight[...])
        grad = grad + back_mul(grad_v[at, :], v_weight[...])
        xhat, scale = layer_norm_parts(tokens[...].astype(jnp.float32))
        back, gain_sum, bias_sum = layer_norm_back(grad, xhat, scale, vectors[0:1, :])
        grad_tokens[...] = grad_res[...] + back
        small[0:1, :] += gain_sum
        small[1:2, :] += bias_sum

    by_step(step, {when: functools.partial(jobs[wave[-1][0]].ship, wave[-1][1]) for when, wave in plan.waves.items()})

    @pl.when(step == plan.steps - 1)
    def _():
        vec_whole[...] = jnp.zeros_like(vec_whole)
        wide = bup_in.shape[1] // (width // model)
        for d in range(width // model):
            at = (d // (2 * dims[1] * dims[2]), d // (2 * dims[2]) % dims[1], d // 2 % dims[2], d % 2)
            vec_whole[at + (pl.ds(0, 8), pl.ds(0, model))] = small[:, d * model : (d + 1) * model]
            vec_whole[at + (pl.ds(8, 1), pl.ds(0, wide))] = bup_in[:, d * wide : (d + 1) * wide]
        late = list(plan.late)
        spread = max(1, len(late) // 5)
        left = None
        for k in range(5):
            take = late[k * spread : (k + 1) * spread] if k < 4 else late[4 * spread :]
            left = add_wave(jobs, take + [(last, k)]) if k < 4 else add_wave(jobs, take[:-1] + [(last, k)] + take[-1:])
            jobs[left[0]].ship(left[1])
        for job in jobs:
            job.finish()


def backward(dims, strips, turned, turned_two, out_grad, q_weight, k_weight, v_weight, vectors, small, grad_bup,
             grad_hidden, active, probs, heads, grad_context, tokens, grad_res, grad_wo):
    width, rows = turned.shape
    ff = grad_hidden.shape[1]
    slots = rows // strips
    plan = Plan(dims, strips, rows, width, ff, SCATTER_LAG, SCATTER_GAP)
    n = 2 * dims[0] * dims[1] * dims[2]
    model, wide = width // n, ff // n
    lanes_wide = 128 * -(-wide // 128)
    full = functools.partial(jax.ShapeDtypeStruct, dtype=jnp.float32)
    vmem = pl.BlockSpec(memory_space=pltpu.VMEM)

    def part(step, first, count):
        return jnp.clip(step - first, 0, count - 1)

    def strip_pair(step):
        k = part(step, plan.attention, strips * plan.pairs)
        return lax.rem(k, strips), lax.div(k, strips)

    def probs_at(step):
        strip, pair = strip_pair(step)
        return (strip * plan.pairs + pair, 0, 0, 0)

    ending = pl.BlockSpec((rows // FINISH, width), lambda step: (part(step, plan.finish, FINISH), 0))
    shapes = plan.shapes
    bufs = []
    for k, shape in enumerate(shapes):
        bufs += reduce_scratch(dims, shape, jnp.bfloat16, 1 + k % 2)
    bufs += reduce_scratch(dims, (16, lanes_wide), jnp.float32, 1 + len(shapes) % 2)
    copies = scatter_copies(dims) * (len(shapes) + 1)
    return pl.pallas_call(
        functools.partial(backward_kernel, dims, plan, strips),
        grid=(plan.steps,),
        out_shape=[full((rows, width))] + [full((model, width))] * 4 + [full((model, ff)), full((wide, width)), full((16, lanes_wide))],
        in_specs=[vmem] * 9
        + [
            pl.BlockSpec((rows, FF_TILE), lambda step: (0, part(step, 0, plan.tiles))),
            pl.BlockSpec((rows, FF_TILE), lambda step: (0, part(step, 0, plan.tiles))),
            pl.BlockSpec((1, 2, slots, slots), probs_at),
            pl.BlockSpec((3, slots, 128), lambda step: (0,) + strip_pair(step)),
            pl.BlockSpec((slots, 128), strip_pair),
            ending, ending,
            pl.BlockSpec(memory_space=pl.ANY),
        ],
        out_specs=[ending] + [vmem] * 7,
        scratch_shapes=[pltpu.VMEM((rows, width), jnp.bfloat16)] * 3
        + [pltpu.VMEM((8, width), jnp.float32), pltpu.VMEM(dims + (2, 16, lanes_wide), jnp.float32)]
        + [pltpu.VMEM(lead + dims + (2,) + shape, jnp.bfloat16) for lead, shape in plan.wholes]
        + bufs
        + [pltpu.SemaphoreType.DMA((1,)), pltpu.SemaphoreType.DMA((copies,)), pltpu.SemaphoreType.DMA((copies,))],
        compiler_params=pltpu.CompilerParams(collective_id=3, has_side_effects=True, vmem_limit_bytes=VMEM_LIMIT),
        name="backward",
    )(turned, turned_two, out_grad, q_weight, k_weight, v_weight, vectors, small, grad_bup,
      grad_hidden, active, probs, heads, grad_context, tokens, grad_res, grad_wo)


def lane_pad(rows, width):
    return jnp.pad(rows, ((0, 0), (0, width - rows.shape[1])))


def pack_vectors(vectors, wide):
    width = 128 * -(-wide.shape[0] // 128)
    rows = lane_pad(jnp.stack(vectors).astype(jnp.float32), width)
    last = lane_pad(wide[None].astype(jnp.float32), width)
    return jnp.pad(jnp.concatenate([rows, last]), ((0, 15 - len(vectors)), (0, 0)))


def shards(
    dims,
    tokens,
    lengths,
    key_mask,
    ln1_gain,
    ln1_bias,
    q_weight,
    q_bias,
    k_weight,
    v_weight,
    v_bias,
    o_weight,
    o_bias,
    ln2_gain,
    ln2_bias,
    up_weight,
    up_bias,
    down_weight,
    down_bias,
    out_grad,
):
    early_weights, late_weights = (q_weight, k_weight, v_weight), (o_weight, up_weight, down_weight)
    vectors = (ln1_gain, ln1_bias, q_bias, v_bias, o_bias, ln2_gain, ln2_bias, down_bias)
    fused = q_weight.shape[0] % 8 == 0
    axes = ("gx", "gy")

    def whole(shard):
        return lax.all_gather(shard, axes, axis=0, tiled=True)

    row_count, width = tokens.shape
    strips = lengths.shape[0]
    slots = row_count // strips
    extra = -slots % 16

    def padded(values):
        return jnp.pad(values.reshape(strips, slots, width), ((0, 0), (0, extra), (0, 0))).reshape(-1, width)

    def cropped(values):
        return values.reshape(strips, slots + extra, width)[:, :slots].reshape(row_count, width)

    slot_ids = lax.iota(jnp.int32, slots)
    visible = (slot_ids[None, :] == 0) | (slot_ids[None, :] < lengths[:, None]) & (key_mask == 1)
    mask = jnp.where(jnp.pad(visible, ((0, 0), (0, extra))), 0.0, NEG_FILL).reshape(-1, 1)
    tokens_in, grads_in = padded(tokens), padded(out_grad)

    if fused:
        turned, heads, probs, context, q_full, k_full, v_full, rows, up_bias_full, *late = forward(
            dims, strips, tokens_in, mask, pack_vectors(vectors, up_bias), early_weights, late_weights
        )
        o_full, up_full, down_full = [w.reshape((-1,) + w.shape[-1:]) for w in late]
    else:
        q_full, k_full, v_full, o_full, up_full, down_full = [whole(w) for w in early_weights + late_weights]
        rows = jnp.stack([whole(v) for v in vectors]).astype(jnp.float32)
        up_bias_full = whole(up_bias).astype(jnp.float32)[None]
        turned, queries, keys, values, probs, context = attend(strips, tokens_in, q_full, k_full, v_full, rows, mask)
    block_out, grad_res, grad_context, grad_wo, active, grad_hidden, turned_two, small, grad_bup = ffn(
        tokens_in, context, grads_in, o_full, up_full, down_full, rows, up_bias_full
    )
    if fused:
        grad_tokens, sum_wq, sum_wk, sum_wv, sum_wo, sum_wup, sum_wdown, least = backward(
            dims, strips, turned, turned_two, grads_in, q_full, k_full, v_full, rows, small, grad_bup,
            grad_hidden, active, probs, heads, grad_context, tokens_in, grad_res,
            grad_wo.reshape(dims + (2,) + o_weight.shape),
        )
        vec = [least[n, : ln1_gain.shape[0]] for n in range(8)]
        sum_bup = least[8, : up_bias.shape[0]]
    else:
        grad_tokens, grad_wq, grad_wk, grad_wv, small_two = attend_back(
            strips, tokens_in, turned, queries, keys, values, probs, grad_context, grad_res, q_full, k_full, v_full, rows
        )
        small = small + small_two
        full = [grad_wq, grad_wk, grad_wv, grad_wo, right_mul(turned_two, grad_hidden), left_mul(active, grads_in), grad_bup[0]]
        full = [g.astype(jnp.float32) for g in full] + [small[n] for n in range(8)]
        sum_wq, sum_wk, sum_wv, sum_wo, sum_wup, sum_wdown, sum_bup, *vec = [
            lax.psum_scatter(g, axes, scatter_dimension=0, tiled=True) for g in full
        ]
    return (
        cropped(block_out), cropped(grad_tokens), vec[0], vec[1], sum_wq, vec[2], sum_wk, sum_wv, vec[3], sum_wo, vec[4],
        vec[5], vec[6], sum_wup, sum_bup, sum_wdown, vec[7],
    )


def solution(mesh):
    rows, flat = P(("gx", "gy"), None), P(("gx", "gy"))
    return jax.shard_map(
        functools.partial(shards, grid_of(mesh)),
        mesh=mesh,
        in_specs=(
            rows, flat, rows, flat, flat, rows, flat, rows, rows, flat, rows, flat, flat, flat, rows, flat, rows, flat, rows,
        ),
        out_specs=(
            rows, rows, flat, flat, rows, flat, rows, rows, flat, rows, flat, flat, flat, rows, flat, rows, flat,
        ),
        check_vma=False,
    )
```

```python
import functools
import math

import jax
import jax.numpy as jnp
from jax import lax
from jax.experimental import pallas as pl
from jax.experimental.pallas import tpu as pltpu
from jax.sharding import PartitionSpec as P

HEAD_DIM = 64
EPSILON = 1e-06
NEG_FILL = -1e30
VMEM_LIMIT = 63 * 1024 * 1024
GATHER_LAG = 12.0
GATHER_GAP = 5.0
SCATTER_LAG = 12.0
SCATTER_GAP = 6.0


def right_mul(left_arg, right_arg):
    return jnp.dot(left_arg, right_arg, preferred_element_type=jnp.float32)


def left_mul(left_arg, right_arg):
    return lax.dot_general(
        left_arg, right_arg, (((0,), (0,)), ((), ())), preferred_element_type=jnp.float32
    )


def back_mul(left_arg, right_arg):
    return lax.dot_general(
        left_arg, right_arg, (((1,), (1,)), ((), ())), preferred_element_type=jnp.float32
    )


MESH = pl.DeviceIdType.MESH


def grid_of(mesh):
    z_size, plane = mesh.shape["gx"], mesh.shape["gy"] // 2
    x_size = max(n for n in range(1, plane + 1) if plane % n == 0 and n * n <= plane)
    return z_size, plane // x_size, x_size


class Place:
    def __init__(self, dims):
        self.dims = dims
        g = lax.axis_index("gy")
        self.z = lax.axis_index("gx")
        self.c = lax.rem(g, 2)
        self.x = lax.rem(lax.div(g, 2), dims[2])
        self.y = lax.div(g, 2 * dims[2])

    def at(self, axis, step):
        here = (self.z, self.y, self.x)[axis]
        return lax.rem(here + step, self.dims[axis])

    def plane(self, first, step, other_step):
        a, b = self.at(first, step), self.at(3 - first, other_step)
        return (a, b) if first == 1 else (b, a)

    def device(self, axis, step):
        where = [self.z, self.y, self.x, self.c]
        if axis == 3:
            where[3] = 1 - self.c
        else:
            where[axis] = self.at(axis, step)
        return (where[0], (where[1] * self.dims[2] + where[2]) * 2 + where[3])

    def barrier(self):
        sem = pltpu.get_barrier_semaphore()
        peers = [(axis, step) for axis in range(3) for step in range(1, self.dims[axis])] + [(3, 1)]
        for axis, step in peers:
            pl.semaphore_signal(sem, inc=1, device_id=self.device(axis, step), device_id_type=MESH)
        pl.semaphore_wait(sem, len(peers))


class Lanes:
    def __init__(self, place, local, send, recv):
        self.place, self.local_sem, self.send, self.recv = place, local, send, recv
        self.used = self.local_used = 0

    def remote(self, src, dst, axis, step):
        n = self.used
        self.used += 1
        return pltpu.make_async_remote_copy(
            src_ref=src, dst_ref=dst, send_sem=self.send.at[n], recv_sem=self.recv.at[n],
            device_id=self.place.device(axis, step), device_id_type=MESH,
        )

    def local(self, src, dst):
        n = self.local_used
        self.local_used += 1
        return pltpu.make_async_copy(src, dst, self.local_sem.at[n])


def gather_copies(dims, z_last):
    z, y, x = dims
    if z_last:
        return (x * y - 1) + (z - 1) + z
    return (z - 1) + (x * y - 1) + x * y


class Gather:
    def __init__(self, lanes, shard, buf, first, z_last):
        p, dims = lanes.place, lanes.place.dims
        firsts, seconds = range(1, dims[first]), range(1, dims[3 - first])
        own = buf.at[p.z, p.y, p.x, p.c]
        local = lanes.local(shard, own)
        remote = lanes.remote

        def cell(step, other):
            y, x = p.plane(first, step, other)
            return buf.at[p.z, y, x, p.c] if z_last else buf.at[:, y, x, p.c]

        def layer(step):
            return buf.at[p.at(0, step), :, :, p.c]

        mine = shard if z_last else cell(0, 0)
        to_first = [remote(mine, cell(0, 0), first, s) for s in firsts]
        to_second = [remote(mine, cell(0, 0), 3 - first, t) for t in seconds]
        onward = [remote(cell(s, 0), cell(s, 0), 3 - first, t) for s in firsts for t in seconds]
        if z_last:
            along_z = [remote(layer(0), layer(0), 0, s) for s in range(1, dims[0])]
            cores = [remote(layer(s), layer(s), 3, 1) for s in range(dims[0])]
            self.stages = [
                ([], [], to_first + to_second + [local]),
                ([], to_first, onward),
                ([local], to_second + onward, along_z + cores[:1]),
                ([], along_z, cores[1:]),
            ]
        else:
            along_z = [remote(shard, own, 0, s) for s in range(1, dims[0])]
            core = {(s, t): remote(cell(s, t), cell(s, t), 3, 1) for s in range(dims[first]) for t in range(dims[3 - first])}
            cores = list(core.values())
            self.stages = [
                ([], [], along_z + [local]),
                ([local], along_z, to_first + to_second + [core[0, 0]]),
                ([], to_first, onward + [core[s, 0] for s in firsts]),
                ([], to_second + onward, [core[s, t] for s in range(dims[first]) for t in seconds]),
            ]
        self.handed = cores
        self.remotes = to_first + to_second + onward + along_z + cores

    def run(self, stage):
        done, arrived, starts = self.stages[stage]
        for copy in done:
            copy.wait()
        for copy in arrived:
            copy.wait_recv()
        for copy in starts:
            copy.start()

    def arrive(self):
        for copy in self.handed:
            copy.wait_recv()

    def finish(self):
        for copy in self.remotes:
            copy.wait_send()


def scatter_copies(dims):
    z, y, x = dims
    return 1 + (z - 1) + (x * y - 1)


def pieces_of(shapes, narrow):
    pieces = []
    for n, shape in enumerate(shapes):
        parts = max(1, shape[-1] // 768)
        if parts == 1 and shape[-2] > narrow and shape[-1] == 768:
            parts = 3
        for k in range(parts):
            size = shape[-1] // parts
            pieces.append((n, k * size, size, 1 + len(pieces) % 2))
    return pieces


def waves(count, stages):
    return [[(b + 1 - s, s) for s in range(1, stages) if 0 <= b + 1 - s < count] for b in range(count + stages - 2)]


def gather_jobs(lanes, pieces, shards, bufs):
    return [
        Gather(lanes, shards[n].at[:, pl.ds(at, size)], bufs[n].at[:, :, :, :, :, pl.ds(at, size)], first, False)
        for n, at, size, first in pieces
    ]


def comm_semaphores(pieces, copies):
    return [
        pltpu.SemaphoreType.DMA((len(pieces),)),
        pltpu.SemaphoreType.DMA((copies * len(pieces),)),
        pltpu.SemaphoreType.DMA((copies * len(pieces),)),
    ]


def run_wave(jobs, wave):
    for n, stage in wave:
        jobs[n].run(stage)


def layer_norm_parts(values):
    center = values - jnp.mean(values, axis=-1, keepdims=True)
    scale = lax.rsqrt(jnp.mean(center * center, axis=-1, keepdims=True) + EPSILON)
    return center * scale, scale


def layer_norm_back(grad, xhat, scale, gain):
    scaled = grad * gain
    inner = scaled - jnp.mean(scaled, axis=-1, keepdims=True)
    back = scale * (inner - xhat * jnp.mean(scaled * xhat, axis=-1, keepdims=True))
    return back, jnp.sum(grad * xhat, axis=0, keepdims=True), jnp.sum(grad, axis=0, keepdims=True)


def gelu_and_slope(v):
    size = jnp.abs(v)
    t = 1.0 / (1.0 + (0.3275911 * math.sqrt(0.5)) * size)
    bell = jnp.exp(-0.5 * v * v)
    poly = ((((0.5 * 1.061405429) * t - 0.5 * 1.453152027) * t + 0.5 * 1.421413741) * t - 0.5 * 0.284496736) * t
    tail = (poly + 0.5 * 0.254829592) * t * bell
    share = jnp.where(v >= 0, 1.0 - tail, tail)
    return v * share, share + (v * (1.0 / math.sqrt(2.0 * math.pi))) * bell


def ffn_kernel(
    a_rows, b_rows, ff_tile, c_rows,
    tokens_hbm, context_hbm, out_grad_hbm, o_hbm, up_hbm, down_hbm, vectors, up_bias,
    block_out, res_hbm, back_hbm, grad_wo, active_hbm, hidden_hbm, normed2_t, small, grad_bup,
    normed2, grad_att, tokens, context, out_grad, o_weight, up_weight, down_weight,
    grad_res, grad_context, active, grad_hidden, outputs, loaded, stored,
):
    rows, width = tokens.shape
    ff = up_weight.shape[1]
    o_bias, gain, bias, down_bias = vectors[4:5, :], vectors[5:6, :], vectors[6:7, :], vectors[7:8, :]
    small[...] = jnp.zeros_like(small)
    loads = [
        pltpu.make_async_copy(src, dst, loaded.at[n])
        for n, (src, dst) in enumerate((
            (context_hbm, context), (o_hbm, o_weight), (tokens_hbm, tokens), (out_grad_hbm, out_grad),
        ))
    ]

    def tile_in(n, kind):
        at = pl.ds(n * ff_tile if isinstance(n, int) else pl.multiple_of(n * ff_tile, ff_tile), ff_tile)
        if kind:
            return pltpu.make_async_copy(down_hbm.at[at, :], down_weight.at[at, :], loaded.at[4 + 2 * n + kind])
        return pltpu.make_async_copy(up_hbm.at[:, at], up_weight.at[:, at], loaded.at[4 + 2 * n + kind])

    for copy in loads:
        copy.start()
    for n in range(ff // ff_tile):
        tile_in(n, 0).start()
        tile_in(n, 1).start()
    for copy in loads[:3]:
        copy.wait()

    def attended(n, carry):
        at = pl.ds(pl.multiple_of(n * a_rows, a_rows), a_rows)
        residual = tokens[at, :].astype(jnp.float32) + right_mul(context[at, :], o_weight[...]) + o_bias
        grad_res[at, :] = residual
        xhat, _ = layer_norm_parts(residual)
        normed2[at, :] = (xhat * gain + bias).astype(jnp.bfloat16)
        return carry

    lax.fori_loop(0, rows // a_rows, attended, 0)
    for copy in loads[3:]:
        copy.wait()

    def tile_out(n, kind):
        cols = pl.ds(pl.multiple_of(n * ff_tile, ff_tile), ff_tile)
        src, dst = ((active, active_hbm), (grad_hidden, hidden_hbm))[kind]
        return pltpu.make_async_copy(src.at[:, cols], dst.at[:, cols], stored.at[2 * n + kind])

    def strip_out(n, kind):
        at = pl.ds(pl.multiple_of(n * c_rows, c_rows), c_rows)
        src, dst = ((grad_res, res_hbm), (grad_context, back_hbm))[kind]
        return pltpu.make_async_copy(src.at[at, :], dst.at[at, :], stored.at[2 * (ff // ff_tile + n) + kind])

    def hidden_tile(n, carry):
        cols = pl.ds(pl.multiple_of(n * ff_tile, ff_tile), ff_tile)
        sums = jnp.zeros((1, ff_tile), jnp.float32)
        tile_in(n, 0).wait()
        tile_in(n, 1).wait()

        def piece(m, sums):
            at = pl.ds(pl.multiple_of(m * b_rows, b_rows), b_rows)
            hidden = right_mul(normed2[at, :], up_weight[:, cols]) + up_bias[:, cols]
            grad_active = back_mul(out_grad[at, :], down_weight[cols, :])
            value, slope = gelu_and_slope(hidden)
            active[at, cols] = value.astype(jnp.bfloat16)
            back = (slope * grad_active).astype(jnp.bfloat16)
            grad_hidden[at, cols] = back
            return sums + jnp.sum(back.astype(jnp.float32), axis=0, keepdims=True)

        grad_bup[:, cols] = lax.fori_loop(0, rows // b_rows, piece, sums)
        tile_out(n, 0).start()
        tile_out(n, 1).start()
        return carry

    lax.fori_loop(0, ff // ff_tile, hidden_tile, 0)

    def finish(n, carry):
        at = pl.ds(pl.multiple_of(n * c_rows, c_rows), c_rows)
        residual = grad_res[at, :]
        cotangent = out_grad[at, :].astype(jnp.float32)
        outputs[at, :] = (residual + right_mul(active[at, :], down_weight[...]) + down_bias).astype(jnp.bfloat16)
        grad = back_mul(grad_hidden[at, :], up_weight[...])
        xhat, scale = layer_norm_parts(residual)
        back, gain_sum, bias_sum = layer_norm_back(grad, xhat, scale, gain)
        total = cotangent + back
        grad_res[at, :] = total
        low = total.astype(jnp.bfloat16)
        grad_att[at, :] = low
        grad_context[at, :] = back_mul(low, o_weight[...]).astype(jnp.bfloat16)
        small[4:5, :] += jnp.sum(low.astype(jnp.float32), axis=0, keepdims=True)
        small[5:6, :] += gain_sum
        small[6:7, :] += bias_sum
        small[7:8, :] += jnp.sum(cotangent, axis=0, keepdims=True)
        strip_out(n, 0).start()
        strip_out(n, 1).start()
        return carry

    lax.fori_loop(0, rows // c_rows, finish, 0)

    normed2_t[...] = normed2[...].T
    grad_wo[...] = left_mul(context[...], grad_att[...]).astype(jnp.bfloat16)
    slots = block_out.shape[0] * c_rows // rows
    for n in range(rows // c_rows):
        block_out[n * slots : (n + 1) * slots, :] = outputs[n * c_rows : n * c_rows + slots, :]
    for n in range(ff // ff_tile):
        tile_out(n, 0).wait()
        tile_out(n, 1).wait()
    for n in range(rows // c_rows):
        strip_out(n, 0).wait()
        strip_out(n, 1).wait()


def ffn(strips, row_count, tokens, context, out_grad, o_weight, up_weight, down_weight, vectors, up_bias):
    rows, width = tokens.shape
    ff = up_weight.shape[1]
    low = functools.partial(jax.ShapeDtypeStruct, dtype=jnp.bfloat16)
    full = functools.partial(jax.ShapeDtypeStruct, dtype=jnp.float32)
    vmem, hbm = pl.BlockSpec(memory_space=pltpu.VMEM), pl.BlockSpec(memory_space=pl.ANY)
    return pl.pallas_call(
        functools.partial(ffn_kernel, rows, rows, 1024, rows // strips),
        out_shape=[
            low((row_count, width)), full((rows, width)), low((rows, width)),
            low((width, width)), low((rows, ff)), low((rows, ff)), low((width, rows)), full((8, width)), full((1, ff)),
        ],
        in_specs=[hbm] * 6 + [vmem] * 2,
        out_specs=[vmem, hbm, hbm, vmem, hbm, hbm, vmem, vmem, vmem],
        scratch_shapes=[pltpu.VMEM((rows, width), jnp.bfloat16)] * 5
        + [
            pltpu.VMEM((width, width), jnp.bfloat16),
            pltpu.VMEM((width, ff), jnp.bfloat16),
            pltpu.VMEM((ff, width), jnp.bfloat16),
            pltpu.VMEM((rows, width), jnp.float32),
            pltpu.VMEM((rows, width), jnp.bfloat16),
            pltpu.VMEM((rows, ff), jnp.bfloat16),
            pltpu.VMEM((rows, ff), jnp.bfloat16),
            pltpu.VMEM((rows, width), jnp.bfloat16),
            pltpu.SemaphoreType.DMA((4 + 2 * ff // 1024,)),
            pltpu.SemaphoreType.DMA((2 * (ff // 1024 + strips),)),
        ],
        compiler_params=pltpu.CompilerParams(vmem_limit_bytes=VMEM_LIMIT),
        name="ffn",
    )(tokens, context, out_grad, o_weight, up_weight, down_weight, vectors, up_bias)


def head_lanes(pair, head):
    lane = lax.broadcasted_iota(jnp.int32, pair.shape, 1)
    return jnp.where(lax.div(lane, HEAD_DIM) == head, pair, jnp.zeros_like(pair))


def attend_pair(strips, step, mask, queries, keys, values, probs, context):
    rows, width = queries.shape
    slots, pairs = rows // strips, width // 128
    at = pl.ds(pl.multiple_of(lax.div(step, pairs) * slots, slots), slots)
    cols = pl.ds(pl.multiple_of(lax.rem(step, pairs) * 128, 128), 128)
    query, key, value = queries[at, cols], keys[at, cols], values[at, cols]
    hidden = mask[at, 0:1]
    total = jnp.zeros((slots, 128), jnp.float32)
    for head in range(2):
        scores = back_mul(key, head_lanes(query, head)) + hidden
        powers = jnp.exp(scores - jnp.max(scores, axis=0, keepdims=True))
        low = (powers * (1.0 / jnp.sum(powers, axis=0, keepdims=True))).astype(jnp.bfloat16)
        probs[0, head] = low
        total = total + left_mul(low, head_lanes(value, head))
    context[at, cols] = total.astype(jnp.bfloat16)


def attend_kernel(strips, tokens, q_weight, k_weight, v_weight, vectors, mask, turned, queries, keys, values, probs, context, normed):
    rows, width = tokens.shape
    slots, pairs = rows // strips, width // 128
    step = pl.program_id(0)

    @pl.when(step == 0)
    def _():
        xhat, _ = layer_norm_parts(tokens[...].astype(jnp.float32))
        normed[...] = (xhat * vectors[0:1, :] + vectors[1:2, :]).astype(jnp.bfloat16)
        turned[...] = normed[...].T
        scale = 1.0 / math.sqrt(HEAD_DIM)
        low = (right_mul(normed[...], q_weight[...]) + vectors[2:3, :]).astype(jnp.bfloat16)
        queries[...] = low * jnp.bfloat16(scale)
        keys[...] = right_mul(normed[...], k_weight[...]).astype(jnp.bfloat16)
        values[...] = (right_mul(normed[...], v_weight[...]) + vectors[3:4, :]).astype(jnp.bfloat16)

    attend_pair(strips, step, mask, queries, keys, values, probs, context)


def attend(strips, tokens, q_weight, k_weight, v_weight, vectors, mask):
    rows, width = tokens.shape
    slots, pairs = rows // strips, width // 128
    low = functools.partial(jax.ShapeDtypeStruct, dtype=jnp.bfloat16)
    return pl.pallas_call(
        functools.partial(attend_kernel, strips),
        grid=(strips * pairs,),
        out_shape=[low((width, rows))] + [low((rows, width))] * 3 + [low((strips * pairs, 2, slots, slots)), low((rows, width))],
        in_specs=[pl.BlockSpec(memory_space=pltpu.VMEM)] * 6,
        out_specs=[pl.BlockSpec(memory_space=pltpu.VMEM)] * 4
        + [pl.BlockSpec((1, 2, slots, slots), lambda n: (n, 0, 0, 0)), pl.BlockSpec(memory_space=pltpu.VMEM)],
        scratch_shapes=[pltpu.VMEM((rows, width), jnp.bfloat16)],
        compiler_params=pltpu.CompilerParams(vmem_limit_bytes=VMEM_LIMIT),
        name="attend",
    )(tokens, q_weight, k_weight, v_weight, vectors, mask)


def attend_back_kernel(
    strips, tokens, turned, queries, keys, values, probs, grad_context, grad_res, q_weight, k_weight, v_weight, vectors,
    grad_tokens, grad_wq, grad_wk, grad_wv, small,
    grad_q, grad_k, grad_v,
):
    rows, width = tokens.shape
    slots, pairs = rows // strips, width // 128
    step = pl.program_id(0)
    at = pl.ds(pl.multiple_of(lax.div(step, pairs) * slots, slots), slots)
    cols = pl.ds(pl.multiple_of(lax.rem(step, pairs) * 128, 128), 128)
    query, key, value, grad = queries[at, cols], keys[at, cols], values[at, cols], grad_context[at, cols]
    back_q = back_k = back_v = jnp.zeros((slots, 128), jnp.float32)
    for head in range(2):
        low = probs[0, head]
        own = head_lanes(grad, head)
        back_v = back_v + right_mul(low, own)
        wide = low.astype(jnp.float32)
        slope = back_mul(value, own)
        inner = jnp.sum(wide * slope, axis=0, keepdims=True)
        pull = (wide * (slope - inner)).astype(jnp.bfloat16)
        back_q = back_q + left_mul(pull, head_lanes(key, head))
        back_k = back_k + right_mul(pull, head_lanes(query, head))
    grad_q[at, cols] = (back_q * (1.0 / math.sqrt(HEAD_DIM))).astype(jnp.bfloat16)
    grad_k[at, cols] = back_k.astype(jnp.bfloat16)
    grad_v[at, cols] = back_v.astype(jnp.bfloat16)

    @pl.when(step == strips * pairs - 1)
    def _():
        grad_wq[...] = right_mul(turned[...], grad_q[...]).astype(jnp.bfloat16)
        grad_wk[...] = right_mul(turned[...], grad_k[...]).astype(jnp.bfloat16)
        grad_wv[...] = right_mul(turned[...], grad_v[...]).astype(jnp.bfloat16)
        small[...] = jnp.zeros_like(small)
        small[2:3, :] = jnp.sum(grad_q[...].astype(jnp.float32), axis=0, keepdims=True)
        small[3:4, :] = jnp.sum(grad_v[...].astype(jnp.float32), axis=0, keepdims=True)

        def finish(n, carry):
            at = pl.ds(pl.multiple_of(n * slots, slots), slots)
            grad = back_mul(grad_q[at, :], q_weight[...]) + back_mul(grad_k[at, :], k_weight[...])
            grad = grad + back_mul(grad_v[at, :], v_weight[...])
            xhat, scale = layer_norm_parts(tokens[at, :].astype(jnp.float32))
            back, gain_sum, bias_sum = layer_norm_back(grad, xhat, scale, vectors[0:1, :])
            grad_tokens[at, :] = grad_res[at, :] + back
            small[0:1, :] += gain_sum
            small[1:2, :] += bias_sum
            return carry

        lax.fori_loop(0, strips, finish, 0)


def attend_back(strips, tokens, turned, queries, keys, values, probs, grad_context, grad_res, q_weight, k_weight, v_weight, vectors):
    rows, width = tokens.shape
    slots, pairs = rows // strips, width // 128
    low = functools.partial(jax.ShapeDtypeStruct, dtype=jnp.bfloat16)
    full = functools.partial(jax.ShapeDtypeStruct, dtype=jnp.float32)
    vmem = pl.BlockSpec(memory_space=pltpu.VMEM)
    block = pl.BlockSpec((1, 2, slots, slots), lambda n: (n, 0, 0, 0))
    return pl.pallas_call(
        functools.partial(attend_back_kernel, strips),
        grid=(strips * pairs,),
        out_shape=[full((rows, width)), low((width, width)), low((width, width)), low((width, width)), full((8, width))],
        in_specs=[vmem] * 5 + [block] + [vmem] * 6,
        out_specs=[vmem] * 5,
        scratch_shapes=[pltpu.VMEM((rows, width), jnp.bfloat16)] * 3,
        compiler_params=pltpu.CompilerParams(vmem_limit_bytes=VMEM_LIMIT),
        name="attend_back",
    )(tokens, turned, queries, keys, values, probs, grad_context, grad_res, q_weight, k_weight, v_weight, vectors)


def forward_plan(sizes, early, steps, lag, gap):
    project, attend = 5.0, 2.3
    events, start = [], 0.0
    for n, size in enumerate(sizes):
        start = start + gap * size
        events += [(start + 2.0 + lag * (k - 1), k, n) for k in range(1, 4)]
    events.sort()
    first = max(k for k, (_, _, n) in enumerate(events) if n < early) + 1
    begin = events[first - 1][0] + project
    plan, late = {0: [(n, k) for _, k, n in events[:first]]}, []
    for when, k, n in events[first:]:
        fits = [s for s in range(1, steps) if begin + attend * (s - 1) >= when]
        plan.setdefault(fits[0], []).append((n, k)) if fits else late.append((n, k))
    return plan, late


def forward_kernel(dims, pieces, early, plan, late, strips, tokens_in, grads_in, mask, *refs):
    count = early + 3
    shards, refs = refs[:count], refs[count:]
    (turned, heads, probs, context, tokens, grads), refs = refs[:6], refs[6:]
    queries, keys, values = heads.at[0], heads.at[1], heads.at[2]
    weights, (vectors, up_bias), bufs, refs = refs[: early - 1], refs[early - 1 : early + 1], refs[early + 1 : early + 4], refs[early + 4 :]
    near, normed, sems = refs[:early], refs[early], refs[early + 1 :]
    rows, width = tokens.shape
    slots, pairs = rows // strips, width // 128
    step = pl.program_id(0)
    place = Place(dims)
    jobs = gather_jobs(Lanes(place, *sems), pieces, shards, list(near) + list(bufs))

    @pl.when(step == 0)
    def _():
        place.barrier()
        for job in jobs:
            job.run(0)
        given = tokens_in.shape[0] // strips
        for src, dst in ((tokens_in, tokens), (grads_in, grads)):
            dst[...] = jnp.zeros_like(dst)
            for n in range(strips):
                dst[n * slots : n * slots + given, :] = src[n * given : (n + 1) * given, :]
        xhat, _ = layer_norm_parts(tokens[...].astype(jnp.float32))
        run_wave(jobs, plan[0])
        for job in jobs[:early]:
            job.arrive()
        model, wide = shards[1].shape[0], up_bias.shape[1] // (width // shards[1].shape[0])
        for d in range(width // model):
            at = (d // (2 * dims[1] * dims[2]), d // (2 * dims[2]) % dims[1], d // 2 % dims[2], d % 2)
            vectors[:, d * model : (d + 1) * model] = near[0][at + (pl.ds(0, 8), pl.ds(0, model))]
            up_bias[:, d * wide : (d + 1) * wide] = near[0][at + (pl.ds(8, 1), pl.ds(0, wide))]
        for whole, buf in zip(weights, near[1:]):
            whole[...] = buf[...].astype(jnp.float32).reshape(width, width).astype(jnp.bfloat16)
        q_weight, k_weight, v_weight = weights
        normed[...] = (xhat * vectors[0:1, :] + vectors[1:2, :]).astype(jnp.bfloat16)
        turned[...] = normed[...].T
        scale = 1.0 / math.sqrt(HEAD_DIM)
        low = (right_mul(normed[...], q_weight[...]) + vectors[2:3, :]).astype(jnp.bfloat16)
        queries[...] = low * jnp.bfloat16(scale)
        keys[...] = right_mul(normed[...], k_weight[...]).astype(jnp.bfloat16)
        values[...] = (right_mul(normed[...], v_weight[...]) + vectors[3:4, :]).astype(jnp.bfloat16)

    for when, wave in plan.items():
        if when:
            pl.when(step == when)(functools.partial(run_wave, jobs, wave))

    attend_pair(strips, step, mask, queries, keys, values, probs, context)

    @pl.when(step == strips * pairs - 1)
    def _():
        run_wave(jobs, late)
        for job in jobs[early:]:
            job.arrive()
        for job in jobs:
            job.finish()


def forward(dims, strips, tokens, grads, mask, packed, early_shards, late_shards):
    rows, width = mask.shape[0], tokens.shape[1]
    slots, pairs = rows // strips, width // 128
    shards = [packed] + list(early_shards) + list(late_shards)
    early = 1 + len(early_shards)
    model = early_shards[0].shape[0]
    ff = late_shards[1].shape[1]
    low = functools.partial(jax.ShapeDtypeStruct, dtype=jnp.bfloat16)
    full = functools.partial(jax.ShapeDtypeStruct, dtype=jnp.float32)
    vmem = pl.BlockSpec(memory_space=pltpu.VMEM)
    pieces = pieces_of([s.shape for s in shards], model)
    sizes = [shards[n].shape[0] * size * shards[n].dtype.itemsize / (model * width * 2) for n, _, size, _ in pieces]
    plan, late = forward_plan(sizes, early, strips * pairs, GATHER_LAG, GATHER_GAP)
    return pl.pallas_call(
        functools.partial(forward_kernel, dims, pieces, early, plan, late, strips),
        grid=(strips * pairs,),
        out_shape=[low((width, rows))]
        + [low((3, rows, width))]
        + [low((strips * pairs, 2, slots, slots))] + [low((rows, width))] * 3
        + [low((width, width))] * len(early_shards)
        + [full((8, width)), full((1, ff))]
        + [low(dims + (2,) + s.shape) for s in late_shards],
        in_specs=[vmem] * (3 + len(shards)),
        out_specs=[vmem] * 2
        + [pl.BlockSpec((1, 2, slots, slots), lambda n: (n, 0, 0, 0)), vmem, vmem, vmem]
        + [vmem] * (early + 1)
        + [pl.BlockSpec(memory_space=pl.ANY)] * 3,
        scratch_shapes=[pltpu.VMEM(dims + (2,) + s.shape, s.dtype) for s in shards[:early]]
        + [pltpu.VMEM((rows, width), jnp.bfloat16)]
        + comm_semaphores(pieces, gather_copies(dims, False)),
        compiler_params=pltpu.CompilerParams(vmem_limit_bytes=VMEM_LIMIT, collective_id=2, has_side_effects=True),
        name="forward",
    )(tokens, grads, mask, *shards)


class Reduce:
    def __init__(self, lanes, whole, bufs, first, write):
        p, dims = lanes.place, lanes.place.dims
        self.p, self.dims, self.first, self.write = p, dims, first, write
        self.firsts, self.seconds = range(1, dims[first]), range(1, dims[3 - first])
        self.from_core, self.from_far, self.from_first, self.from_second, self.from_z = bufs
        self.mine, remote = whole.at[:, :, :, p.c], lanes.remote

        def cell(step, other):
            y, x = p.plane(first, step, other)
            return whole.at[:, y, x, p.c]

        core = [remote(whole.at[:, :, :, 1 - p.c], self.from_core, 3, 1)]
        self.far = [remote(cell(s, t), self.from_far.at[s - 1, t - 1], first, s) for s in self.firsts for t in self.seconds]
        self.to_first = [remote(cell(s, 0), self.from_first.at[s - 1], first, s) for s in self.firsts]
        self.to_second = [remote(cell(0, t), self.from_second.at[t - 1], 3 - first, t) for t in self.seconds]
        along_z = [
            remote(whole.at[p.at(0, s), p.y, p.x, p.c], self.from_z.at[s - 1], 0, s) for s in range(1, dims[0])
        ]
        self.ships = [core, self.far + self.to_first, self.to_second, along_z]

    def total(self, at, terms):
        total = self.mine[at].astype(jnp.float32)
        for ref, index in terms:
            total = total + ref[index].astype(jnp.float32)
        return total

    def add(self, at, terms):
        self.mine[at] = self.total(at, terms).astype(self.mine.dtype)

    def run(self, stage):
        p, (z_size, y_size, x_size) = self.p, self.dims
        arrivals = (self.ships[0], self.far, self.to_first + self.to_second, self.ships[3])[stage - 1]
        for copy in arrivals:
            copy.wait_recv()
        if stage == 1:
            def body(n, carry):
                at = (lax.div(n, y_size * x_size), lax.rem(lax.div(n, x_size), y_size), lax.rem(n, x_size))
                self.add(at, [(self.from_core, at)])
                return carry

            lax.fori_loop(0, z_size * y_size * x_size, body, 0)
        elif stage == 2:
            for z in range(z_size):
                for t in self.seconds:
                    self.add((z,) + p.plane(self.first, 0, t), [(self.from_far, (s - 1, t - 1, z)) for s in self.firsts])
        elif stage == 3:
            for z in range(z_size):
                terms = [(self.from_first, (s - 1, z)) for s in self.firsts]
                self.add((z, p.y, p.x), terms + [(self.from_second, (t - 1, z)) for t in self.seconds])
        else:
            self.write(self.total((p.z, p.y, p.x), [(self.from_z, (s,)) for s in range(z_size - 1)]))

    def ship(self, stage):
        if stage < 4:
            for copy in self.ships[stage]:
                copy.start()

    def finish(self):
        for copies in self.ships:
            for copy in copies:
                copy.wait_send()


def reduce_scratch(dims, shape, dtype, first):
    z, y, x = dims
    f, s = max(dims[first] - 1, 1), max(dims[3 - first] - 1, 1)
    leads = [(z, y, x), (f, s, z), (f, z), (s, z), (max(z - 1, 1),)]
    return [pltpu.VMEM(lead + shape, dtype) for lead in leads]


def add_wave(jobs, wave):
    left = None
    for n, stage in wave:
        if stage:
            jobs[n].run(stage)
        if left:
            jobs[left[0]].ship(left[1])
        left = (n, stage)
    return left


FF_TILE = 384
FINISH = 4
PAIRS_PER_PIECE = 2


class Plan:
    def __init__(self, dims, strips, rows, width, ff, lag, gap):
        self.tiles, self.pairs = ff // FF_TILE, width // 128
        self.attention = self.tiles
        self.finish = self.attention + strips * self.pairs
        self.steps = self.finish + FINISH
        n = 2 * dims[0] * dims[1] * dims[2]
        model, wide = width // n, ff // n
        per_up = width // FF_TILE
        lasts = [0] + [per_up * (k + 1) for k in range(ff // width)] + [self.attention] * 3
        groups = self.pairs // PAIRS_PER_PIECE
        lasts += [self.attention + strips * PAIRS_PER_PIECE * (g + 1) for g in range(groups)]
        self.wholes = [((), (model, width)), ((ff // width,), (model, width)), ((), (wide, width))]
        self.wholes += [((groups,), (3 * model, width // groups))]
        self.shapes = [(model, width)] * (1 + ff // width) + [(wide, width // 3)] * 3 + [(3 * model, width // groups)] * groups
        ends = [2.6] * self.attention + [3.2] * (strips * self.pairs) + [1.6] * FINISH
        starts = [sum(ends[:k]) for k in range(self.steps)]
        events, free = [], 0.0
        for piece, step in enumerate(lasts):
            begin = max(starts[step], free)
            free = begin + gap
            events += [(starts[step], 0, piece, step)]
            events += [(begin + 2.0 + lag * (k - 1), k, piece, 0) for k in range(1, 5)]
        self.waves, self.late = {}, []
        for when, stage, piece, step in sorted(events):
            fits = [k for k in range(self.steps) if starts[k] >= when and k >= step]
            if fits:
                self.waves.setdefault(fits[0], []).append((piece, stage))
            else:
                self.late.append((piece, stage))


def by_step(step, table):
    keys = sorted(table)

    def pick(low, high):
        if high - low == 1:
            pl.when(step == keys[low])(table[keys[low]])
            return
        middle = (low + high) // 2
        lax.cond(step < keys[middle], lambda: pick(low, middle), lambda: pick(middle, high))

    pick(0, len(keys))


def backward_kernel(dims, plan, strips, *refs):
    (turned, turned_two, out_grad, q_weight, k_weight, v_weight, vectors, small_in, bup_in) = refs[:9]
    (grad_hidden, active, probs, heads, grad_b, tokens, grad_res, wo_hbm) = refs[9:17]
    (grad_tokens, sum_q, sum_k, sum_v, sum_o, sum_up, sum_down, sum_vec) = refs[17:25]
    refs = refs[25:]
    grad_q, grad_k, grad_v, small, vec_whole, finished, o_whole, up_whole, down_whole, qkv_whole = refs[:10]
    refs = refs[10:]
    local, send, recv = refs[-3:]
    width, rows = turned.shape
    slots, ff_pieces, groups = rows // strips, up_whole.shape[0], qkv_whole.shape[0]
    step = pl.program_id(0)
    place = Place(dims)
    lanes = Lanes(place, local, send, recv)
    o_copy = lanes.local(wo_hbm, o_whole)

    model = sum_q.shape[0]
    columns = width // groups

    def write_to(ref, at, size):
        def write(total):
            ref[:, pl.ds(at, size)] = total
        return write

    def write_group(g):
        def write(total):
            for n, ref in enumerate((sum_q, sum_k, sum_v)):
                ref[:, pl.ds(g * columns, columns)] = total[n * model : (n + 1) * model]
        return write

    third = width // 3
    views = [(o_whole, write_to(sum_o, 0, width))]
    views += [(up_whole.at[k], write_to(sum_up, k * width, width)) for k in range(ff_pieces)]
    views += [
        (down_whole.at[:, :, :, :, :, pl.ds(k * third, third)], write_to(sum_down, k * third, third)) for k in range(3)
    ]
    views += [(qkv_whole.at[g], write_group(g)) for g in range(groups)]
    views += [(vec_whole, write_to(sum_vec, 0, sum_vec.shape[1]))]
    jobs = [Reduce(lanes, whole, refs[5 * n : 5 * n + 5], 1 + n % 2, write) for n, (whole, write) in enumerate(views)]
    last = len(jobs) - 1

    @pl.when(step == 0)
    def _():
        place.barrier()
        o_copy.start()
        small[...] = small_in[...]
        o_copy.wait()

    by_step(step, {when: lambda wave=wave: add_wave(jobs, wave) and None for when, wave in plan.waves.items()})

    def rows_to_blocks(product):
        n = 2 * dims[0] * dims[1] * dims[2]
        return product.reshape(dims + (2, product.shape[0] // n, product.shape[1])).astype(jnp.bfloat16)

    @pl.when(step < plan.attention)
    def _():
        per = width // FF_TILE
        part = pl.ds(pl.multiple_of(lax.rem(step, per) * FF_TILE, FF_TILE), FF_TILE)
        up_whole[lax.div(step, per), :, :, :, :, :, part] = rows_to_blocks(right_mul(turned_two[...], grad_hidden[...]))
        product = left_mul(active[...], out_grad[...])
        wide = down_whole.shape[4]
        for b in range(FF_TILE // wide):
            d = step * (FF_TILE // wide) + b
            y_x = lax.div(d, 2)
            at = (lax.div(y_x, dims[1] * dims[2]), lax.rem(lax.div(y_x, dims[2]), dims[1]), lax.rem(y_x, dims[2]), lax.rem(d, 2))
            down_whole[at] = product[b * wide : (b + 1) * wide].astype(jnp.bfloat16)

    pair, strip = lax.div(step - plan.attention, strips), lax.rem(step - plan.attention, strips)
    in_attention = (step >= plan.attention) & (step < plan.finish)

    @pl.when(in_attention)
    def _():
        at = pl.ds(pl.multiple_of(strip * slots, slots), slots)
        cols = pl.ds(pl.multiple_of(pair * 128, 128), 128)
        query, key, value, grad = heads[0], heads[1], heads[2], grad_b[...]
        back_q = back_k = back_v = jnp.zeros((slots, 128), jnp.float32)
        for head in range(2):
            low = probs[0, head]
            own = head_lanes(grad, head)
            back_v = back_v + right_mul(low, own)
            wide = low.astype(jnp.float32)
            slope = back_mul(value, own)
            inner = jnp.sum(wide * slope, axis=0, keepdims=True)
            pull = (wide * (slope - inner)).astype(jnp.bfloat16)
            back_q = back_q + left_mul(pull, head_lanes(key, head))
            back_k = back_k + right_mul(pull, head_lanes(query, head))
        grad_q[at, cols] = (back_q * (1.0 / math.sqrt(HEAD_DIM))).astype(jnp.bfloat16)
        grad_k[at, cols] = back_k.astype(jnp.bfloat16)
        grad_v[at, cols] = back_v.astype(jnp.bfloat16)

    group_steps = strips * PAIRS_PER_PIECE

    @pl.when(in_attention & (lax.rem(step - plan.attention, group_steps) == group_steps - 1))
    def _():
        g = lax.div(step - plan.attention, group_steps)
        cols = pl.ds(pl.multiple_of(g * columns, columns), columns)
        for n, grad in enumerate((grad_q, grad_k, grad_v)):
            part = grad[:, cols]
            qkv_whole[g, :, :, :, :, pl.ds(n * model, model), :] = rows_to_blocks(right_mul(turned[...], part))
            if n != 1:
                small[2 + n // 2 : 3 + n // 2, cols] = jnp.sum(part.astype(jnp.float32), axis=0, keepdims=True)

    @pl.when(step >= plan.finish)
    def _():
        size = rows // FINISH
        at = pl.ds(pl.multiple_of((step - plan.finish) * size, size), size)
        grad = back_mul(grad_q[at, :], q_weight[...]) + back_mul(grad_k[at, :], k_weight[...])
        grad = grad + back_mul(grad_v[at, :], v_weight[...])
        xhat, scale = layer_norm_parts(tokens[...].astype(jnp.float32))
        back, gain_sum, bias_sum = layer_norm_back(grad, xhat, scale, vectors[0:1, :])
        finished[...] = grad_res[...] + back
        small[0:1, :] += gain_sum
        small[1:2, :] += bias_sum

    def store(n):
        size, slots_in = rows // FINISH, grad_tokens.shape[0] // strips
        per = FINISH // strips
        low = (n % per) * size
        count = min(size, slots_in - low)
        grad_tokens[pl.ds(n // per * slots_in + low, count), :] = finished[0:count, :]

    by_step(step, {plan.finish + n: functools.partial(store, n) for n in range(FINISH)})
    by_step(step, {when: functools.partial(jobs[wave[-1][0]].ship, wave[-1][1]) for when, wave in plan.waves.items()})

    @pl.when(step == plan.steps - 1)
    def _():
        vec_whole[...] = jnp.zeros_like(vec_whole)
        wide = bup_in.shape[1] // (width // model)
        for d in range(width // model):
            at = (d // (2 * dims[1] * dims[2]), d // (2 * dims[2]) % dims[1], d // 2 % dims[2], d % 2)
            vec_whole[at + (pl.ds(0, 8), pl.ds(0, model))] = small[:, d * model : (d + 1) * model]
            vec_whole[at + (pl.ds(8, 1), pl.ds(0, wide))] = bup_in[:, d * wide : (d + 1) * wide]
        late = list(plan.late)
        spread = max(1, len(late) // 5)
        left = None
        for k in range(5):
            take = late[k * spread : (k + 1) * spread] if k < 4 else late[4 * spread :]
            left = add_wave(jobs, take + [(last, k)]) if k < 4 else add_wave(jobs, take[:-1] + [(last, k)] + take[-1:])
            jobs[left[0]].ship(left[1])
        for job in jobs:
            job.finish()


def backward(dims, strips, row_count, turned, turned_two, out_grad, q_weight, k_weight, v_weight, vectors, small, grad_bup,
             grad_hidden, active, probs, heads, grad_context, tokens, grad_res, grad_wo):
    width, rows = turned.shape
    ff = grad_hidden.shape[1]
    slots = rows // strips
    plan = Plan(dims, strips, rows, width, ff, SCATTER_LAG, SCATTER_GAP)
    n = 2 * dims[0] * dims[1] * dims[2]
    model, wide = width // n, ff // n
    lanes_wide = 128 * -(-wide // 128)
    full = functools.partial(jax.ShapeDtypeStruct, dtype=jnp.float32)
    vmem = pl.BlockSpec(memory_space=pltpu.VMEM)

    def part(step, first, count):
        return jnp.clip(step - first, 0, count - 1)

    def strip_pair(step):
        k = part(step, plan.attention, strips * plan.pairs)
        return lax.rem(k, strips), lax.div(k, strips)

    def probs_at(step):
        strip, pair = strip_pair(step)
        return (strip * plan.pairs + pair, 0, 0, 0)

    ending = pl.BlockSpec((rows // FINISH, width), lambda step: (part(step, plan.finish, FINISH), 0))
    shapes = plan.shapes
    bufs = []
    for k, shape in enumerate(shapes):
        bufs += reduce_scratch(dims, shape, jnp.bfloat16, 1 + k % 2)
    bufs += reduce_scratch(dims, (16, lanes_wide), jnp.float32, 1 + len(shapes) % 2)
    copies = scatter_copies(dims) * (len(shapes) + 1)
    return pl.pallas_call(
        functools.partial(backward_kernel, dims, plan, strips),
        grid=(plan.steps,),
        out_shape=[full((row_count, width))] + [full((model, width))] * 4 + [full((model, ff)), full((wide, width)), full((16, lanes_wide))],
        in_specs=[vmem] * 9
        + [
            pl.BlockSpec((rows, FF_TILE), lambda step: (0, part(step, 0, plan.tiles))),
            pl.BlockSpec((rows, FF_TILE), lambda step: (0, part(step, 0, plan.tiles))),
            pl.BlockSpec((1, 2, slots, slots), probs_at),
            pl.BlockSpec((3, slots, 128), lambda step: (0,) + strip_pair(step)),
            pl.BlockSpec((slots, 128), strip_pair),
            ending, ending,
            pl.BlockSpec(memory_space=pl.ANY),
        ],
        out_specs=[vmem] * 8,
        scratch_shapes=[pltpu.VMEM((rows, width), jnp.bfloat16)] * 3
        + [pltpu.VMEM((8, width), jnp.float32), pltpu.VMEM(dims + (2, 16, lanes_wide), jnp.float32)]
        + [pltpu.VMEM((rows // FINISH, width), jnp.float32)]
        + [pltpu.VMEM(lead + dims + (2,) + shape, jnp.bfloat16) for lead, shape in plan.wholes]
        + bufs
        + [pltpu.SemaphoreType.DMA((1,)), pltpu.SemaphoreType.DMA((copies,)), pltpu.SemaphoreType.DMA((copies,))],
        compiler_params=pltpu.CompilerParams(collective_id=3, has_side_effects=True, vmem_limit_bytes=VMEM_LIMIT),
        name="backward",
    )(turned, turned_two, out_grad, q_weight, k_weight, v_weight, vectors, small, grad_bup,
      grad_hidden, active, probs, heads, grad_context, tokens, grad_res, grad_wo)


def lane_pad(rows, width):
    return jnp.pad(rows, ((0, 0), (0, width - rows.shape[1])))


def pack_vectors(vectors, wide):
    width = 128 * -(-wide.shape[0] // 128)
    rows = lane_pad(jnp.stack(vectors).astype(jnp.float32), width)
    last = lane_pad(wide[None].astype(jnp.float32), width)
    return jnp.pad(jnp.concatenate([rows, last]), ((0, 15 - len(vectors)), (0, 0)))


def shards(
    dims,
    tokens,
    lengths,
    key_mask,
    ln1_gain,
    ln1_bias,
    q_weight,
    q_bias,
    k_weight,
    v_weight,
    v_bias,
    o_weight,
    o_bias,
    ln2_gain,
    ln2_bias,
    up_weight,
    up_bias,
    down_weight,
    down_bias,
    out_grad,
):
    early_weights, late_weights = (q_weight, k_weight, v_weight), (o_weight, up_weight, down_weight)
    vectors = (ln1_gain, ln1_bias, q_bias, v_bias, o_bias, ln2_gain, ln2_bias, down_bias)
    fused = q_weight.shape[0] % 8 == 0
    axes = ("gx", "gy")

    def whole(shard):
        return lax.all_gather(shard, axes, axis=0, tiled=True)

    row_count, width = tokens.shape
    strips = lengths.shape[0]
    slots = row_count // strips
    extra = -slots % 16

    def padded(values):
        return jnp.pad(values.reshape(strips, slots, width), ((0, 0), (0, extra), (0, 0))).reshape(-1, width)

    def cropped(values):
        return values.reshape(strips, slots + extra, width)[:, :slots].reshape(row_count, width)

    slot_ids = lax.iota(jnp.int32, slots)
    visible = (slot_ids[None, :] == 0) | (slot_ids[None, :] < lengths[:, None]) & (key_mask == 1)
    mask = jnp.where(jnp.pad(visible, ((0, 0), (0, extra))), 0.0, NEG_FILL).reshape(-1, 1)

    if fused:
        turned, heads, probs, context, tokens_in, grads_in, q_full, k_full, v_full, rows, up_bias_full, *late = forward(
            dims, strips, tokens, out_grad, mask, pack_vectors(vectors, up_bias), early_weights, late_weights
        )
        o_full, up_full, down_full = [w.reshape((-1,) + w.shape[-1:]) for w in late]
    else:
        tokens_in, grads_in = padded(tokens), padded(out_grad)
        q_full, k_full, v_full, o_full, up_full, down_full = [whole(w) for w in early_weights + late_weights]
        rows = jnp.stack([whole(v) for v in vectors]).astype(jnp.float32)
        up_bias_full = whole(up_bias).astype(jnp.float32)[None]
        turned, queries, keys, values, probs, context = attend(strips, tokens_in, q_full, k_full, v_full, rows, mask)
    block_out, grad_res, grad_context, grad_wo, active, grad_hidden, turned_two, small, grad_bup = ffn(
        strips, row_count, tokens_in, context, grads_in, o_full, up_full, down_full, rows, up_bias_full
    )
    if fused:
        grad_tokens, sum_wq, sum_wk, sum_wv, sum_wo, sum_wup, sum_wdown, least = backward(
            dims, strips, row_count, turned, turned_two, grads_in, q_full, k_full, v_full, rows, small, grad_bup,
            grad_hidden, active, probs, heads, grad_context, tokens_in, grad_res,
            grad_wo.reshape(dims + (2,) + o_weight.shape),
        )
        vec = [least[n, : ln1_gain.shape[0]] for n in range(8)]
        sum_bup = least[8, : up_bias.shape[0]]
    else:
        grad_tokens, grad_wq, grad_wk, grad_wv, small_two = attend_back(
            strips, tokens_in, turned, queries, keys, values, probs, grad_context, grad_res, q_full, k_full, v_full, rows
        )
        grad_tokens = cropped(grad_tokens)
        small = small + small_two
        full = [grad_wq, grad_wk, grad_wv, grad_wo, right_mul(turned_two, grad_hidden), left_mul(active, grads_in), grad_bup[0]]
        full = [g.astype(jnp.float32) for g in full] + [small[n] for n in range(8)]
        sum_wq, sum_wk, sum_wv, sum_wo, sum_wup, sum_wdown, sum_bup, *vec = [
            lax.psum_scatter(g, axes, scatter_dimension=0, tiled=True) for g in full
        ]
    return (
        block_out, grad_tokens, vec[0], vec[1], sum_wq, vec[2], sum_wk, sum_wv, vec[3], sum_wo, vec[4],
        vec[5], vec[6], sum_wup, sum_bup, sum_wdown, vec[7],
    )


def solution(mesh):
    rows, flat = P(("gx", "gy"), None), P(("gx", "gy"))
    return jax.shard_map(
        functools.partial(shards, grid_of(mesh)),
        mesh=mesh,
        in_specs=(
            rows, flat, rows, flat, flat, rows, flat, rows, rows, flat, rows, flat, flat, flat, rows, flat, rows, flat, rows,
        ),
        out_specs=(
            rows, rows, flat, flat, rows, flat, rows, rows, flat, rows, flat, flat, flat, rows, flat, rows, flat,
        ),
        check_vma=False,
    )
```
